128 devices in a mesh: sub: 32 (over y, z, core), grp: 4 (over x).
Axes of the slice: x: 4, y: 4, z: 4, core: 2. Of those that a mesh axis runs over, the one named last changes fastest.
Arguments:
- rr_inverse: float32 [256, 512, 512], P(('sub', 'grp')), may hold values from -4 to 4, as said below
- corner_modes: float32 [256, 64, 512], P(('sub', 'grp')), may hold values from -0.5 to 0.5
- coarse_inverse: float32 [8192, 8192], P(('sub', 'grp')), may hold values from -1 to 1, as said below
- inertia: float32 [256, 512], P(('sub', 'grp')), may hold values from 0.5 to 2
- disp_now: float32 [8, 256, 512], P(None, ('sub', 'grp')), may hold values from -4 to 4
- vel_now: float32 [8, 256, 512], P(None, ('sub', 'grp')), may hold values from -4 to 4
- acc_now: float32 [8, 256, 512], P(None, ('sub', 'grp')), may hold values from -8 to 8
- load_next: float32 [8, 256, 512], P(None, ('sub', 'grp')), may hold values from -10 to 10
- basis_rows: float32 [131072, 256], P(('sub', 'grp')), may hold values from -0.015625 to 0.015625
- piece_owner: int32 [128], replicated, may hold values from 0 to 127, each once
Outputs:
- disp_new: float32 [8, 256, 512], P(None, ('sub', 'grp'))
- vel_new: float32 [8, 256, 512], P(None, ('sub', 'grp'))
- projection: float32 [256, 8], replicated
- r_factor: float32 [8, 8], replicated
- new_columns: float32 [8, 131072], P(None, ('sub', 'grp'))
The draws below stay inside these ranges and needn't reach their ends.
Inputs may be any that keep to these rules, and one draw needn't show every extreme that they name: piece_owner is a permutation. `rr_inverse`: each of the 256 blocks is symmetric positive definite. `coarse_inverse`: symmetric positive definite.
All inputs are finite; a program needn't handle non-finite values.
Results may differ from the reference program's by a relative error of at most 0.00018.
Values sent between devices are 32-bit elements; how exact they have to be, the bound alone decides.
No kernel may reach another device: no remote copies, remote signals or barrier semaphores. Data moves between devices by JAX's collectives and lax.ppermute only.
A program may use at most 64 MiB of HBM per device.

```python
import math
import jax
import jax.numpy as jnp
from jax import lax

NR = 512
NC = 32
RANK = 256
NCASE = 8
ITERS = 2
NI = 128
SUBDOMAINS = 256
NCG = 8192
NROWS = 131072
PIECES = 128


def coupled_block(key, order, floor_value, ceiling_value, shared):
    key_noise, key_diag = jax.random.split(key)
    noise = jax.random.uniform(key_noise, (order, order), jnp.float32, -1.0, 1.0)
    upper = jnp.triu(noise, 1)
    coupling = (upper + upper.T) * (0.3 * math.sqrt(3.0) / math.sqrt(order))
    logs = jax.random.uniform(key_diag, (order,), jnp.float32, math.log(floor_value), math.log(ceiling_value))
    roots = jnp.exp(0.5 * logs)
    middle = jnp.eye(order, dtype=jnp.float32) + coupling + shared / order
    return roots[:, None] * middle * roots[None, :]


def draw_rr_inverse(key, part):
    subkeys = jax.random.split(key, SUBDOMAINS)
    return lax.map(lambda single: coupled_block(single, NR, 0.05, 2.0, 0.0), subkeys)


def draw_coarse_inverse(key, part):
    return coupled_block(key, NCG, 0.1, 0.5, 0.3)


def draw_load_next(key, part):
    key_base, key_rows = jax.random.split(key, 2)
    position = jnp.arange(SUBDOMAINS, dtype=jnp.float32) / max(SUBDOMAINS - 1, 1)
    row_scale = 10.0 ** jax.random.uniform(key_rows, (1, SUBDOMAINS, NR), jnp.float32)
    base = jax.random.truncated_normal(key_base, -4.0, 4.0, (NCASE, SUBDOMAINS, NR), jnp.float32)
    ramp = 3.0 ** position
    return 0.04 * base * ramp[None, :, None] * row_scale


def shard_levels(rng, dims, cuts, low, largest):
    level, own = 1.0, jax.random.fold_in(rng, 6)
    for axis_at, blocks in cuts:
        draws = jnp.exp(jax.random.uniform(jax.random.fold_in(own, axis_at), (blocks,), jnp.float32, low / len(cuts), largest / len(cuts)))
        level = level * jnp.repeat(draws, dims[axis_at] // blocks).reshape([-1 if axis == axis_at else 1 for axis in range(len(dims))])
    return level


def gaussian(stream_key, dims, scale, most, shards=(), kind=jnp.bfloat16):
    values = jax.random.normal(stream_key, dims, jnp.float32) * scale
    if len(shards) > 0:
        values = shard_levels(stream_key, dims, shards, -0.22, 0.18) * values
    return jnp.clip(values, min=-most, max=most).astype(kind)


def setup_inputs(seed: int = 0) -> dict:
    key_of = jax.random.split(jax.random.key(seed), 11)
    return {
        "rr_inverse": draw_rr_inverse(jax.random.fold_in(key_of[10], 71), 0),
        "corner_modes": gaussian(key_of[1], (SUBDOMAINS, 2 * NC, NR), (NR // 4) ** -0.5, 0.5, ((0, 128),), jnp.float32),
        "coarse_inverse": draw_coarse_inverse(jax.random.fold_in(key_of[10], 71), 0),
        "inertia": jnp.clip(jnp.exp(math.log(2.0) - 1.3862944 * jax.random.uniform(key_of[3], (SUBDOMAINS, NR), jnp.float32) ** shard_levels(key_of[3], (SUBDOMAINS, NR), ((0, 128),), -0.2, 0.2)), 0.5, 2.0),
        "disp_now": gaussian(key_of[4], (NCASE, SUBDOMAINS, NR), 1.0, 4.0, ((1, 128),), jnp.float32),
        "vel_now": gaussian(key_of[5], (NCASE, SUBDOMAINS, NR), 1.0, 4.0, ((1, 128),), jnp.float32),
        "acc_now": gaussian(key_of[6], (NCASE, SUBDOMAINS, NR), 2.0, 8.0, ((1, 128),), jnp.float32),
        "load_next": draw_load_next(jax.random.fold_in(key_of[10], 71), 0),
        "basis_rows": gaussian(key_of[8], (NROWS, RANK), NROWS ** -0.5, 0.015625, ((0, 128),), jnp.float32),
        "piece_owner": jax.random.permutation(key_of[9], PIECES).astype(jnp.int32),
    }


highest = lax.Precision.HIGHEST
time_step = 0.5
newmark_beta = 0.25
newmark_gamma = 0.5

def green_apply(rr_inverse, corner_modes, coarse_inverse, field):

    def products(operands):
        return jnp.dot(operands[0], operands[1], precision=highest)
    local_part = lax.map(products, (rr_inverse, jnp.transpose(field, (1, 2, 0))))
    local_part = jnp.transpose(local_part, (2, 0, 1))
    corner_terms = jnp.einsum('kmb,ckb->ckm', corner_modes, field, precision=highest)
    assembled = corner_terms[:, :, NC:] + jnp.roll(corner_terms[:, :, :NC], -1, axis=1)
    coarse_rhs = assembled.reshape(NCASE, NCG)
    coarse_sol = lax.dot_general(coarse_rhs, coarse_inverse, (((1,), (1,)), ((), ())), precision=highest)
    coarse_sol = coarse_sol.reshape(NCASE, SUBDOMAINS, NC)
    coarse_values = jnp.concatenate([jnp.roll(coarse_sol, 1, axis=1), coarse_sol], axis=2)
    return local_part + jnp.einsum('kmb,ckm->ckb', corner_modes, coarse_values, precision=highest)

def interface_jump(field):
    return field[:, :, NR - NI:] - jnp.roll(field[:, :, :NI], -1, axis=1)

def spread(values):
    middle = jnp.zeros((NCASE, SUBDOMAINS, NR - 2 * NI), jnp.float32)
    return jnp.concatenate([-jnp.roll(values, 1, axis=1), middle, values], axis=2)

def reference(rr_inverse, corner_modes, coarse_inverse, inertia, disp_now, vel_now, acc_now, load_next, basis_rows, piece_owner):
    right_side = load_next + inertia[None] * (disp_now + time_step * vel_now + (0.5 - newmark_beta) * time_step * time_step * acc_now)
    green_rhs = green_apply(rr_inverse, corner_modes, coarse_inverse, right_side)
    residual = interface_jump(green_rhs)
    multipliers = jnp.zeros_like(residual)
    direction = residual
    norm_now = lax.optimization_barrier(jnp.sum(residual * residual, axis=(1, 2)))
    for iteration in range(ITERS):
        image = interface_jump(green_apply(rr_inverse, corner_modes, coarse_inverse, spread(direction)))
        curvature = lax.optimization_barrier(jnp.sum(direction * image, axis=(1, 2)))
        alpha = (norm_now / curvature)[:, None, None]
        multipliers = multipliers + alpha * direction
        residual = residual - alpha * image
        norm_next = lax.optimization_barrier(jnp.sum(residual * residual, axis=(1, 2)))
        direction = residual + (norm_next / norm_now)[:, None, None] * direction
        norm_now = norm_next
    disp_new = green_apply(rr_inverse, corner_modes, coarse_inverse, right_side - spread(multipliers))
    accel_new = (disp_new - disp_now) / (newmark_beta * time_step * time_step) - vel_now / (newmark_beta * time_step) - (0.5 / newmark_beta - 1.0) * acc_now
    vel_new = vel_now + time_step * ((1.0 - newmark_gamma) * acc_now + newmark_gamma * accel_new)
    inverse = jnp.zeros((PIECES,), jnp.int32).at[piece_owner].set(jnp.arange(PIECES, dtype=jnp.int32))
    piece_rows = NR // PIECES
    snapshots = disp_new.reshape(NCASE, SUBDOMAINS, PIECES, piece_rows)[:, :, inverse, :]
    snapshots = jnp.transpose(snapshots, (0, 2, 1, 3)).reshape(NCASE, NROWS)
    projection = lax.dot_general(basis_rows, snapshots, (((0,), (1,)), ((), ())), precision=highest)
    remainder = snapshots - lax.dot_general(projection, basis_rows, (((0,), (1,)), ((), ())), precision=highest)
    gram = lax.dot_general(remainder, remainder, (((1,), (1,)), ((), ())), precision=highest)
    lower = jnp.linalg.cholesky(gram)
    scale_rows = math.sqrt(NROWS)
    new_columns = jax.scipy.linalg.solve_triangular(lower, remainder, lower=True) * scale_rows
    r_factor = lower.T / scale_rows
    return (disp_new, vel_new, projection, r_factor, new_columns)
```

```python
import math

import jax
import jax.numpy as jnp
from jax import lax
from jax.sharding import Mesh
from jax.sharding import PartitionSpec as P

NC = 32
NI = 128
AXES = ("sub_0", "sub_1", "sub_2", "grp")
FAR, NEAR = ("sub_0", "sub_1"), ("sub_2", "grp")

highest = lax.Precision.HIGHEST
time_step = 0.5
newmark_beta = 0.25
newmark_gamma = 0.5


def exchange(pieces, axes=AXES):
    return lax.all_to_all(pieces, axes, split_axis=0, concat_axis=0, tiled=True)


def to_everyone(array, axes=AXES):
    return exchange(jnp.broadcast_to(array, (lax.axis_size(axes), *array.shape)), axes)


def shifted(array, by):
    count = lax.axis_size(AXES)
    return lax.ppermute(array, AXES, [(i, (i + by) % count) for i in range(count)])


def total(array):
    return to_everyone(to_everyone(array, NEAR).sum(axis=0), FAR).sum(axis=0)


def ein(spec, *operands):
    return jnp.einsum(spec, *operands, precision=highest)


def shards(
    rr_inverse,
    corner_modes,
    coarse_inverse,
    inertia,
    disp_now,
    vel_now,
    acc_now,
    load_next,
    basis_rows,
    piece_owner,
):
    case_count, sub_count, unknowns = disp_now.shape
    devices = lax.axis_size(AXES)
    coarse_total = coarse_inverse.shape[1]
    last = unknowns - NI

    right_modes = shifted(corner_modes, -1)
    left_edge_modes = shifted(corner_modes[1, :, last:], 1)

    def edges(field):
        return field[..., :NI], field[..., last:]

    def corner_blocks(y_first, y_last):
        d_a = -y_first[0]
        d_b = y_last[0] - y_first[1]
        d_c = y_last[1] - y_first[2]
        d_d = y_last[2]
        c0f, c0l = edges(corner_modes[0])
        c1f, c1l = edges(corner_modes[1])
        c2f, c2l = edges(right_modes[0])
        c3f, _ = edges(right_modes[1])
        mul = lambda d, m: ein("ci,mi->cm", d, m)
        h_l = mul(d_a, left_edge_modes)
        h_0 = mul(-d_a, c0f) + mul(d_b, c0l)
        h_1 = mul(-d_b, c1f) + mul(d_c, c1l)
        h_2 = mul(-d_c, c2f) + mul(d_d, c2l)
        h_3 = mul(-d_d, c3f)
        return jnp.concatenate(
            [
                h_l[:, :NC],
                h_l[:, NC:] + h_0[:, :NC],
                h_0[:, NC:] + h_1[:, :NC],
                h_1[:, NC:] + h_2[:, :NC],
                h_2[:, NC:] + h_3[:, :NC],
                h_3[:, NC:],
            ],
            axis=1,
        )

    def spread_owned(z):
        z_a, z_b = z[:, :NC], z[:, NC:]
        y_0 = ein("cm,mb->cb", z_a, corner_modes[0, NC:])
        y_1 = ein("cm,mb->cb", z, corner_modes[1])
        y_2 = ein("cm,mb->cb", z_b, right_modes[0, :NC])
        return y_0, y_1, y_2

    def blocks_of(y_0, y_1, y_2):
        return corner_blocks(
            [y_0[:, :NI], y_1[:, :NI], y_2[:, :NI]], [y_0[:, last:], y_1[:, last:], y_2[:, last:]]
        )

    coupling = blocks_of(*spread_owned(jnp.eye(2 * NC, dtype=jnp.float32)))

    def solve(blocks):
        got = to_everyone(blocks)
        width = 2 * NC
        assembled = (
            got[:, :, width : 2 * width]
            + jnp.roll(got[:, :, 2 * width :], 1, axis=0)
            + jnp.roll(got[:, :, :width], -1, axis=0)
        )
        full = jnp.transpose(assembled, (1, 0, 2)).reshape(case_count, coarse_total)
        owned = lax.dynamic_index_in_dim(assembled, lax.axis_index(AXES), 0, keepdims=False)
        return owned, lax.dot_general(
            full, coarse_inverse, (((1,), (1,)), ((), ())), precision=highest
        )

    def finish(local, z):
        y_0, y_1, y_2 = spread_owned(z)
        mine_0, mine_1 = local[:, 0] + y_0, local[:, 1] + y_1
        from_left = shifted(jnp.concatenate([mine_1[:, last:], z[:, NC:]], axis=1), 1)
        from_right = shifted(mine_0[:, :NI], -1)
        mine_0 = mine_0 + ein("cm,mb->cb", from_left[:, NI:], corner_modes[0, :NC])
        jump_a = from_left[:, :NI] - mine_0[:, :NI]
        jump_b = mine_0[:, last:] - mine_1[:, :NI]
        jump_c = mine_1[:, last:] - (from_right + y_2[:, :NI])
        return jnp.stack([mine_0, mine_1], axis=1), jump_a, jump_b, jump_c

    def local_apply(jump_a, jump_b, jump_c):
        first = jnp.stack([-jump_a, -jump_b], axis=1)
        final = jnp.stack([jump_b, jump_c], axis=1)
        out = ein("jab,cjb->cja", rr_inverse[:, :, :NI], first) + ein(
            "jab,cjb->cja", rr_inverse[:, :, last:], final
        )
        inner = jnp.sum(out[:, :, :NI] * first + out[:, :, last:] * final, axis=(1, 2))
        none = jnp.zeros((case_count, unknowns), jnp.float32)
        return out, inner, blocks_of(out[:, 0], out[:, 1], none)

    right_side = load_next + inertia[None] * (
        disp_now + time_step * vel_now + (0.5 - newmark_beta) * time_step * time_step * acc_now
    )
    terms = ein("jmb,cjb->cjm", corner_modes, right_side)
    blank = jnp.zeros((case_count, NC), jnp.float32)
    start_blocks = jnp.concatenate(
        [
            blank,
            terms[:, 0, :NC],
            terms[:, 0, NC:] + terms[:, 1, :NC],
            terms[:, 1, NC:],
            blank,
            blank,
        ],
        axis=1,
    )
    _, z_0 = solve(start_blocks)
    local_0 = ein("jab,cjb->cja", rr_inverse, right_side)
    none = jnp.zeros((case_count, unknowns), jnp.float32)
    local_blocks_0 = blocks_of(local_0[:, 0], local_0[:, 1], none)
    blocks_1 = local_blocks_0 + jnp.dot(z_0, coupling, precision=highest)
    coarse_1, z_1 = solve(blocks_1)
    green, b_a, b_b, b_c = finish(local_0, z_0)
    local_1, inner_1, local_blocks_1 = local_apply(b_a, b_b, b_c)
    blocks_2 = local_blocks_1 + jnp.dot(z_1, coupling, precision=highest)
    coarse_2, z_2 = solve(blocks_2)
    image_1, v_a, v_b, v_c = finish(local_1, z_1)
    local_2, inner_2, _ = local_apply(v_a, v_b, v_c)

    sums = jnp.stack(
        [
            jnp.sum(b_b * b_b + b_c * b_c, axis=1),
            inner_1 + jnp.sum(coarse_1 * z_1, axis=1),
            jnp.sum(v_b * v_b + v_c * v_c, axis=1),
            inner_2 + jnp.sum(coarse_2 * z_2, axis=1),
        ]
    )
    y_0, y_1, y_2 = spread_owned(z_2)
    part_2 = jnp.stack([local_2[:, 0] + y_0, local_2[:, 1] + y_1, y_2], axis=1)
    inverse = (
        jnp.zeros((devices,), jnp.int32)
        .at[piece_owner]
        .set(jnp.arange(devices, dtype=jnp.int32))
    )
    piece_rows = unknowns // devices
    sent = jnp.concatenate([green, image_1, part_2], axis=1)
    sent = sent.reshape(case_count, 7, devices, piece_rows)[:, :, inverse, :]
    sent = jnp.transpose(sent, (2, 0, 1, 3)).reshape(devices, case_count * 7 * piece_rows)
    sent = jnp.concatenate(
        [sent, jnp.broadcast_to(sums.reshape(1, -1), (devices, 4 * case_count))], axis=1
    )
    got = exchange(sent.reshape(devices, 2, 128)).reshape(devices, 256)
    sums = got[:, 7 * case_count * piece_rows :].sum(axis=0).reshape(4, case_count)
    bb, bf, ff, fff = sums
    alpha_0 = bb / bf
    norm_1 = bb - 2.0 * alpha_0 * bf + alpha_0 * alpha_0 * ff
    beta_0 = norm_1 / bb
    gain = 1.0 + beta_0
    curvature = gain * gain * bf - 2.0 * gain * alpha_0 * ff + alpha_0 * alpha_0 * fff
    alpha_1 = norm_1 / curvature
    kappa_1 = (alpha_0 + alpha_1 * gain)[:, None, None]
    kappa_2 = (alpha_1 * alpha_0)[:, None, None]

    got = got[:, : 7 * case_count * piece_rows].reshape(devices, case_count, 7, piece_rows)
    late = got[:, :, 4:6].at[:, :, 0].add(jnp.roll(got[:, :, 6], 1, axis=0))
    snapshots = got[:, :, 0:2] - kappa_1 * got[:, :, 2:4] + kappa_2 * late
    snapshots = jnp.transpose(snapshots, (1, 0, 2, 3)).reshape(case_count, -1)

    ghost = shifted(z_2[:, NC:], 1)
    image_2 = part_2[:, :2].at[:, 0].add(ein("cm,mb->cb", ghost, corner_modes[0, :NC]))
    disp_new = green - kappa_1 * image_1 + kappa_2 * image_2
    accel_new = (
        (disp_new - disp_now) / (newmark_beta * time_step * time_step)
        - vel_now / (newmark_beta * time_step)
        - (0.5 / newmark_beta - 1.0) * acc_now
    )
    vel_new = vel_now + time_step * ((1.0 - newmark_gamma) * acc_now + newmark_gamma * accel_new)

    projection = total(
        lax.dot_general(basis_rows, snapshots, (((0,), (1,)), ((), ())), precision=highest)
    )
    remainder = snapshots - lax.dot_general(
        projection, basis_rows, (((0,), (1,)), ((), ())), precision=highest
    )
    gram = lax.dot_general(remainder, remainder, (((1,), (1,)), ((), ())), precision=highest)
    lower = jnp.linalg.cholesky(to_everyone(gram).sum(axis=0))
    scale_rows = math.sqrt(snapshots.shape[1] * devices)
    new_columns = jax.scipy.linalg.solve_triangular(lower, remainder, lower=True) * scale_rows
    r_factor = lower.T / scale_rows
    return (disp_new, vel_new, projection, r_factor, new_columns)


def solution(mesh):
    finer = Mesh(
        mesh.devices.reshape(4, 4, 2, mesh.shape["grp"]), ("sub_0", "sub_1", "sub_2", "grp")
    )
    placed = (
        P(AXES, None, None),
        P(AXES, None, None),
        P(AXES, None),
        P(AXES, None),
        P(None, AXES, None),
        P(None, AXES, None),
        P(None, AXES, None),
        P(None, AXES, None),
        P(AXES, None),
        P(),
    )
    return jax.shard_map(
        shards,
        mesh=finer,
        in_specs=placed,
        out_specs=(P(None, AXES, None), P(None, AXES, None), P(), P(), P(None, AXES)),
        check_vma=False,
    )
```

```python
import functools
import math

import jax
import jax.numpy as jnp
from jax import lax
from jax.experimental import pallas as pl
from jax.experimental.pallas import tpu as pltpu
from jax.sharding import Mesh
from jax.sharding import PartitionSpec as P

NC = 32
NI = 128
LANES = 128
HALF = 64
AXES = ("sub_0", "sub_1", "sub_2", "grp")
FAR, NEAR = ("sub_0", "sub_1"), ("sub_2", "grp")

highest = lax.Precision.HIGHEST
time_step = 0.5
newmark_beta = 0.25
newmark_gamma = 0.5
f32, bf16 = jnp.float32, jnp.bfloat16
NT = (((1,), (1,)), ((), ()))
NN = (((1,), (0,)), ((), ()))
VMEM = pl.BlockSpec(memory_space=pltpu.VMEM)
SMEM = pl.BlockSpec(memory_space=pltpu.SMEM)


def exchange(pieces, axes=AXES):
    return lax.all_to_all(pieces, axes, split_axis=0, concat_axis=0, tiled=True)


def to_everyone(array, axes=AXES):
    return exchange(jnp.broadcast_to(array, (lax.axis_size(axes), *array.shape)), axes)


def shifted(array, by):
    count = lax.axis_size(AXES)
    return lax.ppermute(array, AXES, [(i, (i + by) % count) for i in range(count)])


def ein(spec, *operands):
    return jnp.einsum(spec, *operands, precision=highest)


def dot(a, b, dims):
    return lax.dot_general(a, b, dims, precision=highest, preferred_element_type=f32)


def fast(a, b, dims):
    return lax.dot_general(a, b, dims, preferred_element_type=f32)


def call(body, outs, ins, scratch=(), flops=0):
    return pl.pallas_call(
        body,
        out_shape=[jax.ShapeDtypeStruct(shape, f32 if len(rest) == 0 else rest[0]) for shape, *rest in outs],
        in_specs=ins,
        out_specs=[VMEM] * len(outs),
        scratch_shapes=list(scratch),
        cost_estimate=pl.CostEstimate(flops=flops, bytes_accessed=1 << 20, transcendentals=0),
    )


def two_parts(x):
    high = x.astype(bf16)
    return high, (x - high.astype(f32)).astype(bf16)


def three_parts(x):
    high = x.astype(bf16)
    rest = x - high.astype(f32)
    middle = rest.astype(bf16)
    return high, middle, (rest - middle.astype(f32)).astype(bf16)


def split_body(matrix_ref, parts_ref):
    rows = matrix_ref.shape[0]
    high, low = two_parts(matrix_ref[...])
    parts_ref[:rows] = high
    parts_ref[rows:] = low


def coarse_product(assembled_ref, parts_ref):
    cases = assembled_ref.shape[0]
    high, low = two_parts(assembled_ref[...])
    both = fast(jnp.concatenate([high, low], axis=0), parts_ref[...], NT)
    both = both[:cases] + both[cases:]
    return both[:, :HALF] + both[:, HALF:]


def assemble_packed(got_ref, assembled_ref):
    tiles = assembled_ref.shape[1] // LANES
    lane = lax.broadcasted_iota(jnp.int32, (4, LANES), 1)
    lower = lane < HALF
    for m in range(tiles):
        even, odd = 8 * m, 8 * m + 4
        following = 8 * ((m + 1) % tiles) + 2
        previous = 8 * ((m - 1) % tiles) + 6
        extra_even, extra_odd = got_ref[following], got_ref[previous]
        top = got_ref[even] + got_ref[odd] + jnp.where(lower, extra_odd, extra_even)
        turned = pltpu.roll(jnp.where(lower, extra_even, extra_odd), HALF, 1)
        bottom = got_ref[even + 1] + got_ref[odd + 1] + turned
        assembled_ref[0:4, m * LANES : (m + 1) * LANES] = top
        assembled_ref[4:8, m * LANES : (m + 1) * LANES] = bottom


def assemble_first(got_ref, assembled_ref):
    tiles = assembled_ref.shape[1] // LANES
    lane = lax.broadcasted_iota(jnp.int32, (8, LANES), 1)
    for m in range(tiles):
        following = (2 * m + 2) % (2 * tiles)
        own = got_ref[2 * m + 1] + jnp.where(lane < HALF, got_ref[2 * m], 0.0)
        assembled_ref[:, m * LANES : (m + 1) * LANES] = own + jnp.where(
            lane >= LANES - NC, got_ref[following], 0.0
        )


def owned_terms(device_ref, assembled_ref, z):
    device = device_ref[0]
    tile = assembled_ref[:, pl.ds(pl.multiple_of((device // 2) * LANES, LANES), LANES)]
    even = lax.rem(device, 2) == 0
    return jnp.where(even, tile[:, :HALF], tile[:, HALF:]) * z


def send_blocks(z, coupling_ref, local_ref, riding, pieces_ref):
    blocks = local_ref[...] + dot(z, coupling_ref[...], NN)
    main, extra = blocks[:, :LANES], blocks[:, LANES:]
    turned = pltpu.roll(extra, HALF, 1)
    packed = extra[0:4] + turned[4:8]
    for d in range(pieces_ref.shape[0] // 4):
        pieces_ref[4 * d] = main[0:4]
        pieces_ref[4 * d + 1] = main[4:8]
        pieces_ref[4 * d + 2] = packed
        pieces_ref[4 * d + 3] = riding(d)


def first_body(got_ref, parts_ref, coupling_ref, local_ref, square_ref, pieces_ref, z_ref, assembled_ref):
    assemble_first(got_ref, assembled_ref)
    z = coarse_product(assembled_ref, parts_ref)
    z_ref[...] = z
    send_blocks(z, coupling_ref, local_ref, lambda d: square_ref[d], pieces_ref)


def second_body(device_ref, got_ref, parts_ref, coupling_ref, local_ref, pieces_ref, z_ref, terms_ref, assembled_ref):
    assemble_packed(got_ref, assembled_ref)
    z = coarse_product(assembled_ref, parts_ref)
    z_ref[...] = z
    terms_ref[...] = owned_terms(device_ref, assembled_ref, z)
    square = got_ref[3]
    for d in range(1, got_ref.shape[0] // 4):
        square = square + got_ref[4 * d + 3]
    send_blocks(z, coupling_ref, local_ref, lambda d: square, pieces_ref)


def choose_rows(select_ref, rows):
    high, middle, low = three_parts(rows)
    select = select_ref[...]
    return fast(select, high, NT) + fast(select, middle, NT) + fast(select, low, NT)


def by_offset(field):
    lane = lax.broadcasted_iota(jnp.int32, field.shape, 1)
    return [jnp.where(lane % 4 == o, field, 0.0) for o in range(4)]


def early_body(select_ref, green_ref, image_ref, chosen_ref):
    rows = []
    for ref in (green_ref, image_ref):
        for s in range(2):
            rows += by_offset(ref[s])
    chosen_ref[...] = choose_rows(select_ref, jnp.concatenate(rows, axis=0))


def third_body(
    device_ref, got_ref, parts_ref, local_ref, modes_a_ref, modes_b_ref, modes_c_ref, select_ref, sums_ref, early_ref,
    sent_ref, z_ref, assembled_ref,
):
    assemble_packed(got_ref, assembled_ref)
    z = coarse_product(assembled_ref, parts_ref)
    z_ref[...] = z
    y_0 = local_ref[0] + dot(z[:, :NC], modes_a_ref[...], NN)
    y_1 = local_ref[1] + dot(z, modes_b_ref[...], NN)
    y_2 = dot(z[:, NC:], modes_c_ref[...], NN)
    rows = by_offset(y_0) + by_offset(y_1) + by_offset(y_2)
    rows.append(jnp.zeros((32, y_0.shape[1]), f32))
    late = choose_rows(select_ref, jnp.concatenate(rows, axis=0))
    curvature = jnp.sum(owned_terms(device_ref, assembled_ref, z), axis=1, keepdims=True)
    lane = lax.broadcasted_iota(jnp.int32, (8, LANES), 1)
    case = lax.broadcasted_iota(jnp.int32, (8, LANES), 0)
    placed = jnp.where(lane == 120 + case, curvature, 0.0)
    for k in range(4):
        placed = placed + jnp.where(lane == 96 + 8 * k + case, sums_ref[:, k : k + 1], 0.0)
    late = late + jnp.sum(placed, axis=0, keepdims=True)
    sent_ref[:, 0, :] = early_ref[...]
    sent_ref[:, 1, :] = late


def project_body(got_ref, basis_ref, part_ref, rows_ref, gains_ref):
    early, late = got_ref[:, 0, :], got_ref[:, 1, :]
    sums = jnp.broadcast_to(jnp.sum(late, axis=0, keepdims=True), (8, LANES))
    lane = lax.broadcasted_iota(jnp.int32, (8, LANES), 1)
    bb, bf, ff, fff = (pltpu.roll(sums, 32 - 8 * k, 1) for k in range(4))
    good = lane < 8
    bb, bf = jnp.where(good, bb, 1.0), jnp.where(good, bf, 1.0)
    ff, fff = jnp.where(good, ff, 2.0), jnp.where(good, fff, 8.0)
    alpha_0 = bb / bf
    norm_1 = bb - 2.0 * alpha_0 * bf + alpha_0 * alpha_0 * ff
    gain = 1.0 + norm_1 / bb
    curvature = gain * gain * bf - 2.0 * gain * alpha_0 * ff + alpha_0 * alpha_0 * fff
    alpha_1 = norm_1 / curvature
    kappas = []
    for kappa in (alpha_0 + alpha_1 * gain, alpha_1 * alpha_0):
        kappa = jnp.where(good, kappa, 0.0)
        for shift in (8, 16, 32, 64):
            kappa = kappa + pltpu.roll(kappa, shift, 1)
        kappas.append(kappa)
    gains_ref[0], gains_ref[1] = kappas[0], kappas[1]
    kappa_1, kappa_2 = kappas[0][:1], kappas[1][:1]
    wide = lax.broadcasted_iota(jnp.int32, late.shape, 1)
    extra = pltpu.roll(pltpu.roll(late, HALF, 1), 1, 0)
    last = late + jnp.where(wide < NC, extra, 0.0)
    rows = early - kappa_1 * pltpu.roll(early, HALF, 1) + kappa_2 * last
    turned = jnp.transpose(rows)
    snapshots = jnp.concatenate([turned[8 * j : 8 * j + 8] for j in range(8)], axis=1)
    rows_ref[...] = snapshots
    high, low = two_parts(snapshots)
    both = jnp.concatenate([high, low], axis=0)
    count = snapshots.shape[1]
    product = fast(both, basis_ref[:count], NN) + fast(both, basis_ref[count:], NN)
    part_ref[:, : basis_ref.shape[1]] = product[:8] + product[8:]
    part_ref[:, basis_ref.shape[1] :] = dot(
        snapshots, jnp.concatenate([snapshots, jnp.zeros((LANES - 8, count), f32)], axis=0), NT
    )


def finish_body(got_ref, square_ref, basis_ref, rows_ref, columns_ref, projection_ref, factor_ref, *, scale):
    count = got_ref.shape[0]
    reduced = got_ref[0]
    for i in range(1, count):
        reduced = reduced + got_ref[i]
    rank = reduced.shape[1] - LANES
    coefficients = reduced[:, :rank]
    projection_ref[...] = coefficients
    low_rows, high_rows = coefficients[:, :LANES], coefficients[:, LANES:]
    squares = [square_ref[:, i, :] for i in range(4)]
    image = jnp.concatenate(
        [
            dot(low_rows, squares[0], NN) + dot(high_rows, squares[2], NN),
            dot(low_rows, squares[1], NN) + dot(high_rows, squares[3], NN),
        ],
        axis=1,
    )
    gap = image - 2.0 * coefficients
    gram = reduced[:, rank : rank + 8]
    blank = jnp.zeros((LANES - 8, rank), f32)
    gram = reduced[:, rank:] + dot(coefficients, jnp.concatenate([gap, blank], axis=0), NT)
    row = lax.broadcasted_iota(jnp.int32, (8, LANES), 0)
    lane = lax.broadcasted_iota(jnp.int32, (8, LANES), 1)
    gram = jnp.where(lane < 8, gram, 0.0)
    work = gram + jnp.where(lane == row + 8, 1.0, 0.0)
    upper = jnp.zeros((8, LANES), f32)
    for j in range(8):
        pivot = jnp.sum(jnp.where((row == j) & (lane == j), work, 0.0), axis=(0, 1), keepdims=True)
        line = jnp.sum(jnp.where(row == j, work, 0.0), axis=0, keepdims=True) / jnp.sqrt(pivot)
        upper = jnp.where(row == j, line, upper)
        column = jnp.sum(jnp.where(lane == j, work, 0.0), axis=1, keepdims=True) / jnp.sqrt(pivot)
        work = jnp.where(row > j, work - column * line, work)
    factor_ref[...] = jnp.where((lane >= row) & (lane < 8), upper, 0.0) * (1.0 / scale)
    inverse = pltpu.roll(upper, LANES - 8, 1)
    inverse = jnp.where((lane <= row) & (lane < 8), inverse, 0.0)[:, :8]
    high, low = two_parts(coefficients)
    total = rows_ref.shape[1]
    both = jnp.concatenate([high, low], axis=0)
    product = fast(both, basis_ref[:total], NT) + fast(both, basis_ref[total:], NT)
    remainder = rows_ref[...] - (product[:8] + product[8:])
    columns = dot(inverse, remainder, NN) * scale
    for t in range(8):
        index = 16 * t + lane // 8
        out = jnp.zeros((8, LANES), f32)
        for j in range(8):
            picked = jnp.take_along_axis(columns[:, j * LANES : (j + 1) * LANES], index, axis=1)
            out = jnp.where(lane % 8 == j, picked, out)
        columns_ref[:, t * LANES : (t + 1) * LANES] = out


def shards(
    rr_inverse,
    corner_modes,
    coarse_inverse,
    inertia,
    disp_now,
    vel_now,
    acc_now,
    load_next,
    basis_rows,
    piece_owner,
):
    case_count, sub_count, unknowns = disp_now.shape
    devices = lax.axis_size(AXES)
    coarse_total = coarse_inverse.shape[1]
    rank = basis_rows.shape[1]
    last = unknowns - NI
    me = lax.axis_index(AXES)
    even = me % 2 == 0
    device = me.reshape(1).astype(jnp.int32)

    right_modes = shifted(corner_modes, -1)
    left_edge = shifted(corner_modes[1, :, last:], 1)

    right_side = load_next + inertia[None] * (
        disp_now + time_step * vel_now + (0.5 - newmark_beta) * time_step * time_step * acc_now
    )
    terms = ein("jmb,cjb->jcm", corner_modes, right_side)
    low, middle, high = terms[0, :, :NC], terms[0, :, NC:] + terms[1, :, :NC], terms[1, :, NC:]
    gap = jnp.zeros((case_count, NC), f32)
    start = jnp.where(
        even,
        jnp.concatenate([middle, high, gap, low], axis=1),
        jnp.concatenate([gap, low, middle, high], axis=1),
    )
    got_1 = to_everyone(start)

    (coarse_parts,) = call(split_body, [((4 * NC, coarse_total), bf16)], [VMEM], flops=1 << 22)(coarse_inverse)
    basis_sorted = basis_rows.reshape(devices, -1, rank).swapaxes(0, 1).reshape(-1, rank)
    (basis_parts,) = call(split_body, [((2 * basis_sorted.shape[0], rank), bf16)], [VMEM], flops=1 << 22)(basis_sorted)
    square = lax.dot_general(basis_rows, basis_rows, (((0,), (0,)), ((), ())), precision=highest)
    square = jnp.stack(
        [square[:LANES, :LANES], square[:LANES, LANES:], square[LANES:, :LANES], square[LANES:, LANES:]], axis=1
    )
    owner = jnp.broadcast_to(piece_owner[:, None], (devices, unknowns // devices)).reshape(1, unknowns)
    select = (owner == lax.broadcasted_iota(jnp.int32, (devices, unknowns), 0)).astype(bf16)

    zero = jnp.zeros((NC, NI), f32)
    first, final = corner_modes[:, :, :NI], corner_modes[:, :, last:]
    right_first, right_final = right_modes[:, :, :NI], right_modes[:, :, last:]
    rows = [
        [left_edge[:NC], zero, zero, zero],
        [left_edge[NC:] - first[0, :NC], final[0, :NC], zero, zero],
        [-first[0, NC:], final[0, NC:] - first[1, :NC], final[1, :NC], zero],
        [zero, -first[1, NC:], final[1, NC:] - right_first[0, :NC], right_final[0, :NC]],
        [zero, zero, -right_first[0, NC:], right_final[0, NC:] - right_first[1, :NC]],
        [zero, zero, zero, -right_first[1, NC:]],
    ]
    rows = jnp.concatenate([jnp.concatenate(parts, axis=1) for parts in rows], axis=0)
    blank = jnp.zeros((HALF, 4 * NI), f32)
    to_blocks = jnp.where(
        even,
        jnp.concatenate([rows[HALF:], blank, rows[:HALF]], axis=0),
        jnp.concatenate([rows, blank], axis=0),
    )

    def blocks_of(d_a, d_b, d_c, d_d):
        return dot(jnp.concatenate([d_a, d_b, d_c, d_d], axis=1), to_blocks, NT)

    def local_blocks(field):
        return blocks_of(
            -field[0, :, :NI], field[0, :, last:] - field[1, :, :NI], field[1, :, last:], jnp.zeros((case_count, NI), f32)
        )

    unit_0 = jnp.concatenate([corner_modes[0, NC:], jnp.zeros((NC, unknowns), f32)], axis=0)
    unit_1 = corner_modes[1]
    unit_2 = jnp.concatenate([jnp.zeros((NC, unknowns), f32), right_modes[0, :NC]], axis=0)
    coupling = blocks_of(
        -unit_0[:, :NI], unit_0[:, last:] - unit_1[:, :NI], unit_1[:, last:] - unit_2[:, :NI], unit_2[:, last:]
    )

    def finish(local, z):
        z_a, z_b = z[:, :NC], z[:, NC:]
        mine_0 = local[0] + dot(z_a, corner_modes[0, NC:], NN)
        mine_1 = local[1] + dot(z, corner_modes[1], NN)
        from_left = shifted(jnp.concatenate([mine_1[:, last:], z_b], axis=1), 1)
        from_right = shifted(mine_0[:, :NI], -1)
        mine_0 = mine_0 + dot(from_left[:, NI:], corner_modes[0, :NC], NN)
        jump_a = from_left[:, :NI] - mine_0[:, :NI]
        jump_b = mine_0[:, last:] - mine_1[:, :NI]
        jump_c = mine_1[:, last:] - (from_right + dot(z_b, right_modes[0, :NC, :NI], NN))
        return jnp.stack([mine_0, mine_1]), jump_a, jump_b, jump_c

    def local_apply(jump_a, jump_b, jump_c):
        first = jnp.stack([-jump_a, -jump_b])
        final = jnp.stack([jump_b, jump_c])
        out = ein("jcb,jab->jca", first, rr_inverse[:, :, :NI]) + ein("jcb,jab->jca", final, rr_inverse[:, :, last:])
        inner = jnp.sum(out[:, :, :NI] * first + out[:, :, last:] * final, axis=(0, 2))
        return out, inner

    local_0 = ein("cjb,jab->jca", right_side, rr_inverse)
    assembled = [pltpu.VMEM((case_count, coarse_total), f32)]
    piece_shape = ((4 * devices, 4, LANES),)
    z_shape = ((case_count, 2 * NC),)
    pieces, z_0 = call(first_body, [piece_shape, z_shape], [VMEM] * 5, assembled, flops=1 << 24)(
        got_1, coarse_parts, coupling, local_blocks(local_0), square
    )
    got_2 = exchange(pieces)
    green, b_a, b_b, b_c = finish(local_0, z_0)
    local_1, inner_1 = local_apply(b_a, b_b, b_c)
    pieces, z_1, terms_1 = call(second_body, [piece_shape, z_shape, z_shape], [SMEM] + [VMEM] * 4, assembled, flops=1 << 24)(
        device, got_2, coarse_parts, coupling, local_blocks(local_1)
    )
    got_3 = exchange(pieces)
    image_1, v_a, v_b, v_c = finish(local_1, z_1)
    local_2, inner_2 = local_apply(v_a, v_b, v_c)
    sums = jnp.stack(
        [
            jnp.sum(b_b * b_b + b_c * b_c, axis=1),
            inner_1 + jnp.sum(terms_1, axis=1),
            jnp.sum(v_b * v_b + v_c * v_c, axis=1),
            inner_2,
        ],
        axis=1,
    )
    (early,) = call(early_body, [((devices, LANES),)], [VMEM] * 3, flops=1 << 24)(select, green, image_1)
    sent, z_2 = call(third_body, [((devices, 2, LANES),), z_shape], [SMEM] + [VMEM] * 9, assembled, flops=1 << 24)(
        device, got_3, coarse_parts, local_2, corner_modes[0, NC:], corner_modes[1], right_modes[0, :NC], select, sums, early
    )
    got_4 = exchange(sent)
    ghost = shifted(z_2[:, NC:], 1)
    part, snapshots, gains = call(
        project_body,
        [((case_count, rank + LANES),), ((case_count, basis_rows.shape[0]),), ((2, case_count, LANES),)],
        [VMEM] * 2,
        flops=1 << 24,
    )(got_4, basis_parts)
    near = to_everyone(part, NEAR).sum(axis=0)
    got_5 = to_everyone(near, FAR)
    squares = got_3.reshape(devices, 4, 4, LANES)[:, 3]
    scale = math.sqrt(basis_rows.shape[0] * devices)
    new_columns, projection, factor = call(
        functools.partial(finish_body, scale=scale),
        [((case_count, basis_rows.shape[0]),), ((case_count, rank),), ((case_count, LANES),)],
        [VMEM] * 4,
        flops=1 << 24,
    )(got_5, squares, basis_parts, snapshots)

    kappa_1, kappa_2 = gains[0, 0, :case_count, None], gains[1, 0, :case_count, None]
    image_2 = jnp.stack(
        [
            local_2[0] + dot(z_2[:, :NC], corner_modes[0, NC:], NN) + dot(ghost, corner_modes[0, :NC], NN),
            local_2[1] + dot(z_2, corner_modes[1], NN),
        ]
    )
    disp_new = green - kappa_1 * image_1 + kappa_2 * image_2
    disp_new = jnp.swapaxes(disp_new, 0, 1)
    accel_new = (
        (disp_new - disp_now) / (newmark_beta * time_step * time_step)
        - vel_now / (newmark_beta * time_step)
        - (0.5 / newmark_beta - 1.0) * acc_now
    )
    vel_new = vel_now + time_step * ((1.0 - newmark_gamma) * acc_now + newmark_gamma * accel_new)
    return (disp_new, vel_new, projection.T, factor[:, :case_count], new_columns)


def solution(mesh):
    finer = Mesh(
        mesh.devices.reshape(4, 4, 2, mesh.shape["grp"]), ("sub_0", "sub_1", "sub_2", "grp")
    )
    placed = (
        P(AXES, None, None),
        P(AXES, None, None),
        P(AXES, None),
        P(AXES, None),
        P(None, AXES, None),
        P(None, AXES, None),
        P(None, AXES, None),
        P(None, AXES, None),
        P(AXES, None),
        P(),
    )
    return jax.shard_map(
        shards,
        mesh=finer,
        in_specs=placed,
        out_specs=(P(None, AXES, None), P(None, AXES, None), P(), P(), P(None, AXES)),
        check_vma=False,
    )
```

```python
import functools
import math

import jax
import jax.numpy as jnp
from jax import lax
from jax.experimental import pallas as pl
from jax.experimental.pallas import tpu as pltpu
from jax.sharding import Mesh
from jax.sharding import PartitionSpec as P

NC = 32
NI = 128
LANES = 128
HALF = 64
AXES = ("sub_0", "sub_1", "sub_2", "grp")
FAR, NEAR = ("sub_0", "sub_1"), ("sub_2", "grp")

highest = lax.Precision.HIGHEST
time_step = 0.5
newmark_beta = 0.25
newmark_gamma = 0.5
f32, bf16 = jnp.float32, jnp.bfloat16
NT = (((1,), (1,)), ((), ()))
NN = (((1,), (0,)), ((), ()))
VMEM = pl.BlockSpec(memory_space=pltpu.VMEM)
SMEM = pl.BlockSpec(memory_space=pltpu.SMEM)


def exchange(pieces, axes=AXES):
    return lax.all_to_all(pieces, axes, split_axis=0, concat_axis=0, tiled=True)


def to_everyone(array, axes=AXES):
    return exchange(jnp.broadcast_to(array, (lax.axis_size(axes), *array.shape)), axes)


def shifted(array, by):
    count = lax.axis_size(AXES)
    return lax.ppermute(array, AXES, [(i, (i + by) % count) for i in range(count)])


def ein(spec, *operands):
    return jnp.einsum(spec, *operands, precision=highest)


def dot(a, b, dims):
    return lax.dot_general(a, b, dims, precision=highest, preferred_element_type=f32)


def fast(a, b, dims):
    return lax.dot_general(a, b, dims, preferred_element_type=f32)


def call(body, outs, ins, scratch=(), flops=0):
    return pl.pallas_call(
        body,
        out_shape=[jax.ShapeDtypeStruct(shape, f32 if len(rest) == 0 else rest[0]) for shape, *rest in outs],
        in_specs=ins,
        out_specs=[VMEM] * len(outs),
        scratch_shapes=list(scratch),
        compiler_params=pltpu.CompilerParams(vmem_limit_bytes=16 << 20),
        cost_estimate=pl.CostEstimate(flops=flops, bytes_accessed=1 << 20, transcendentals=0),
    )


def two_parts(x):
    high = x.astype(bf16)
    return high, (x - high.astype(f32)).astype(bf16)


def three_parts(x):
    high = x.astype(bf16)
    rest = x - high.astype(f32)
    middle = rest.astype(bf16)
    return high, middle, (rest - middle.astype(f32)).astype(bf16)


def split_body(matrix_ref, parts_ref):
    rows = matrix_ref.shape[0]
    high, low = two_parts(matrix_ref[...])
    parts_ref[:rows] = high
    parts_ref[rows:] = low


def coarse_product(assembled_ref, parts_ref):
    cases = assembled_ref.shape[0]
    high, low = two_parts(assembled_ref[...])
    both = fast(jnp.concatenate([high, low], axis=0), parts_ref[...], NT)
    both = both[:cases] + both[cases:]
    return both[:, :HALF] + both[:, HALF:]


def assemble_packed(got_ref, assembled_ref, slots):
    tiles = assembled_ref.shape[1] // LANES
    lane = lax.broadcasted_iota(jnp.int32, (4, LANES), 1)
    lower = lane < HALF
    for m in range(tiles):
        even, odd = 2 * slots * m, 2 * slots * m + slots
        following = 2 * slots * ((m + 1) % tiles) + 2
        previous = 2 * slots * ((m - 1) % tiles) + slots + 2
        extra_even, extra_odd = got_ref[following], got_ref[previous]
        top = got_ref[even] + got_ref[odd] + jnp.where(lower, extra_odd, extra_even)
        turned = pltpu.roll(jnp.where(lower, extra_even, extra_odd), HALF, 1)
        bottom = got_ref[even + 1] + got_ref[odd + 1] + turned
        assembled_ref[0:4, m * LANES : (m + 1) * LANES] = top
        assembled_ref[4:8, m * LANES : (m + 1) * LANES] = bottom


def assemble_first(got_ref, assembled_ref):
    tiles = assembled_ref.shape[1] // LANES
    lane = lax.broadcasted_iota(jnp.int32, (8, LANES), 1)
    for m in range(tiles):
        following = (2 * m + 2) % (2 * tiles)
        own = got_ref[2 * m + 1] + jnp.where(lane < HALF, got_ref[2 * m], 0.0)
        assembled_ref[:, m * LANES : (m + 1) * LANES] = own + jnp.where(
            lane >= LANES - NC, got_ref[following], 0.0
        )


def owned_terms(device_ref, assembled_ref, z):
    device = device_ref[0]
    tile = assembled_ref[:, pl.ds(pl.multiple_of((device // 2) * LANES, LANES), LANES)]
    even = lax.rem(device, 2) == 0
    return jnp.where(even, tile[:, :HALF], tile[:, HALF:]) * z


def send_blocks(z, coupling_ref, local_ref, pieces_ref, slots, riding_ref=None):
    blocks = local_ref[...] + dot(z, coupling_ref[...], NN)
    main, extra = blocks[:, :LANES], blocks[:, LANES:]
    turned = pltpu.roll(extra, HALF, 1)
    packed = extra[0:4] + turned[4:8]
    for d in range(pieces_ref.shape[0] // slots):
        pieces_ref[slots * d] = main[0:4]
        pieces_ref[slots * d + 1] = main[4:8]
        pieces_ref[slots * d + 2] = packed
        if riding_ref is not None:
            pieces_ref[slots * d + 3] = riding_ref[d]


def first_body(got_ref, parts_ref, coupling_ref, local_ref, pieces_ref, z_ref, assembled_ref):
    assemble_first(got_ref, assembled_ref)
    z = coarse_product(assembled_ref, parts_ref)
    z_ref[...] = z
    send_blocks(z, coupling_ref, local_ref, pieces_ref, 3)


def second_body(
    device_ref, got_ref, parts_ref, coupling_ref, local_ref, square_ref, pieces_ref, z_ref, terms_ref, assembled_ref
):
    assemble_packed(got_ref, assembled_ref, 3)
    z = coarse_product(assembled_ref, parts_ref)
    z_ref[...] = z
    terms_ref[...] = owned_terms(device_ref, assembled_ref, z)
    send_blocks(z, coupling_ref, local_ref, pieces_ref, 4, square_ref)


def choose_rows(select_ref, rows):
    high, middle, low = three_parts(rows)
    select = select_ref[...]
    return fast(select, high, NT) + fast(select, middle, NT) + fast(select, low, NT)


def by_offset(field):
    lane = lax.broadcasted_iota(jnp.int32, field.shape, 1)
    return [jnp.where(lane % 4 == o, field, 0.0) for o in range(4)]


def early_body(select_ref, green_ref, image_ref, chosen_ref):
    rows = []
    for ref in (green_ref, image_ref):
        for s in range(2):
            rows += by_offset(ref[s])
    chosen_ref[...] = choose_rows(select_ref, jnp.concatenate(rows, axis=0))


def third_body(
    device_ref, got_ref, parts_ref, local_ref, modes_a_ref, modes_b_ref, modes_c_ref, select_ref, sums_ref, early_ref,
    sent_ref, z_ref, assembled_ref,
):
    assemble_packed(got_ref, assembled_ref, 4)
    z = coarse_product(assembled_ref, parts_ref)
    z_ref[...] = z
    square = got_ref[3]
    for d in range(1, got_ref.shape[0] // 4):
        square = square + got_ref[4 * d + 3]
    y_0 = local_ref[0] + dot(z[:, :NC], modes_a_ref[...], NN)
    y_1 = local_ref[1] + dot(z, modes_b_ref[...], NN)
    y_2 = dot(z[:, NC:], modes_c_ref[...], NN)
    rows = by_offset(y_0) + by_offset(y_1) + by_offset(y_2)
    rows.append(jnp.zeros((32, y_0.shape[1]), f32))
    late = choose_rows(select_ref, jnp.concatenate(rows, axis=0))
    curvature = jnp.sum(owned_terms(device_ref, assembled_ref, z), axis=1, keepdims=True)
    lane = lax.broadcasted_iota(jnp.int32, (8, LANES), 1)
    case = lax.broadcasted_iota(jnp.int32, (8, LANES), 0)
    placed = jnp.where(lane == 120 + case, curvature, 0.0)
    for k in range(4):
        placed = placed + jnp.where(lane == 96 + 8 * k + case, sums_ref[:, k : k + 1], 0.0)
    late = late + jnp.sum(placed, axis=0, keepdims=True)
    sent_ref[:, 0, 0, :] = early_ref[...]
    sent_ref[:, 0, 1, :] = late
    sent_ref[:, 1] = jnp.broadcast_to(square[None, 0:2], (late.shape[0], 2, LANES))
    sent_ref[:, 2] = jnp.broadcast_to(square[None, 2:4], (late.shape[0], 2, LANES))


def project_body(got_ref, basis_ref, part_ref, rows_ref, gains_ref):
    early, late = got_ref[:, 0, 0, :], got_ref[:, 0, 1, :]
    sums = jnp.broadcast_to(jnp.sum(late, axis=0, keepdims=True), (8, LANES))
    lane = lax.broadcasted_iota(jnp.int32, (8, LANES), 1)
    bb, bf, ff, fff = (pltpu.roll(sums, 32 - 8 * k, 1) for k in range(4))
    good = lane < 8
    bb, bf = jnp.where(good, bb, 1.0), jnp.where(good, bf, 1.0)
    ff, fff = jnp.where(good, ff, 2.0), jnp.where(good, fff, 8.0)
    alpha_0 = bb / bf
    norm_1 = bb - 2.0 * alpha_0 * bf + alpha_0 * alpha_0 * ff
    gain = 1.0 + norm_1 / bb
    curvature = gain * gain * bf - 2.0 * gain * alpha_0 * ff + alpha_0 * alpha_0 * fff
    alpha_1 = norm_1 / curvature
    kappas = []
    for kappa in (alpha_0 + alpha_1 * gain, alpha_1 * alpha_0):
        kappa = jnp.where(good, kappa, 0.0)
        for shift in (8, 16, 32, 64):
            kappa = kappa + pltpu.roll(kappa, shift, 1)
        kappas.append(kappa)
    gains_ref[0], gains_ref[1] = kappas[0], kappas[1]
    kappa_1, kappa_2 = kappas[0][:1], kappas[1][:1]
    wide = lax.broadcasted_iota(jnp.int32, late.shape, 1)
    extra = pltpu.roll(pltpu.roll(late, HALF, 1), 1, 0)
    last = late + jnp.where(wide < NC, extra, 0.0)
    rows = early - kappa_1 * pltpu.roll(early, HALF, 1) + kappa_2 * last
    turned = jnp.transpose(rows)
    snapshots = jnp.concatenate([turned[8 * j : 8 * j + 8] for j in range(8)], axis=1)
    rows_ref[...] = snapshots
    high, low = two_parts(snapshots)
    both = jnp.concatenate([high, low], axis=0)
    count = snapshots.shape[1]
    product = fast(both, basis_ref[:count], NN) + fast(both, basis_ref[count:], NN)
    gram = dot(snapshots, jnp.concatenate([snapshots, jnp.zeros((LANES - 8, count), f32)], axis=0), NT)
    part = jnp.concatenate([product[:8] + product[8:], gram], axis=1)
    for d in range(part_ref.shape[0]):
        part_ref[d] = part


def finish_body(got_ref, square_ref, basis_ref, rows_ref, columns_ref, projection_ref, factor_ref, *, scale):
    count = got_ref.shape[0]
    reduced = got_ref[0]
    for i in range(1, count):
        reduced = reduced + got_ref[i]
    rank = reduced.shape[1] - LANES
    coefficients = reduced[:, :rank]
    projection_ref[...] = coefficients
    low_rows, high_rows = coefficients[:, :LANES], coefficients[:, LANES:]
    squares = [square_ref[:, 1 + i // 2, i % 2, :] for i in range(4)]
    image = jnp.concatenate(
        [
            dot(low_rows, squares[0], NN) + dot(high_rows, squares[2], NN),
            dot(low_rows, squares[1], NN) + dot(high_rows, squares[3], NN),
        ],
        axis=1,
    )
    gap = image - 2.0 * coefficients
    blank = jnp.zeros((LANES - 8, rank), f32)
    gram = reduced[:, rank:] + dot(coefficients, jnp.concatenate([gap, blank], axis=0), NT)
    row = lax.broadcasted_iota(jnp.int32, (8, LANES), 0)
    lane = lax.broadcasted_iota(jnp.int32, (8, LANES), 1)
    gram = jnp.where(lane < 8, gram, 0.0)
    work = gram + jnp.where(lane == row + 8, 1.0, 0.0)
    upper = jnp.zeros((8, LANES), f32)
    for j in range(8):
        pivot = jnp.sum(jnp.where((row == j) & (lane == j), work, 0.0), axis=(0, 1), keepdims=True)
        line = jnp.sum(jnp.where(row == j, work, 0.0), axis=0, keepdims=True) / jnp.sqrt(pivot)
        upper = jnp.where(row == j, line, upper)
        column = jnp.sum(jnp.where(lane == j, work, 0.0), axis=1, keepdims=True) / jnp.sqrt(pivot)
        work = jnp.where(row > j, work - column * line, work)
    factor_ref[...] = jnp.where((lane >= row) & (lane < 8), upper, 0.0) * (1.0 / scale)
    inverse = pltpu.roll(upper, LANES - 8, 1)
    inverse = jnp.where((lane <= row) & (lane < 8), inverse, 0.0)[:, :8]
    high, low = two_parts(coefficients)
    total = rows_ref.shape[1]
    both = jnp.concatenate([high, low], axis=0)
    product = fast(both, basis_ref[:total], NT) + fast(both, basis_ref[total:], NT)
    remainder = rows_ref[...] - (product[:8] + product[8:])
    columns = dot(inverse, remainder, NN) * scale
    for t in range(8):
        index = 16 * t + lane // 8
        out = jnp.zeros((8, LANES), f32)
        for j in range(8):
            picked = jnp.take_along_axis(columns[:, j * LANES : (j + 1) * LANES], index, axis=1)
            out = jnp.where(lane % 8 == j, picked, out)
        columns_ref[:, t * LANES : (t + 1) * LANES] = out


def shards(
    rr_inverse,
    corner_modes,
    coarse_inverse,
    inertia,
    disp_now,
    vel_now,
    acc_now,
    load_next,
    basis_rows,
    piece_owner,
):
    case_count, _, unknowns = disp_now.shape
    devices = lax.axis_size(AXES)
    coarse_total = coarse_inverse.shape[1]
    rank = basis_rows.shape[1]
    last = unknowns - NI
    me = lax.axis_index(AXES)
    even = me % 2 == 0
    device = me.reshape(1).astype(jnp.int32)

    right_side = load_next + inertia[None] * (
        disp_now + time_step * vel_now + (0.5 - newmark_beta) * time_step * time_step * acc_now
    )
    terms = ein("jmb,cjb->jcm", corner_modes, right_side)
    low, middle, high = terms[0, :, :NC], terms[0, :, NC:] + terms[1, :, :NC], terms[1, :, NC:]
    gap = jnp.zeros((case_count, NC), f32)
    start = jnp.where(
        even,
        jnp.concatenate([middle, high, gap, low], axis=1),
        jnp.concatenate([gap, low, middle, high], axis=1),
    )
    got_1 = to_everyone(start)
    right_modes = shifted(corner_modes, -1)
    left_edge = shifted(corner_modes[1, :, last:], 1)

    (coarse_parts,) = call(split_body, [((4 * NC, coarse_total), bf16)], [VMEM], flops=1 << 22)(coarse_inverse)
    zero = jnp.zeros((NC, NI), f32)
    first, final = corner_modes[:, :, :NI], corner_modes[:, :, last:]
    right_first, right_final = right_modes[:, :, :NI], right_modes[:, :, last:]
    rows = [
        [left_edge[:NC], zero, zero, zero],
        [left_edge[NC:] - first[0, :NC], final[0, :NC], zero, zero],
        [-first[0, NC:], final[0, NC:] - first[1, :NC], final[1, :NC], zero],
        [zero, -first[1, NC:], final[1, NC:] - right_first[0, :NC], right_final[0, :NC]],
        [zero, zero, -right_first[0, NC:], right_final[0, NC:] - right_first[1, :NC]],
        [zero, zero, zero, -right_first[1, NC:]],
    ]
    rows = jnp.concatenate([jnp.concatenate(parts, axis=1) for parts in rows], axis=0)
    blank = jnp.zeros((HALF, 4 * NI), f32)
    to_blocks = jnp.where(
        even,
        jnp.concatenate([rows[HALF:], blank, rows[:HALF]], axis=0),
        jnp.concatenate([rows, blank], axis=0),
    )

    def blocks_of(d_a, d_b, d_c, d_d):
        return dot(jnp.concatenate([d_a, d_b, d_c, d_d], axis=1), to_blocks, NT)

    def local_blocks(field):
        return blocks_of(
            -field[0, :, :NI], field[0, :, last:] - field[1, :, :NI], field[1, :, last:], jnp.zeros((case_count, NI), f32)
        )

    unit_0 = jnp.concatenate([corner_modes[0, NC:], jnp.zeros((NC, unknowns), f32)], axis=0)
    unit_1 = corner_modes[1]
    unit_2 = jnp.concatenate([jnp.zeros((NC, unknowns), f32), right_modes[0, :NC]], axis=0)
    coupling = blocks_of(
        -unit_0[:, :NI], unit_0[:, last:] - unit_1[:, :NI], unit_1[:, last:] - unit_2[:, :NI], unit_2[:, last:]
    )

    def finish(local, z):
        z_a, z_b = z[:, :NC], z[:, NC:]
        mine_0 = local[0] + dot(z_a, corner_modes[0, NC:], NN)
        mine_1 = local[1] + dot(z, corner_modes[1], NN)
        from_left = shifted(jnp.concatenate([mine_1[:, last:], z_b], axis=1), 1)
        from_right = shifted(mine_0[:, :NI], -1)
        mine_0 = mine_0 + dot(from_left[:, NI:], corner_modes[0, :NC], NN)
        jump_a = from_left[:, :NI] - mine_0[:, :NI]
        jump_b = mine_0[:, last:] - mine_1[:, :NI]
        jump_c = mine_1[:, last:] - (from_right + dot(z_b, right_modes[0, :NC, :NI], NN))
        return jnp.stack([mine_0, mine_1]), jump_a, jump_b, jump_c

    def local_apply(jump_a, jump_b, jump_c):
        first = jnp.stack([-jump_a, -jump_b])
        final = jnp.stack([jump_b, jump_c])
        out = ein("jcb,jab->jca", first, rr_inverse[:, :, :NI]) + ein("jcb,jab->jca", final, rr_inverse[:, :, last:])
        inner = jnp.sum(out[:, :, :NI] * first + out[:, :, last:] * final, axis=(0, 2))
        return out, inner

    local_0 = ein("cjb,jab->jca", right_side, rr_inverse)
    assembled = [pltpu.VMEM((case_count, coarse_total), f32)]
    z_shape = ((case_count, 2 * NC),)
    pieces, z_0 = call(first_body, [((3 * devices, 4, LANES),), z_shape], [VMEM] * 4, assembled, flops=1 << 24)(
        got_1, coarse_parts, coupling, local_blocks(local_0)
    )
    got_2 = exchange(pieces)
    green, b_a, b_b, b_c = finish(local_0, z_0)
    b_b, basis_rows, piece_owner = lax.optimization_barrier((b_b, basis_rows, piece_owner))
    basis_sorted = basis_rows.reshape(devices, -1, rank).swapaxes(0, 1).reshape(-1, rank)
    (basis_parts,) = call(split_body, [((2 * basis_sorted.shape[0], rank), bf16)], [VMEM], flops=1 << 22)(basis_sorted)
    square = lax.dot_general(basis_rows, basis_rows, (((0,), (0,)), ((), ())), precision=highest)
    square = jnp.stack(
        [square[:LANES, :LANES], square[:LANES, LANES:], square[LANES:, :LANES], square[LANES:, LANES:]], axis=1
    )
    owner = jnp.broadcast_to(piece_owner[:, None], (devices, unknowns // devices)).reshape(1, unknowns)
    select = (owner == lax.broadcasted_iota(jnp.int32, (devices, unknowns), 0)).astype(bf16)

    local_1, inner_1 = local_apply(b_a, b_b, b_c)
    pieces, z_1, terms_1 = call(
        second_body, [((4 * devices, 4, LANES),), z_shape, z_shape], [SMEM] + [VMEM] * 5, assembled, flops=1 << 24
    )(device, got_2, coarse_parts, coupling, local_blocks(local_1), square)
    got_3 = exchange(pieces)
    image_1, v_a, v_b, v_c = finish(local_1, z_1)
    local_2, inner_2 = local_apply(v_a, v_b, v_c)
    sums = jnp.stack(
        [
            jnp.sum(b_b * b_b + b_c * b_c, axis=1),
            inner_1 + jnp.sum(terms_1, axis=1),
            jnp.sum(v_b * v_b + v_c * v_c, axis=1),
            inner_2,
        ],
        axis=1,
    )
    (early,) = call(early_body, [((devices, LANES),)], [VMEM] * 3, flops=1 << 24)(select, green, image_1)
    sent, z_2 = call(third_body, [((devices, 3, 2, LANES),), z_shape], [SMEM] + [VMEM] * 9, assembled, flops=1 << 24)(
        device, got_3, coarse_parts, local_2, corner_modes[0, NC:], corner_modes[1], right_modes[0, :NC], select, sums, early
    )
    got_4 = exchange(sent)
    ghost = shifted(z_2[:, NC:], 1)
    part, snapshots, gains = call(
        project_body,
        [
            ((lax.axis_size(NEAR), case_count, rank + LANES),),
            ((case_count, basis_rows.shape[0]),),
            ((2, case_count, LANES),),
        ],
        [VMEM] * 2,
        flops=1 << 24,
    )(got_4, basis_parts)
    near = exchange(part, NEAR).sum(axis=0)
    got_5 = to_everyone(near, FAR)
    scale = math.sqrt(basis_rows.shape[0] * devices)
    new_columns, projection, factor = call(
        functools.partial(finish_body, scale=scale),
        [((case_count, basis_rows.shape[0]),), ((case_count, rank),), ((case_count, LANES),)],
        [VMEM] * 4,
        flops=1 << 24,
    )(got_5, got_4, basis_parts, snapshots)

    kappa_1, kappa_2 = gains[0, 0, :case_count, None], gains[1, 0, :case_count, None]
    image_2 = jnp.stack(
        [
            local_2[0] + dot(z_2[:, :NC], corner_modes[0, NC:], NN) + dot(ghost, corner_modes[0, :NC], NN),
            local_2[1] + dot(z_2, corner_modes[1], NN),
        ]
    )
    disp_new = green - kappa_1 * image_1 + kappa_2 * image_2
    disp_new = jnp.swapaxes(disp_new, 0, 1)
    accel_new = (
        (disp_new - disp_now) / (newmark_beta * time_step * time_step)
        - vel_now / (newmark_beta * time_step)
        - (0.5 / newmark_beta - 1.0) * acc_now
    )
    vel_new = vel_now + time_step * ((1.0 - newmark_gamma) * acc_now + newmark_gamma * accel_new)
    return (disp_new, vel_new, projection.T, factor[:, :case_count], new_columns)


def solution(mesh):
    finer = Mesh(
        mesh.devices.reshape(4, 4, 2, mesh.shape["grp"]), ("sub_0", "sub_1", "sub_2", "grp")
    )
    placed = (
        P(AXES, None, None),
        P(AXES, None, None),
        P(AXES, None),
        P(AXES, None),
        P(None, AXES, None),
        P(None, AXES, None),
        P(None, AXES, None),
        P(None, AXES, None),
        P(AXES, None),
        P(),
    )

    return jax.shard_map(
        shards,
        mesh=finer,
        in_specs=placed,
        out_specs=(P(None, AXES, None), P(None, AXES, None), P(), P(), P(None, AXES)),
        check_vma=False,
    )
```

```python
import functools
import math

import jax
import jax.numpy as jnp
from jax import lax
from jax.experimental import pallas as pl
from jax.experimental.pallas import tpu as pltpu
from jax.sharding import Mesh
from jax.sharding import PartitionSpec as P

NC = 32
NI = 128
LANES = 128
HALF = 64
AXES = ("sub_0", "sub_1", "sub_2", "grp")
FAR, NEAR = ("sub_0", "sub_1"), ("sub_2", "grp")

highest = lax.Precision.HIGHEST
time_step = 0.5
newmark_beta = 0.25
newmark_gamma = 0.5
f32, bf16 = jnp.float32, jnp.bfloat16
NT = (((1,), (1,)), ((), ()))
NN = (((1,), (0,)), ((), ()))
VMEM = pl.BlockSpec(memory_space=pltpu.VMEM)
SMEM = pl.BlockSpec(memory_space=pltpu.SMEM)


def exchange(pieces, axes=AXES):
    return lax.all_to_all(pieces, axes, split_axis=0, concat_axis=0, tiled=True)


def to_everyone(array, axes=AXES):
    return exchange(jnp.broadcast_to(array, (lax.axis_size(axes), *array.shape)), axes)


def shifted(array, by):
    count = lax.axis_size(AXES)
    return lax.ppermute(array, AXES, [(i, (i + by) % count) for i in range(count)])


def dot(a, b, dims):
    return lax.dot_general(a, b, dims, precision=highest, preferred_element_type=f32)


def fast(a, b, dims):
    return lax.dot_general(a, b, dims, preferred_element_type=f32)


def call(body, outs, ins, scratch=(), flops=0):
    return pl.pallas_call(
        body,
        out_shape=[jax.ShapeDtypeStruct(shape, f32 if len(rest) == 0 else rest[0]) for shape, *rest in outs],
        in_specs=ins,
        out_specs=[VMEM] * len(outs),
        scratch_shapes=list(scratch),
        compiler_params=pltpu.CompilerParams(vmem_limit_bytes=16 << 20),
        cost_estimate=pl.CostEstimate(flops=flops, bytes_accessed=1 << 20, transcendentals=0),
    )


def two_parts(x):
    high = x.astype(bf16)
    return high, (x - high.astype(f32)).astype(bf16)


def three_parts(x):
    high = x.astype(bf16)
    rest = x - high.astype(f32)
    middle = rest.astype(bf16)
    return high, middle, (rest - middle.astype(f32)).astype(bf16)


def start_body(device_ref, load_ref, inertia_ref, disp_ref, vel_ref, acc_ref, modes_ref, start_ref, right_ref):
    blank = jnp.zeros((NC, modes_ref.shape[2]), f32)
    fields = []
    for s in range(2):
        moved = disp_ref[:, s, :] + time_step * vel_ref[:, s, :]
        moved = moved + (0.5 - newmark_beta) * time_step * time_step * acc_ref[:, s, :]
        fields.append(load_ref[:, s, :] + inertia_ref[s : s + 1] * moved)
        right_ref[s] = fields[s]
    part_0 = jnp.concatenate([modes_ref[0, NC:], blank, blank, modes_ref[0, :NC]], axis=0)
    part_1 = jnp.concatenate([modes_ref[1, :NC], modes_ref[1, NC:], blank, blank], axis=0)
    blocks = dot(fields[0], part_0, NT) + dot(fields[1], part_1, NT)
    even = lax.rem(device_ref[0], 2) == 0
    blocks = jnp.where(even, blocks, pltpu.roll(blocks, HALF, 1))
    for d in range(start_ref.shape[0]):
        start_ref[d] = blocks


def pre_body(matrix_ref, right_ref, rr_ref, parts_ref, local_ref):
    rows = matrix_ref.shape[0]
    high, low = two_parts(matrix_ref[...])
    parts_ref[:rows] = high
    parts_ref[rows:] = low
    for s in range(2):
        local_ref[s] = dot(right_ref[s], rr_ref[s], NN)


def couple_body(device_ref, modes_ref, right_ref, left_ref, local_ref, blocks_ref, coupling_ref, to_blocks_ref):
    last = modes_ref.shape[2] - NI
    even = jnp.where(lax.rem(device_ref[0], 2) == 0, 1, 0)
    first, final = [modes_ref[s, :, :NI] for s in range(2)], [modes_ref[s, :, last:] for s in range(2)]
    right_first, right_final = [right_ref[s, :, :NI] for s in range(2)], right_ref[0, :, last:]
    left = left_ref[...]
    rows = [
        {0: left[:NC]},
        {0: left[NC:] - first[0][:NC], 1: final[0][:NC]},
        {0: -first[0][NC:], 1: final[0][NC:] - first[1][:NC], 2: final[1][:NC]},
        {1: -first[1][NC:], 2: final[1][NC:] - right_first[0][:NC], 3: right_final[:NC]},
        {2: -right_first[0][NC:], 3: right_final[NC:] - right_first[1][:NC]},
        {3: -right_first[1][NC:]},
    ]
    to_blocks_ref[...] = jnp.zeros(to_blocks_ref.shape, f32)
    for i, parts in enumerate(rows):
        at = pl.multiple_of(lax.rem(i * NC + 192 * even, 256), NC)
        for k, values in parts.items():
            to_blocks_ref[pl.ds(at, NC), k * NI : (k + 1) * NI] = values
    blank = jnp.zeros((NC, modes_ref.shape[2]), f32)
    unit_0 = jnp.concatenate([modes_ref[0, NC:], blank], axis=0)
    unit_1 = modes_ref[1]
    unit_2 = jnp.concatenate([blank, right_ref[0, :NC]], axis=0)
    jumps = jnp.concatenate(
        [-unit_0[:, :NI], unit_0[:, last:] - unit_1[:, :NI], unit_1[:, last:] - unit_2[:, :NI], unit_2[:, last:]], axis=1
    )
    coupling_ref[...] = dot(jumps, to_blocks_ref[...], NT)
    blocks_ref[...] = own_blocks(local_ref[0], local_ref[1], to_blocks_ref)


def own_blocks(field_0, field_1, to_blocks_ref):
    last = field_0.shape[1] - NI
    jumps = [-field_0[:, :NI], field_0[:, last:] - field_1[:, :NI], field_1[:, last:]]
    return dot(jnp.concatenate(jumps, axis=1), to_blocks_ref[:, : 3 * NI], NT)


def edge_body(local_ref, z_ref, modes_ref, mine_ref, to_right_ref, to_left_ref):
    last = local_ref.shape[2] - NI
    z = z_ref[...]
    mine_0 = local_ref[0] + dot(z[:, :NC], modes_ref[0, NC:], NN)
    mine_1 = local_ref[1] + dot(z, modes_ref[1], NN)
    mine_ref[0], mine_ref[1] = mine_0, mine_1
    to_left_ref[...] = mine_0[:, :NI]
    to_right_ref[:, :NI] = mine_1[:, last:]
    to_right_ref[:, NI:] = jnp.concatenate([z, z], axis=1)


def join_body(
    mine_ref, from_left_ref, from_right_ref, z_ref, modes_ref, right_ref, rr_ref, to_blocks_ref,
    field_ref, local_ref, blocks_ref, sums_ref,
):
    last = mine_ref.shape[2] - NI
    mine_1 = mine_ref[1]
    ghost = from_left_ref[:, NI : NI + 2 * NC]
    mine_0 = mine_ref[0] + dot(ghost[:, NC:], modes_ref[0, :NC], NN)
    field_ref[0], field_ref[1] = mine_0, mine_1
    jump_a = from_left_ref[:, :NI] - mine_0[:, :NI]
    jump_b = mine_0[:, last:] - mine_1[:, :NI]
    jump_c = mine_1[:, last:] - (from_right_ref[...] + dot(z_ref[:, NC:], right_ref[0, :NC, :NI], NN))
    inner = jnp.zeros((mine_1.shape[0], 1), f32)
    outs = []
    for s, (first, final) in enumerate([(-jump_a, jump_b), (-jump_b, jump_c)]):
        out = dot(first, rr_ref[s, :NI], NN) + dot(final, rr_ref[s, last:], NN)
        local_ref[s] = out
        inner = inner + jnp.sum(out[:, :NI] * first + out[:, last:] * final, axis=1, keepdims=True)
        outs.append(out)
    blocks_ref[...] = own_blocks(outs[0], outs[1], to_blocks_ref)
    square = jnp.sum(jump_b * jump_b + jump_c * jump_c, axis=1, keepdims=True)
    lane = lax.broadcasted_iota(jnp.int32, sums_ref.shape, 1)
    sums_ref[...] = jnp.where(lane == 0, square, 0.0) + jnp.where(lane == 1, inner, 0.0)


def prep_body(basis_ref, owner_ref, after_ref, parts_ref, square_ref, select_ref):
    devices, width, rank = basis_ref.shape
    total = devices * width
    square = jnp.zeros((rank, rank), f32)
    for j in range(width):
        rows = basis_ref[:, j, :]
        high, low = two_parts(rows)
        parts_ref[j * devices : (j + 1) * devices] = high
        parts_ref[total + j * devices : total + (j + 1) * devices] = low
        turned_high, turned_low = two_parts(jnp.transpose(rows))
        square = square + fast(turned_high, high, NN) + (fast(turned_high, low, NN) + fast(turned_low, high, NN))
    for i in range(4):
        r, h = i // 2, i % 2
        square_ref[:, i, :] = square[r * LANES : (r + 1) * LANES, h * LANES : (h + 1) * LANES]
    unknowns = select_ref.shape[1]
    rows = lax.broadcasted_iota(jnp.int32, (devices, unknowns), 0)
    columns = lax.broadcasted_iota(jnp.int32, (devices, unknowns), 1)
    each = unknowns // devices
    repeat = jnp.where(columns // each == rows, 1.0, 0.0).astype(bf16)
    owner = jnp.broadcast_to(owner_ref[...].astype(f32), (8, devices)).astype(bf16)
    owner = fast(owner, repeat, NN)[:1]
    select_ref[...] = jnp.where(owner == rows.astype(f32), 1.0, 0.0).astype(bf16)


def out_body(
    green_ref, image_ref, local_ref, z_ref, ghost_ref, modes_ref, gains_ref, disp_ref, vel_ref, acc_ref,
    disp_out_ref, vel_out_ref,
):
    kappa_1, kappa_2 = gains_ref[0], gains_ref[1]
    case = lax.broadcasted_iota(jnp.int32, kappa_1.shape, 0)
    lane = lax.broadcasted_iota(jnp.int32, kappa_1.shape, 1)
    kappa_1 = jnp.sum(jnp.where(case == lane, kappa_1, 0.0), axis=1, keepdims=True)
    kappa_2 = jnp.sum(jnp.where(case == lane, kappa_2, 0.0), axis=1, keepdims=True)
    z = z_ref[...]
    late = [
        local_ref[0] + dot(z[:, :NC], modes_ref[0, NC:], NN) + dot(ghost_ref[:, NC:], modes_ref[0, :NC], NN),
        local_ref[1] + dot(z, modes_ref[1], NN),
    ]
    for s in range(2):
        disp = green_ref[s] - kappa_1 * image_ref[s] + kappa_2 * late[s]
        vel, acc = vel_ref[:, s, :], acc_ref[:, s, :]
        accel = (
            (disp - disp_ref[:, s, :]) * (1.0 / (newmark_beta * time_step * time_step))
            - vel * (1.0 / (newmark_beta * time_step))
            - (0.5 / newmark_beta - 1.0) * acc
        )
        disp_out_ref[:, s, :] = disp
        vel_out_ref[:, s, :] = vel + time_step * ((1.0 - newmark_gamma) * acc + newmark_gamma * accel)


def coarse_product(assembled_ref, parts_ref):
    cases = assembled_ref.shape[0]
    high, low = two_parts(assembled_ref[...])
    both = fast(jnp.concatenate([high, low], axis=0), parts_ref[...], NT)
    both = both[:cases] + both[cases:]
    return both[:, :HALF] + both[:, HALF:]


def assemble_packed(got_ref, assembled_ref, slots):
    tiles = assembled_ref.shape[1] // LANES
    lane = lax.broadcasted_iota(jnp.int32, (4, LANES), 1)
    lower = lane < HALF
    for m in range(tiles):
        even, odd = 2 * slots * m, 2 * slots * m + slots
        following = 2 * slots * ((m + 1) % tiles) + 2
        previous = 2 * slots * ((m - 1) % tiles) + slots + 2
        extra_even, extra_odd = got_ref[following], got_ref[previous]
        top = got_ref[even] + got_ref[odd] + jnp.where(lower, extra_odd, extra_even)
        turned = pltpu.roll(jnp.where(lower, extra_even, extra_odd), HALF, 1)
        bottom = got_ref[even + 1] + got_ref[odd + 1] + turned
        assembled_ref[0:4, m * LANES : (m + 1) * LANES] = top
        assembled_ref[4:8, m * LANES : (m + 1) * LANES] = bottom


def assemble_first(got_ref, assembled_ref):
    tiles = assembled_ref.shape[1] // LANES
    lane = lax.broadcasted_iota(jnp.int32, (8, LANES), 1)
    for m in range(tiles):
        following = (2 * m + 2) % (2 * tiles)
        own = got_ref[2 * m + 1] + jnp.where(lane < HALF, got_ref[2 * m], 0.0)
        assembled_ref[:, m * LANES : (m + 1) * LANES] = own + jnp.where(
            lane >= LANES - NC, got_ref[following], 0.0
        )


def owned_terms(device_ref, assembled_ref, z):
    device = device_ref[0]
    tile = assembled_ref[:, pl.ds(pl.multiple_of((device // 2) * LANES, LANES), LANES)]
    even = lax.rem(device, 2) == 0
    return jnp.where(even, tile[:, :HALF], tile[:, HALF:]) * z


def send_blocks(z, coupling_ref, local_ref, pieces_ref, slots, riding_ref=None):
    blocks = local_ref[...] + dot(z, coupling_ref[...], NN)
    main, extra = blocks[:, :LANES], blocks[:, LANES:]
    turned = pltpu.roll(extra, HALF, 1)
    packed = extra[0:4] + turned[4:8]
    for d in range(pieces_ref.shape[0] // slots):
        pieces_ref[slots * d] = main[0:4]
        pieces_ref[slots * d + 1] = main[4:8]
        pieces_ref[slots * d + 2] = packed
        if riding_ref is not None:
            pieces_ref[slots * d + 3] = riding_ref[d]


def first_body(got_ref, parts_ref, coupling_ref, local_ref, pieces_ref, z_ref, assembled_ref):
    assemble_first(got_ref, assembled_ref)
    z = coarse_product(assembled_ref, parts_ref)
    z_ref[...] = z
    send_blocks(z, coupling_ref, local_ref, pieces_ref, 3)


def second_body(
    device_ref, got_ref, parts_ref, coupling_ref, local_ref, square_ref, pieces_ref, z_ref, terms_ref, assembled_ref
):
    assemble_packed(got_ref, assembled_ref, 3)
    z = coarse_product(assembled_ref, parts_ref)
    z_ref[...] = z
    terms_ref[...] = owned_terms(device_ref, assembled_ref, z)
    send_blocks(z, coupling_ref, local_ref, pieces_ref, 4, square_ref)


def choose_rows(select_ref, rows):
    high, middle, low = three_parts(rows)
    select = select_ref[...]
    return fast(select, high, NT) + fast(select, middle, NT) + fast(select, low, NT)


def by_offset(field):
    lane = lax.broadcasted_iota(jnp.int32, field.shape, 1)
    return [jnp.where(lane % 4 == o, field, 0.0) for o in range(4)]


def early_body(select_ref, green_ref, image_ref, chosen_ref):
    rows = []
    for ref in (green_ref, image_ref):
        for s in range(2):
            rows += by_offset(ref[s])
    chosen_ref[...] = choose_rows(select_ref, jnp.concatenate(rows, axis=0))


def third_body(
    device_ref, got_ref, parts_ref, local_ref, modes_ref, right_ref, select_ref, sums_2_ref, sums_3_ref, terms_ref,
    early_ref,
    sent_ref, z_ref, assembled_ref,
):
    assemble_packed(got_ref, assembled_ref, 4)
    z = coarse_product(assembled_ref, parts_ref)
    z_ref[...] = z
    square = got_ref[3]
    for d in range(1, got_ref.shape[0] // 4):
        square = square + got_ref[4 * d + 3]
    y_0 = local_ref[0] + dot(z[:, :NC], modes_ref[0, NC:], NN)
    y_1 = local_ref[1] + dot(z, modes_ref[1], NN)
    y_2 = dot(z[:, NC:], right_ref[0, :NC], NN)
    rows = by_offset(y_0) + by_offset(y_1) + by_offset(y_2)
    rows.append(jnp.zeros((32, y_0.shape[1]), f32))
    late = choose_rows(select_ref, jnp.concatenate(rows, axis=0))
    curvature = jnp.sum(owned_terms(device_ref, assembled_ref, z), axis=1, keepdims=True)
    lane = lax.broadcasted_iota(jnp.int32, (8, LANES), 1)
    case = lax.broadcasted_iota(jnp.int32, (8, LANES), 0)
    parts = [
        sums_2_ref[:, 0:1],
        sums_2_ref[:, 1:2] + jnp.sum(terms_ref[...], axis=1, keepdims=True),
        sums_3_ref[:, 0:1],
        sums_3_ref[:, 1:2] + curvature,
    ]
    placed = jnp.zeros((8, LANES), f32)
    for k in range(4):
        placed = placed + jnp.where(lane == 96 + 8 * k + case, parts[k], 0.0)
    late = late + jnp.sum(placed, axis=0, keepdims=True)
    sent_ref[:, 0, 0, :] = early_ref[...]
    sent_ref[:, 0, 1, :] = late
    sent_ref[:, 1] = jnp.broadcast_to(square[None, 0:2], (late.shape[0], 2, LANES))
    sent_ref[:, 2] = jnp.broadcast_to(square[None, 2:4], (late.shape[0], 2, LANES))


def project_body(got_ref, basis_ref, part_ref, rows_ref, gains_ref):
    early, late = got_ref[:, 0, 0, :], got_ref[:, 0, 1, :]
    sums = jnp.broadcast_to(jnp.sum(late, axis=0, keepdims=True), (8, LANES))
    lane = lax.broadcasted_iota(jnp.int32, (8, LANES), 1)
    bb, bf, ff, fff = (pltpu.roll(sums, 32 - 8 * k, 1) for k in range(4))
    good = lane < 8
    bb, bf = jnp.where(good, bb, 1.0), jnp.where(good, bf, 1.0)
    ff, fff = jnp.where(good, ff, 2.0), jnp.where(good, fff, 8.0)
    alpha_0 = bb / bf
    norm_1 = bb - 2.0 * alpha_0 * bf + alpha_0 * alpha_0 * ff
    gain = 1.0 + norm_1 / bb
    curvature = gain * gain * bf - 2.0 * gain * alpha_0 * ff + alpha_0 * alpha_0 * fff
    alpha_1 = norm_1 / curvature
    kappas = []
    for kappa in (alpha_0 + alpha_1 * gain, alpha_1 * alpha_0):
        kappa = jnp.where(good, kappa, 0.0)
        for shift in (8, 16, 32, 64):
            kappa = kappa + pltpu.roll(kappa, shift, 1)
        kappas.append(kappa)
    gains_ref[0], gains_ref[1] = kappas[0], kappas[1]
    kappa_1, kappa_2 = kappas[0][:1], kappas[1][:1]
    wide = lax.broadcasted_iota(jnp.int32, late.shape, 1)
    extra = pltpu.roll(pltpu.roll(late, HALF, 1), 1, 0)
    last = late + jnp.where(wide < NC, extra, 0.0)
    rows = early - kappa_1 * pltpu.roll(early, HALF, 1) + kappa_2 * last
    turned = jnp.transpose(rows)
    snapshots = jnp.concatenate([turned[8 * j : 8 * j + 8] for j in range(8)], axis=1)
    rows_ref[...] = snapshots
    high, low = two_parts(snapshots)
    both = jnp.concatenate([high, low], axis=0)
    count = snapshots.shape[1]
    product = fast(both, basis_ref[:count], NN) + fast(both, basis_ref[count:], NN)
    gram = dot(snapshots, jnp.concatenate([snapshots, jnp.zeros((LANES - 8, count), f32)], axis=0), NT)
    part = jnp.concatenate([product[:8] + product[8:], gram], axis=1)
    for d in range(part_ref.shape[0]):
        part_ref[d] = part


def finish_body(got_ref, square_ref, basis_ref, rows_ref, columns_ref, projection_ref, factor_ref, *, scale):
    count = got_ref.shape[0]
    reduced = got_ref[0]
    for i in range(1, count):
        reduced = reduced + got_ref[i]
    rank = reduced.shape[1] - LANES
    coefficients = reduced[:, :rank]
    projection_ref[...] = coefficients
    low_rows, high_rows = coefficients[:, :LANES], coefficients[:, LANES:]
    squares = [square_ref[:, 1 + i // 2, i % 2, :] for i in range(4)]
    image = jnp.concatenate(
        [
            dot(low_rows, squares[0], NN) + dot(high_rows, squares[2], NN),
            dot(low_rows, squares[1], NN) + dot(high_rows, squares[3], NN),
        ],
        axis=1,
    )
    gap = image - 2.0 * coefficients
    blank = jnp.zeros((LANES - 8, rank), f32)
    gram = reduced[:, rank:] + dot(coefficients, jnp.concatenate([gap, blank], axis=0), NT)
    row = lax.broadcasted_iota(jnp.int32, (8, LANES), 0)
    lane = lax.broadcasted_iota(jnp.int32, (8, LANES), 1)
    gram = jnp.where(lane < 8, gram, 0.0)
    work = gram + jnp.where(lane == row + 8, 1.0, 0.0)
    upper = jnp.zeros((8, LANES), f32)
    for j in range(8):
        pivot = jnp.sum(jnp.where((row == j) & (lane == j), work, 0.0), axis=(0, 1), keepdims=True)
        line = jnp.sum(jnp.where(row == j, work, 0.0), axis=0, keepdims=True) / jnp.sqrt(pivot)
        upper = jnp.where(row == j, line, upper)
        column = jnp.sum(jnp.where(lane == j, work, 0.0), axis=1, keepdims=True) / jnp.sqrt(pivot)
        work = jnp.where(row > j, work - column * line, work)
    factor_ref[...] = jnp.where((lane >= row) & (lane < 8), upper, 0.0) * (1.0 / scale)
    inverse = pltpu.roll(upper, LANES - 8, 1)
    inverse = jnp.where((lane <= row) & (lane < 8), inverse, 0.0)[:, :8]
    high, low = two_parts(coefficients)
    total = rows_ref.shape[1]
    both = jnp.concatenate([high, low], axis=0)
    product = fast(both, basis_ref[:total], NT) + fast(both, basis_ref[total:], NT)
    remainder = rows_ref[...] - (product[:8] + product[8:])
    columns = dot(inverse, remainder, NN) * scale
    for t in range(8):
        index = 16 * t + lane // 8
        out = jnp.zeros((8, LANES), f32)
        for j in range(8):
            picked = jnp.take_along_axis(columns[:, j * LANES : (j + 1) * LANES], index, axis=1)
            out = jnp.where(lane % 8 == j, picked, out)
        columns_ref[:, t * LANES : (t + 1) * LANES] = out


def shards(
    rr_inverse,
    corner_modes,
    coarse_inverse,
    inertia,
    disp_now,
    vel_now,
    acc_now,
    load_next,
    basis_rows,
    piece_owner,
):
    case_count, _, unknowns = disp_now.shape
    devices = lax.axis_size(AXES)
    coarse_total = coarse_inverse.shape[1]
    rank = basis_rows.shape[1]
    last = unknowns - NI
    device = lax.axis_index(AXES).reshape(1).astype(jnp.int32)
    pair = ((2, case_count, unknowns),)
    z_shape = ((case_count, 2 * NC),)
    blocks_shape = ((case_count, 2 * LANES),)
    assembled = [pltpu.VMEM((case_count, coarse_total), f32)]

    start, right_side = call(start_body, [((devices, case_count, LANES),), pair], [SMEM] + [VMEM] * 6)(
        device, load_next, inertia, disp_now, vel_now, acc_now, corner_modes
    )
    got_1 = exchange(start)
    right_modes = shifted(corner_modes, -1)
    left_edge = shifted(corner_modes[1, :, last:], 1)
    coarse_parts, local_0 = call(pre_body, [((4 * NC, coarse_total), bf16), pair], [VMEM] * 3, flops=1 << 26)(
        coarse_inverse, right_side, rr_inverse
    )
    blocks_0, coupling, to_blocks = call(
        couple_body, [blocks_shape, ((2 * NC, 2 * LANES),), ((2 * LANES, 4 * NI),)], [SMEM] + [VMEM] * 4, flops=1 << 26
    )(device, corner_modes, right_modes, left_edge, local_0)

    def finish(local, z):
        mine, to_right, to_left = call(
            edge_body, [pair, ((case_count, 2 * NI),), ((case_count, NI),)], [VMEM] * 3, flops=1 << 20
        )(local, z, corner_modes)
        from_left = shifted(to_right, 1)
        from_right = shifted(to_left, -1)
        return call(join_body, [pair, pair, blocks_shape, ((case_count, LANES),)], [VMEM] * 8, flops=1 << 26)(
            mine, from_left, from_right, z, corner_modes, right_modes, rr_inverse, to_blocks
        )

    pieces, z_0 = call(first_body, [((3 * devices, 4, LANES),), z_shape], [VMEM] * 4, assembled, flops=1 << 24)(
        got_1, coarse_parts, coupling, blocks_0
    )
    got_2 = exchange(pieces)
    basis_parts, square, select = call(
        prep_body,
        [((2 * basis_rows.shape[0], rank), bf16), ((devices, 4, LANES),), ((devices, unknowns), bf16)],
        [VMEM, VMEM, VMEM],
        flops=1 << 26,
    )(basis_rows.reshape(devices, -1, rank), piece_owner.reshape(1, devices), z_0)
    green, local_1, blocks_1, sums_2 = finish(local_0, z_0)
    pieces, z_1, terms_1 = call(
        second_body, [((4 * devices, 4, LANES),), z_shape, z_shape], [SMEM] + [VMEM] * 5, assembled, flops=1 << 24
    )(device, got_2, coarse_parts, coupling, blocks_1, square)
    got_3 = exchange(pieces)
    image_1, local_2, _, sums_3 = finish(local_1, z_1)
    (early,) = call(early_body, [((devices, LANES),)], [VMEM] * 3, flops=1 << 24)(select, green, image_1)
    sent, z_2 = call(third_body, [((devices, 3, 2, LANES),), z_shape], [SMEM] + [VMEM] * 10, assembled, flops=1 << 24)(
        device, got_3, coarse_parts, local_2, corner_modes, right_modes, select, sums_2, sums_3, terms_1, early
    )
    got_4 = exchange(sent)
    ghost = shifted(z_2, 1)
    part, snapshots, gains = call(
        project_body,
        [
            ((lax.axis_size(NEAR), case_count, rank + LANES),),
            ((case_count, basis_rows.shape[0]),),
            ((2, case_count, LANES),),
        ],
        [VMEM] * 2,
        flops=1 << 24,
    )(got_4, basis_parts)
    near = exchange(part, NEAR)
    near = near.sum(axis=0)
    got_5 = to_everyone(near, FAR)
    disp_new, vel_new = call(
        out_body, [(disp_now.shape,), (disp_now.shape,)], [VMEM] * 10, flops=1 << 22
    )(green, image_1, local_2, z_2, ghost, corner_modes, gains, disp_now, vel_now, acc_now)
    scale = math.sqrt(basis_rows.shape[0] * devices)
    new_columns, projection, factor = call(
        functools.partial(finish_body, scale=scale),
        [((case_count, basis_rows.shape[0]),), ((case_count, rank),), ((case_count, LANES),)],
        [VMEM] * 4,
        flops=1 << 24,
    )(got_5, got_4, basis_parts, snapshots)
    return (disp_new, vel_new, projection.T, factor[:, :case_count], new_columns)


def solution(mesh):
    finer = Mesh(
        mesh.devices.reshape(4, 4, 2, mesh.shape["grp"]), ("sub_0", "sub_1", "sub_2", "grp")
    )
    placed = (
        P(AXES, None, None),
        P(AXES, None, None),
        P(AXES, None),
        P(AXES, None),
        P(None, AXES, None),
        P(None, AXES, None),
        P(None, AXES, None),
        P(None, AXES, None),
        P(AXES, None),
        P(),
    )

    return jax.shard_map(
        shards,
        mesh=finer,
        in_specs=placed,
        out_specs=(P(None, AXES, None), P(None, AXES, None), P(), P(), P(None, AXES)),
        check_vma=False,
    )
```

```python
import functools
import math

import jax
import jax.numpy as jnp
from jax import lax
from jax.experimental import pallas as pl
from jax.experimental.pallas import tpu as pltpu
from jax.sharding import Mesh
from jax.sharding import PartitionSpec as P

NC = 32
NI = 128
LANES = 128
HALF = 64
AXES = ("sub_0", "sub_1", "sub_2", "grp")
FAR, NEAR = ("sub_0", "sub_1"), ("sub_2", "grp")

highest = lax.Precision.HIGHEST
time_step = 0.5
newmark_beta = 0.25
newmark_gamma = 0.5
f32, bf16 = jnp.float32, jnp.bfloat16
NT = (((1,), (1,)), ((), ()))
NN = (((1,), (0,)), ((), ()))
VMEM = pl.BlockSpec(memory_space=pltpu.VMEM)
SMEM = pl.BlockSpec(memory_space=pltpu.SMEM)


def exchange(pieces, axes=AXES):
    return lax.all_to_all(pieces, axes, split_axis=0, concat_axis=0, tiled=True)


def to_everyone(array, axes=AXES):
    return exchange(jnp.broadcast_to(array, (lax.axis_size(axes), *array.shape)), axes)


def shifted(array, by):
    count = lax.axis_size(AXES)
    return lax.ppermute(array, AXES, [(i, (i + by) % count) for i in range(count)])


def dot(a, b, dims):
    return lax.dot_general(a, b, dims, precision=highest, preferred_element_type=f32)


def fast(a, b, dims):
    return lax.dot_general(a, b, dims, preferred_element_type=f32)


def call(body, outs, ins, scratch=(), flops=0, room=0):
    return pl.pallas_call(
        body,
        out_shape=[jax.ShapeDtypeStruct(shape, f32 if len(rest) == 0 else rest[0]) for shape, *rest in outs],
        in_specs=ins,
        out_specs=[VMEM] * len(outs),
        scratch_shapes=list(scratch),
        compiler_params=pltpu.CompilerParams(vmem_limit_bytes=(60 * 1024 - room) << 10),
        cost_estimate=pl.CostEstimate(flops=flops, bytes_accessed=1 << 20, transcendentals=0),
    )


def two_parts(x):
    high = x.astype(bf16)
    return high, (x - high.astype(f32)).astype(bf16)


def three_parts(x):
    high = x.astype(bf16)
    rest = x - high.astype(f32)
    middle = rest.astype(bf16)
    return high, middle, (rest - middle.astype(f32)).astype(bf16)


def start_body(device_ref, load_ref, inertia_ref, disp_ref, vel_ref, acc_ref, modes_ref, start_ref, right_ref):
    blank = jnp.zeros((NC, modes_ref.shape[2]), f32)
    fields = []
    for s in range(2):
        moved = disp_ref[:, s, :] + time_step * vel_ref[:, s, :]
        moved = moved + (0.5 - newmark_beta) * time_step * time_step * acc_ref[:, s, :]
        fields.append(load_ref[:, s, :] + inertia_ref[s : s + 1] * moved)
        right_ref[s] = fields[s]
    part_0 = jnp.concatenate([modes_ref[0, NC:], blank, blank, modes_ref[0, :NC]], axis=0)
    part_1 = jnp.concatenate([modes_ref[1, :NC], modes_ref[1, NC:], blank, blank], axis=0)
    blocks = dot(fields[0], part_0, NT) + dot(fields[1], part_1, NT)
    even = lax.rem(device_ref[0], 2) == 0
    blocks = jnp.where(even, blocks, pltpu.roll(blocks, HALF, 1))
    for d in range(start_ref.shape[0]):
        start_ref[d] = blocks


def pre_body(matrix_ref, right_ref, rr_ref, parts_ref, local_ref):
    rows = matrix_ref.shape[0]
    high, low = two_parts(matrix_ref[...])
    parts_ref[:rows] = high
    parts_ref[rows:] = low
    for s in range(2):
        local_ref[s] = dot(right_ref[s], rr_ref[s], NN)


def couple_body(device_ref, modes_ref, right_ref, left_ref, local_ref, blocks_ref, coupling_ref, to_blocks_ref):
    last = modes_ref.shape[2] - NI
    even = jnp.where(lax.rem(device_ref[0], 2) == 0, 1, 0)
    first, final = [modes_ref[s, :, :NI] for s in range(2)], [modes_ref[s, :, last:] for s in range(2)]
    right_first, right_final = [right_ref[s, :, :NI] for s in range(2)], right_ref[0, :, last:]
    left = left_ref[...]
    rows = [
        {0: left[:NC]},
        {0: left[NC:] - first[0][:NC], 1: final[0][:NC]},
        {0: -first[0][NC:], 1: final[0][NC:] - first[1][:NC], 2: final[1][:NC]},
        {1: -first[1][NC:], 2: final[1][NC:] - right_first[0][:NC], 3: right_final[:NC]},
        {2: -right_first[0][NC:], 3: right_final[NC:] - right_first[1][:NC]},
        {3: -right_first[1][NC:]},
    ]
    to_blocks_ref[...] = jnp.zeros(to_blocks_ref.shape, f32)
    for i, parts in enumerate(rows):
        at = pl.multiple_of(lax.rem(i * NC + 192 * even, 256), NC)
        for k, values in parts.items():
            to_blocks_ref[pl.ds(at, NC), k * NI : (k + 1) * NI] = values
    blank = jnp.zeros((NC, modes_ref.shape[2]), f32)
    unit_0 = jnp.concatenate([modes_ref[0, NC:], blank], axis=0)
    unit_1 = modes_ref[1]
    unit_2 = jnp.concatenate([blank, right_ref[0, :NC]], axis=0)
    jumps = jnp.concatenate(
        [-unit_0[:, :NI], unit_0[:, last:] - unit_1[:, :NI], unit_1[:, last:] - unit_2[:, :NI], unit_2[:, last:]], axis=1
    )
    coupling_ref[...] = dot(jumps, to_blocks_ref[...], NT)
    blocks_ref[...] = own_blocks(local_ref[0], local_ref[1], to_blocks_ref)


def own_blocks(field_0, field_1, to_blocks_ref):
    last = field_0.shape[1] - NI
    jumps = [-field_0[:, :NI], field_0[:, last:] - field_1[:, :NI], field_1[:, last:]]
    return dot(jnp.concatenate(jumps, axis=1), to_blocks_ref[:, : 3 * NI], NT)


def edge_body(local_ref, z_ref, modes_ref, mine_ref, to_right_ref, to_left_ref):
    last = local_ref.shape[2] - NI
    z = z_ref[...]
    mine_0 = local_ref[0] + dot(z[:, :NC], modes_ref[0, NC:], NN)
    mine_1 = local_ref[1] + dot(z, modes_ref[1], NN)
    mine_ref[0], mine_ref[1] = mine_0, mine_1
    to_left_ref[...] = mine_0[:, :NI]
    to_right_ref[:, :NI] = mine_1[:, last:]
    to_right_ref[:, NI:] = jnp.concatenate([z, z], axis=1)


def join_body(
    mine_ref, from_left_ref, from_right_ref, z_ref, modes_ref, right_ref, rr_ref, to_blocks_ref,
    field_ref, local_ref, blocks_ref, sums_ref,
):
    last = mine_ref.shape[2] - NI
    mine_1 = mine_ref[1]
    ghost = from_left_ref[:, NI : NI + 2 * NC]
    mine_0 = mine_ref[0] + dot(ghost[:, NC:], modes_ref[0, :NC], NN)
    field_ref[0], field_ref[1] = mine_0, mine_1
    jump_a = from_left_ref[:, :NI] - mine_0[:, :NI]
    jump_b = mine_0[:, last:] - mine_1[:, :NI]
    jump_c = mine_1[:, last:] - (from_right_ref[...] + dot(z_ref[:, NC:], right_ref[0, :NC, :NI], NN))
    inner = jnp.zeros((mine_1.shape[0], 1), f32)
    outs = []
    for s, (first, final) in enumerate([(-jump_a, jump_b), (-jump_b, jump_c)]):
        out = dot(first, rr_ref[s, :NI], NN) + dot(final, rr_ref[s, last:], NN)
        local_ref[s] = out
        inner = inner + jnp.sum(out[:, :NI] * first + out[:, last:] * final, axis=1, keepdims=True)
        outs.append(out)
    blocks_ref[...] = own_blocks(outs[0], outs[1], to_blocks_ref)
    square = jnp.sum(jump_b * jump_b + jump_c * jump_c, axis=1, keepdims=True)
    lane = lax.broadcasted_iota(jnp.int32, sums_ref.shape, 1)
    sums_ref[...] = jnp.where(lane == 0, square, 0.0) + jnp.where(lane == 1, inner, 0.0)


def prep_body(basis_ref, owner_ref, after_ref, parts_ref, square_ref, select_ref):
    devices, width, rank = basis_ref.shape
    total = devices * width
    square = jnp.zeros((rank, rank), f32)
    for j in range(width):
        rows = basis_ref[:, j, :]
        high, low = two_parts(rows)
        parts_ref[j * devices : (j + 1) * devices] = high
        parts_ref[total + j * devices : total + (j + 1) * devices] = low
        turned_high, turned_low = two_parts(jnp.transpose(rows))
        square = square + fast(turned_high, high, NN) + (fast(turned_high, low, NN) + fast(turned_low, high, NN))
    for i in range(4):
        r, h = i // 2, i % 2
        square_ref[:, i, :] = square[r * LANES : (r + 1) * LANES, h * LANES : (h + 1) * LANES]
    unknowns = select_ref.shape[1]
    rows = lax.broadcasted_iota(jnp.int32, (devices, unknowns), 0)
    columns = lax.broadcasted_iota(jnp.int32, (devices, unknowns), 1)
    each = unknowns // devices
    repeat = jnp.where(columns // each == rows, 1.0, 0.0).astype(bf16)
    owner = jnp.broadcast_to(owner_ref[...].astype(f32), (8, devices)).astype(bf16)
    owner = fast(owner, repeat, NN)[:1]
    select_ref[...] = jnp.where(owner == rows.astype(f32), 1.0, 0.0).astype(bf16)


def late_body(local_ref, z_ref, modes_ref, late_ref, to_right_ref):
    z = z_ref[...]
    late_ref[0] = local_ref[0] + dot(z[:, :NC], modes_ref[0, NC:], NN)
    late_ref[1] = local_ref[1] + dot(z, modes_ref[1], NN)
    to_right_ref[...] = jnp.concatenate([z, z], axis=1)


def out_body(
    green_ref, image_ref, late_ref, ghost_ref, modes_ref, gains_ref, disp_ref, vel_ref, acc_ref, disp_out_ref, vel_out_ref
):
    kappa_1, kappa_2 = gains_ref[0], gains_ref[1]
    case = lax.broadcasted_iota(jnp.int32, kappa_1.shape, 0)
    lane = lax.broadcasted_iota(jnp.int32, kappa_1.shape, 1)
    kappa_1 = jnp.sum(jnp.where(case == lane, kappa_1, 0.0), axis=1, keepdims=True)
    kappa_2 = jnp.sum(jnp.where(case == lane, kappa_2, 0.0), axis=1, keepdims=True)
    late = [late_ref[0] + dot(ghost_ref[:, NC : 2 * NC], modes_ref[0, :NC], NN), late_ref[1]]
    for s in range(2):
        disp = green_ref[s] - kappa_1 * image_ref[s] + kappa_2 * late[s]
        vel, acc = vel_ref[:, s, :], acc_ref[:, s, :]
        accel = (
            (disp - disp_ref[:, s, :]) * (1.0 / (newmark_beta * time_step * time_step))
            - vel * (1.0 / (newmark_beta * time_step))
            - (0.5 / newmark_beta - 1.0) * acc
        )
        disp_out_ref[:, s, :] = disp
        vel_out_ref[:, s, :] = vel + time_step * ((1.0 - newmark_gamma) * acc + newmark_gamma * accel)


def coarse_product(assembled_ref, parts_ref):
    cases = assembled_ref.shape[0]
    high, low = two_parts(assembled_ref[...])
    both = fast(jnp.concatenate([high, low], axis=0), parts_ref[...], NT)
    both = both[:cases] + both[cases:]
    return both[:, :HALF] + both[:, HALF:]


def assemble_packed(got_ref, assembled_ref, slots):
    tiles = assembled_ref.shape[1] // LANES
    lane = lax.broadcasted_iota(jnp.int32, (4, LANES), 1)
    lower = lane < HALF
    for m in range(tiles):
        even, odd = 2 * slots * m, 2 * slots * m + slots
        following = 2 * slots * ((m + 1) % tiles) + 2
        previous = 2 * slots * ((m - 1) % tiles) + slots + 2
        extra_even, extra_odd = got_ref[following], got_ref[previous]
        top = got_ref[even] + got_ref[odd] + jnp.where(lower, extra_odd, extra_even)
        turned = pltpu.roll(jnp.where(lower, extra_even, extra_odd), HALF, 1)
        bottom = got_ref[even + 1] + got_ref[odd + 1] + turned
        assembled_ref[0:4, m * LANES : (m + 1) * LANES] = top
        assembled_ref[4:8, m * LANES : (m + 1) * LANES] = bottom


def assemble_first(got_ref, assembled_ref):
    tiles = assembled_ref.shape[1] // LANES
    lane = lax.broadcasted_iota(jnp.int32, (8, LANES), 1)
    for m in range(tiles):
        following = (2 * m + 2) % (2 * tiles)
        own = got_ref[2 * m + 1] + jnp.where(lane < HALF, got_ref[2 * m], 0.0)
        assembled_ref[:, m * LANES : (m + 1) * LANES] = own + jnp.where(
            lane >= LANES - NC, got_ref[following], 0.0
        )


def owned_terms(device_ref, assembled_ref, z):
    device = device_ref[0]
    tile = assembled_ref[:, pl.ds(pl.multiple_of((device // 2) * LANES, LANES), LANES)]
    even = lax.rem(device, 2) == 0
    return jnp.where(even, tile[:, :HALF], tile[:, HALF:]) * z


def send_blocks(z, coupling_ref, local_ref, pieces_ref, slots, riding_ref=None):
    blocks = local_ref[...] + dot(z, coupling_ref[...], NN)
    main, extra = blocks[:, :LANES], blocks[:, LANES:]
    turned = pltpu.roll(extra, HALF, 1)
    packed = extra[0:4] + turned[4:8]
    for d in range(pieces_ref.shape[0] // slots):
        pieces_ref[slots * d] = main[0:4]
        pieces_ref[slots * d + 1] = main[4:8]
        pieces_ref[slots * d + 2] = packed
        if riding_ref is not None:
            pieces_ref[slots * d + 3] = riding_ref[d]


def first_body(got_ref, parts_ref, coupling_ref, local_ref, pieces_ref, z_ref, assembled_ref):
    assemble_first(got_ref, assembled_ref)
    z = coarse_product(assembled_ref, parts_ref)
    z_ref[...] = z
    send_blocks(z, coupling_ref, local_ref, pieces_ref, 3)


def second_body(
    device_ref, got_ref, parts_ref, coupling_ref, local_ref, square_ref, pieces_ref, z_ref, terms_ref, assembled_ref
):
    assemble_packed(got_ref, assembled_ref, 3)
    z = coarse_product(assembled_ref, parts_ref)
    z_ref[...] = z
    terms_ref[...] = owned_terms(device_ref, assembled_ref, z)
    send_blocks(z, coupling_ref, local_ref, pieces_ref, 4, square_ref)


def choose_rows(select_ref, rows):
    high, middle, low = three_parts(rows)
    select = select_ref[...]
    return fast(select, high, NT) + fast(select, middle, NT) + fast(select, low, NT)


def by_offset(field):
    lane = lax.broadcasted_iota(jnp.int32, field.shape, 1)
    return [jnp.where(lane % 4 == o, field, 0.0) for o in range(4)]


def early_body(select_ref, green_ref, image_ref, chosen_ref):
    rows = []
    for ref in (green_ref, image_ref):
        for s in range(2):
            rows += by_offset(ref[s])
    chosen_ref[...] = choose_rows(select_ref, jnp.concatenate(rows, axis=0))


def third_body(
    device_ref, got_ref, parts_ref, local_ref, modes_ref, right_ref, select_ref, sums_2_ref, sums_3_ref, terms_ref,
    early_ref,
    sent_ref, z_ref, assembled_ref,
):
    assemble_packed(got_ref, assembled_ref, 4)
    z = coarse_product(assembled_ref, parts_ref)
    z_ref[...] = z
    square = got_ref[3]
    for d in range(1, got_ref.shape[0] // 4):
        square = square + got_ref[4 * d + 3]
    y_0 = local_ref[0] + dot(z[:, :NC], modes_ref[0, NC:], NN)
    y_1 = local_ref[1] + dot(z, modes_ref[1], NN)
    y_2 = dot(z[:, NC:], right_ref[0, :NC], NN)
    rows = by_offset(y_0) + by_offset(y_1) + by_offset(y_2)
    rows.append(jnp.zeros((32, y_0.shape[1]), f32))
    late = choose_rows(select_ref, jnp.concatenate(rows, axis=0))
    curvature = jnp.sum(owned_terms(device_ref, assembled_ref, z), axis=1, keepdims=True)
    lane = lax.broadcasted_iota(jnp.int32, (8, LANES), 1)
    case = lax.broadcasted_iota(jnp.int32, (8, LANES), 0)
    parts = [
        sums_2_ref[:, 0:1],
        sums_2_ref[:, 1:2] + jnp.sum(terms_ref[...], axis=1, keepdims=True),
        sums_3_ref[:, 0:1],
        sums_3_ref[:, 1:2] + curvature,
    ]
    placed = jnp.zeros((8, LANES), f32)
    for k in range(4):
        placed = placed + jnp.where(lane == 96 + 8 * k + case, parts[k], 0.0)
    late = late + jnp.sum(placed, axis=0, keepdims=True)
    sent_ref[:, 0, 0, :] = early_ref[...]
    sent_ref[:, 0, 1, :] = late
    sent_ref[:, 1] = jnp.broadcast_to(square[None, 0:2], (late.shape[0], 2, LANES))
    sent_ref[:, 2] = jnp.broadcast_to(square[None, 2:4], (late.shape[0], 2, LANES))


def project_body(got_ref, basis_ref, part_ref, rows_ref, gains_ref):
    early, late = got_ref[:, 0, 0, :], got_ref[:, 0, 1, :]
    sums = jnp.broadcast_to(jnp.sum(late, axis=0, keepdims=True), (8, LANES))
    lane = lax.broadcasted_iota(jnp.int32, (8, LANES), 1)
    bb, bf, ff, fff = (pltpu.roll(sums, 32 - 8 * k, 1) for k in range(4))
    good = lane < 8
    bb, bf = jnp.where(good, bb, 1.0), jnp.where(good, bf, 1.0)
    ff, fff = jnp.where(good, ff, 2.0), jnp.where(good, fff, 8.0)
    alpha_0 = bb / bf
    norm_1 = bb - 2.0 * alpha_0 * bf + alpha_0 * alpha_0 * ff
    gain = 1.0 + norm_1 / bb
    curvature = gain * gain * bf - 2.0 * gain * alpha_0 * ff + alpha_0 * alpha_0 * fff
    alpha_1 = norm_1 / curvature
    kappas = []
    for kappa in (alpha_0 + alpha_1 * gain, alpha_1 * alpha_0):
        kappa = jnp.where(good, kappa, 0.0)
        for shift in (8, 16, 32, 64):
            kappa = kappa + pltpu.roll(kappa, shift, 1)
        kappas.append(kappa)
    gains_ref[0], gains_ref[1] = kappas[0], kappas[1]
    kappa_1, kappa_2 = kappas[0][:1], kappas[1][:1]
    wide = lax.broadcasted_iota(jnp.int32, late.shape, 1)
    extra = pltpu.roll(pltpu.roll(late, HALF, 1), 1, 0)
    last = late + jnp.where(wide < NC, extra, 0.0)
    rows = early - kappa_1 * pltpu.roll(early, HALF, 1) + kappa_2 * last
    turned = jnp.transpose(rows)
    snapshots = jnp.concatenate([turned[8 * j : 8 * j + 8] for j in range(8)], axis=1)
    rows_ref[...] = snapshots
    high, low = two_parts(snapshots)
    both = jnp.concatenate([high, low], axis=0)
    count = snapshots.shape[1]
    product = fast(both, basis_ref[:count], NN) + fast(both, basis_ref[count:], NN)
    gram = dot(snapshots, jnp.concatenate([snapshots, jnp.zeros((LANES - 8, count), f32)], axis=0), NT)
    part = jnp.concatenate([product[:8] + product[8:], gram], axis=1)
    for d in range(part_ref.shape[0]):
        part_ref[d] = part


def finish_body(got_ref, square_ref, basis_ref, rows_ref, columns_ref, projection_ref, factor_ref, *, scale):
    count = got_ref.shape[0]
    reduced = got_ref[0]
    for i in range(1, count):
        reduced = reduced + got_ref[i]
    rank = reduced.shape[1] - LANES
    coefficients = reduced[:, :rank]
    projection_ref[...] = coefficients
    low_rows, high_rows = coefficients[:, :LANES], coefficients[:, LANES:]
    squares = [square_ref[:, 1 + i // 2, i % 2, :] for i in range(4)]
    image = jnp.concatenate(
        [
            dot(low_rows, squares[0], NN) + dot(high_rows, squares[2], NN),
            dot(low_rows, squares[1], NN) + dot(high_rows, squares[3], NN),
        ],
        axis=1,
    )
    gap = image - 2.0 * coefficients
    blank = jnp.zeros((LANES - 8, rank), f32)
    gram = reduced[:, rank:] + dot(coefficients, jnp.concatenate([gap, blank], axis=0), NT)
    row = lax.broadcasted_iota(jnp.int32, (8, LANES), 0)
    lane = lax.broadcasted_iota(jnp.int32, (8, LANES), 1)
    gram = jnp.where(lane < 8, gram, 0.0)
    work = gram + jnp.where(lane == row + 8, 1.0, 0.0)
    upper = jnp.zeros((8, LANES), f32)
    for j in range(8):
        pivot = jnp.sum(jnp.where((row == j) & (lane == j), work, 0.0), axis=(0, 1), keepdims=True)
        line = jnp.sum(jnp.where(row == j, work, 0.0), axis=0, keepdims=True) / jnp.sqrt(pivot)
        upper = jnp.where(row == j, line, upper)
        column = jnp.sum(jnp.where(lane == j, work, 0.0), axis=1, keepdims=True) / jnp.sqrt(pivot)
        work = jnp.where(row > j, work - column * line, work)
    factor_ref[...] = jnp.where((lane >= row) & (lane < 8), upper, 0.0) * (1.0 / scale)
    inverse = pltpu.roll(upper, LANES - 8, 1)
    inverse = jnp.where((lane <= row) & (lane < 8), inverse, 0.0)[:, :8]
    high, low = two_parts(coefficients)
    total = rows_ref.shape[1]
    both = jnp.concatenate([high, low], axis=0)
    product = fast(both, basis_ref[:total], NT) + fast(both, basis_ref[total:], NT)
    remainder = rows_ref[...] - (product[:8] + product[8:])
    columns = dot(inverse, remainder, NN) * scale
    for t in range(8):
        index = 16 * t + lane // 8
        out = jnp.zeros((8, LANES), f32)
        for j in range(8):
            picked = jnp.take_along_axis(columns[:, j * LANES : (j + 1) * LANES], index, axis=1)
            out = jnp.where(lane % 8 == j, picked, out)
        columns_ref[:, t * LANES : (t + 1) * LANES] = out


def shards(
    rr_inverse,
    corner_modes,
    coarse_inverse,
    inertia,
    disp_now,
    vel_now,
    acc_now,
    load_next,
    basis_rows,
    piece_owner,
):
    case_count, _, unknowns = disp_now.shape
    devices = lax.axis_size(AXES)
    coarse_total = coarse_inverse.shape[1]
    rank = basis_rows.shape[1]
    last = unknowns - NI
    device = lax.axis_index(AXES).reshape(1).astype(jnp.int32)
    pair = ((2, case_count, unknowns),)
    z_shape = ((case_count, 2 * NC),)
    blocks_shape = ((case_count, 2 * LANES),)
    assembled = [pltpu.VMEM((case_count, coarse_total), f32)]

    start, right_side = call(start_body, [((devices, case_count, LANES),), pair], [SMEM] + [VMEM] * 6)(
        device, load_next, inertia, disp_now, vel_now, acc_now, corner_modes
    )
    got_1 = exchange(start)
    right_modes = shifted(corner_modes, -1)
    left_edge = shifted(corner_modes[1, :, last:], 1)
    coarse_parts, local_0 = call(pre_body, [((4 * NC, coarse_total), bf16), pair], [VMEM] * 3, flops=1 << 26)(
        coarse_inverse, right_side, rr_inverse
    )
    blocks_0, coupling, to_blocks = call(
        couple_body, [blocks_shape, ((2 * NC, 2 * LANES),), ((2 * LANES, 4 * NI),)], [SMEM] + [VMEM] * 4, flops=1 << 26, room=296
    )(device, corner_modes, right_modes, left_edge, local_0)

    def finish(local, z):
        mine, to_right, to_left = call(
            edge_body, [pair, ((case_count, 2 * NI),), ((case_count, NI),)], [VMEM] * 3, flops=1 << 20, room=16
        )(local, z, corner_modes)
        from_left = shifted(to_right, 1)
        from_right = shifted(to_left, -1)
        return call(join_body, [pair, pair, blocks_shape, ((case_count, LANES),)], [VMEM] * 8, flops=1 << 26, room=16)(
            mine, from_left, from_right, z, corner_modes, right_modes, rr_inverse, to_blocks
        )

    pieces, z_0 = call(first_body, [((3 * devices, 4, LANES),), z_shape], [VMEM] * 4, assembled, flops=1 << 24, room=516)(
        got_1, coarse_parts, coupling, blocks_0
    )
    got_2 = exchange(pieces)
    basis_parts, square, select = call(
        prep_body,
        [((2 * basis_rows.shape[0], rank), bf16), ((devices, 4, LANES),), ((devices, unknowns), bf16)],
        [VMEM, VMEM, VMEM],
        flops=1 << 26,
    )(basis_rows.reshape(devices, -1, rank), piece_owner.reshape(1, devices), z_0)
    green, local_1, blocks_1, sums_2 = finish(local_0, z_0)
    pieces, z_1, terms_1 = call(
        second_body, [((4 * devices, 4, LANES),), z_shape, z_shape], [SMEM] + [VMEM] * 5, assembled, flops=1 << 24, room=772
    )(device, got_2, coarse_parts, coupling, blocks_1, square)
    got_3 = exchange(pieces)
    image_1, local_2, _, sums_3 = finish(local_1, z_1)
    (early,) = call(early_body, [((devices, LANES),)], [VMEM] * 3, flops=1 << 24)(select, green, image_1)
    sent, z_2 = call(third_body, [((devices, 3, 2, LANES),), z_shape], [SMEM] + [VMEM] * 10, assembled, flops=1 << 24, room=1028)(
        device, got_3, coarse_parts, local_2, corner_modes, right_modes, select, sums_2, sums_3, terms_1, early
    )
    got_4 = exchange(sent)
    late, to_right = call(late_body, [pair, ((case_count, LANES),)], [VMEM] * 3, flops=1 << 20)(
        local_2, z_2, corner_modes
    )
    ghost = shifted(to_right, 1)
    part, snapshots, gains = call(
        project_body,
        [
            ((lax.axis_size(NEAR), case_count, rank + LANES),),
            ((case_count, basis_rows.shape[0]),),
            ((2, case_count, LANES),),
        ],
        [VMEM] * 2,
        flops=1 << 24,
        room=388,
    )(got_4, basis_parts)
    near = exchange(part, NEAR)
    near = near.sum(axis=0)
    got_5 = to_everyone(near, FAR)
    disp_new, vel_new = call(
        out_body, [(disp_now.shape,), (disp_now.shape,)], [VMEM] * 9, flops=1 << 22, room=8
    )(green, image_1, late, ghost, corner_modes, gains, disp_now, vel_now, acc_now)
    scale = math.sqrt(basis_rows.shape[0] * devices)
    new_columns, projection, factor = call(
        functools.partial(finish_body, scale=scale),
        [((case_count, basis_rows.shape[0]),), ((case_count, rank),), ((case_count, LANES),)],
        [VMEM] * 4,
        flops=1 << 24,
        room=196,
    )(got_5, got_4, basis_parts, snapshots)
    return (disp_new, vel_new, projection.T, factor[:, :case_count], new_columns)


def solution(mesh):
    finer = Mesh(
        mesh.devices.reshape(4, 4, 2, mesh.shape["grp"]), ("sub_0", "sub_1", "sub_2", "grp")
    )
    placed = (
        P(AXES, None, None),
        P(AXES, None, None),
        P(AXES, None),
        P(AXES, None),
        P(None, AXES, None),
        P(None, AXES, None),
        P(None, AXES, None),
        P(None, AXES, None),
        P(AXES, None),
        P(),
    )

    return jax.shard_map(
        shards,
        mesh=finer,
        in_specs=placed,
        out_specs=(P(None, AXES, None), P(None, AXES, None), P(), P(), P(None, AXES)),
        check_vma=False,
    )
```

```python
import functools
import math

import jax
import jax.numpy as jnp
from jax import lax
from jax.experimental import pallas as pl
from jax.experimental.pallas import tpu as pltpu
from jax.sharding import Mesh
from jax.sharding import PartitionSpec as P

NC = 32
NI = 128
LANES = 128
HALF = 64
AXES = ("sub_0", "sub_1", "sub_2", "grp")
FAR, NEAR = ("sub_0", "sub_1"), ("sub_2", "grp")

highest = lax.Precision.HIGHEST
time_step = 0.5
newmark_beta = 0.25
newmark_gamma = 0.5
f32, bf16 = jnp.float32, jnp.bfloat16
NT = (((1,), (1,)), ((), ()))
NN = (((1,), (0,)), ((), ()))
VMEM = pl.BlockSpec(memory_space=pltpu.VMEM)
SMEM = pl.BlockSpec(memory_space=pltpu.SMEM)


def exchange(pieces, axes=AXES):
    return lax.all_to_all(pieces, axes, split_axis=0, concat_axis=0, tiled=True)


def to_everyone(array, axes=AXES):
    return exchange(jnp.broadcast_to(array, (lax.axis_size(axes), *array.shape)), axes)


def shifted(array, by):
    count = lax.axis_size(AXES)
    return lax.ppermute(array, AXES, [(i, (i + by) % count) for i in range(count)])


def dot(a, b, dims):
    return lax.dot_general(a, b, dims, precision=highest, preferred_element_type=f32)


def fast(a, b, dims):
    return lax.dot_general(a, b, dims, preferred_element_type=f32)


def call(body, outs, ins, scratch=(), flops=0, grant=16000):
    return pl.pallas_call(
        body,
        out_shape=[jax.ShapeDtypeStruct(shape, f32 if len(rest) == 0 else rest[0]) for shape, *rest in outs],
        in_specs=ins,
        out_specs=[VMEM] * len(outs),
        scratch_shapes=list(scratch),
        compiler_params=pltpu.CompilerParams(vmem_limit_bytes=grant << 10),
        cost_estimate=pl.CostEstimate(flops=flops, bytes_accessed=1 << 20, transcendentals=0),
    )


def two_parts(x):
    high = x.astype(bf16)
    return high, (x - high.astype(f32)).astype(bf16)


def three_parts(x):
    high = x.astype(bf16)
    rest = x - high.astype(f32)
    middle = rest.astype(bf16)
    return high, middle, (rest - middle.astype(f32)).astype(bf16)


def start_body(device_ref, load_ref, inertia_ref, disp_ref, vel_ref, acc_ref, modes_ref, start_ref, right_ref):
    blank = jnp.zeros((NC, modes_ref.shape[2]), f32)
    fields = []
    for s in range(2):
        moved = disp_ref[:, s, :] + time_step * vel_ref[:, s, :]
        moved = moved + (0.5 - newmark_beta) * time_step * time_step * acc_ref[:, s, :]
        fields.append(load_ref[:, s, :] + inertia_ref[s : s + 1] * moved)
        right_ref[s] = fields[s]
    part_0 = jnp.concatenate([modes_ref[0, NC:], blank, blank, modes_ref[0, :NC]], axis=0)
    part_1 = jnp.concatenate([modes_ref[1, :NC], modes_ref[1, NC:], blank, blank], axis=0)
    blocks = dot(fields[0], part_0, NT) + dot(fields[1], part_1, NT)
    even = lax.rem(device_ref[0], 2) == 0
    blocks = jnp.where(even, blocks, pltpu.roll(blocks, HALF, 1))
    for d in range(start_ref.shape[0]):
        start_ref[d] = blocks


def pre_body(matrix_ref, right_ref, rr_ref, parts_ref, local_ref):
    rows = matrix_ref.shape[0]
    high, low = two_parts(matrix_ref[...])
    parts_ref[:rows] = high
    parts_ref[rows:] = low
    for s in range(2):
        local_ref[s] = dot(right_ref[s], rr_ref[s], NN)


def couple_body(device_ref, modes_ref, right_ref, left_ref, local_ref, blocks_ref, coupling_ref, to_blocks_ref):
    last = modes_ref.shape[2] - NI
    even = jnp.where(lax.rem(device_ref[0], 2) == 0, 1, 0)
    first, final = [modes_ref[s, :, :NI] for s in range(2)], [modes_ref[s, :, last:] for s in range(2)]
    right_first, right_final = [right_ref[s, :, :NI] for s in range(2)], right_ref[0, :, last:]
    left = left_ref[...]
    rows = [
        {0: left[:NC]},
        {0: left[NC:] - first[0][:NC], 1: final[0][:NC]},
        {0: -first[0][NC:], 1: final[0][NC:] - first[1][:NC], 2: final[1][:NC]},
        {1: -first[1][NC:], 2: final[1][NC:] - right_first[0][:NC], 3: right_final[:NC]},
        {2: -right_first[0][NC:], 3: right_final[NC:] - right_first[1][:NC]},
        {3: -right_first[1][NC:]},
    ]
    to_blocks_ref[...] = jnp.zeros(to_blocks_ref.shape, f32)
    for i, parts in enumerate(rows):
        at = pl.multiple_of(lax.rem(i * NC + 192 * even, 256), NC)
        for k, values in parts.items():
            to_blocks_ref[pl.ds(at, NC), k * NI : (k + 1) * NI] = values
    blank = jnp.zeros((NC, modes_ref.shape[2]), f32)
    unit_0 = jnp.concatenate([modes_ref[0, NC:], blank], axis=0)
    unit_1 = modes_ref[1]
    unit_2 = jnp.concatenate([blank, right_ref[0, :NC]], axis=0)
    jumps = jnp.concatenate(
        [-unit_0[:, :NI], unit_0[:, last:] - unit_1[:, :NI], unit_1[:, last:] - unit_2[:, :NI], unit_2[:, last:]], axis=1
    )
    coupling_ref[...] = dot(jumps, to_blocks_ref[...], NT)
    blocks_ref[...] = own_blocks(local_ref[0], local_ref[1], to_blocks_ref)


def own_blocks(field_0, field_1, to_blocks_ref):
    last = field_0.shape[1] - NI
    jumps = [-field_0[:, :NI], field_0[:, last:] - field_1[:, :NI], field_1[:, last:]]
    return dot(jnp.concatenate(jumps, axis=1), to_blocks_ref[:, : 3 * NI], NT)


def edge_body(local_ref, z_ref, modes_ref, mine_ref, to_right_ref, to_left_ref):
    last = local_ref.shape[2] - NI
    z = z_ref[...]
    mine_0 = local_ref[0] + dot(z[:, :NC], modes_ref[0, NC:], NN)
    mine_1 = local_ref[1] + dot(z, modes_ref[1], NN)
    mine_ref[0], mine_ref[1] = mine_0, mine_1
    to_left_ref[...] = mine_0[:, :NI]
    to_right_ref[:, :NI] = mine_1[:, last:]
    to_right_ref[:, NI:] = jnp.concatenate([z, z], axis=1)


def join_body(
    mine_ref, from_left_ref, from_right_ref, z_ref, modes_ref, right_ref, rr_ref, to_blocks_ref,
    field_ref, local_ref, blocks_ref, sums_ref,
):
    last = mine_ref.shape[2] - NI
    mine_1 = mine_ref[1]
    ghost = from_left_ref[:, NI : NI + 2 * NC]
    mine_0 = mine_ref[0] + dot(ghost[:, NC:], modes_ref[0, :NC], NN)
    field_ref[0], field_ref[1] = mine_0, mine_1
    jump_a = from_left_ref[:, :NI] - mine_0[:, :NI]
    jump_b = mine_0[:, last:] - mine_1[:, :NI]
    jump_c = mine_1[:, last:] - (from_right_ref[...] + dot(z_ref[:, NC:], right_ref[0, :NC, :NI], NN))
    inner = jnp.zeros((mine_1.shape[0], 1), f32)
    outs = []
    for s, (first, final) in enumerate([(-jump_a, jump_b), (-jump_b, jump_c)]):
        out = dot(first, rr_ref[s, :NI], NN) + dot(final, rr_ref[s, last:], NN)
        local_ref[s] = out
        inner = inner + jnp.sum(out[:, :NI] * first + out[:, last:] * final, axis=1, keepdims=True)
        outs.append(out)
    blocks_ref[...] = own_blocks(outs[0], outs[1], to_blocks_ref)
    square = jnp.sum(jump_b * jump_b + jump_c * jump_c, axis=1, keepdims=True)
    lane = lax.broadcasted_iota(jnp.int32, sums_ref.shape, 1)
    sums_ref[...] = jnp.where(lane == 0, square, 0.0) + jnp.where(lane == 1, inner, 0.0)


def prep_body(basis_ref, owner_ref, after_ref, parts_ref, square_ref, select_ref):
    devices, width, rank = basis_ref.shape
    total = devices * width
    square = jnp.zeros((rank, rank), f32)
    for j in range(width):
        rows = basis_ref[:, j, :]
        high, low = two_parts(rows)
        parts_ref[j * devices : (j + 1) * devices] = high
        parts_ref[total + j * devices : total + (j + 1) * devices] = low
        turned_high, turned_low = two_parts(jnp.transpose(rows))
        square = square + fast(turned_high, high, NN) + (fast(turned_high, low, NN) + fast(turned_low, high, NN))
    for i in range(4):
        r, h = i // 2, i % 2
        square_ref[:, i, :] = square[r * LANES : (r + 1) * LANES, h * LANES : (h + 1) * LANES]
    unknowns = select_ref.shape[1]
    rows = lax.broadcasted_iota(jnp.int32, (devices, unknowns), 0)
    columns = lax.broadcasted_iota(jnp.int32, (devices, unknowns), 1)
    each = unknowns // devices
    repeat = jnp.where(columns // each == rows, 1.0, 0.0).astype(bf16)
    owner = jnp.broadcast_to(owner_ref[...].astype(f32), (8, devices)).astype(bf16)
    owner = fast(owner, repeat, NN)[:1]
    select_ref[...] = jnp.where(owner == rows.astype(f32), 1.0, 0.0).astype(bf16)


def late_body(local_ref, z_ref, ghost_ref, modes_ref, late_ref):
    z = z_ref[...]
    ghost = ghost_ref[...][:, NC:]
    late_ref[0] = local_ref[0] + dot(z[:, :NC], modes_ref[0, NC:], NN) + dot(ghost, modes_ref[0, :NC], NN)
    late_ref[1] = local_ref[1] + dot(z, modes_ref[1], NN)


def out_body(
    green_ref, image_ref, late_ref, gains_ref, disp_ref, vel_ref, acc_ref, disp_out_ref, vel_out_ref
):
    kappa_1, kappa_2 = gains_ref[0], gains_ref[1]
    case = lax.broadcasted_iota(jnp.int32, kappa_1.shape, 0)
    lane = lax.broadcasted_iota(jnp.int32, kappa_1.shape, 1)
    kappa_1 = jnp.sum(jnp.where(case == lane, kappa_1, 0.0), axis=1, keepdims=True)
    kappa_2 = jnp.sum(jnp.where(case == lane, kappa_2, 0.0), axis=1, keepdims=True)
    for s in range(2):
        disp = green_ref[s] - kappa_1 * image_ref[s] + kappa_2 * late_ref[s]
        vel, acc = vel_ref[:, s, :], acc_ref[:, s, :]
        accel = (
            (disp - disp_ref[:, s, :]) * (1.0 / (newmark_beta * time_step * time_step))
            - vel * (1.0 / (newmark_beta * time_step))
            - (0.5 / newmark_beta - 1.0) * acc
        )
        disp_out_ref[:, s, :] = disp
        vel_out_ref[:, s, :] = vel + time_step * ((1.0 - newmark_gamma) * acc + newmark_gamma * accel)


def coarse_product(assembled_ref, parts_ref):
    cases = assembled_ref.shape[0]
    high, low = two_parts(assembled_ref[...])
    both = fast(jnp.concatenate([high, low], axis=0), parts_ref[...], NT)
    both = both[:cases] + both[cases:]
    return both[:, :HALF] + both[:, HALF:]


def assemble_packed(got_ref, assembled_ref, slots):
    tiles = assembled_ref.shape[1] // LANES
    lane = lax.broadcasted_iota(jnp.int32, (4, LANES), 1)
    lower = lane < HALF
    for m in range(tiles):
        even, odd = 2 * slots * m, 2 * slots * m + slots
        following = 2 * slots * ((m + 1) % tiles) + 2
        previous = 2 * slots * ((m - 1) % tiles) + slots + 2
        extra_even, extra_odd = got_ref[following], got_ref[previous]
        top = got_ref[even] + got_ref[odd] + jnp.where(lower, extra_odd, extra_even)
        turned = pltpu.roll(jnp.where(lower, extra_even, extra_odd), HALF, 1)
        bottom = got_ref[even + 1] + got_ref[odd + 1] + turned
        assembled_ref[0:4, m * LANES : (m + 1) * LANES] = top
        assembled_ref[4:8, m * LANES : (m + 1) * LANES] = bottom


def assemble_first(got_ref, assembled_ref):
    tiles = assembled_ref.shape[1] // LANES
    lane = lax.broadcasted_iota(jnp.int32, (8, LANES), 1)
    for m in range(tiles):
        following = (2 * m + 2) % (2 * tiles)
        own = got_ref[2 * m + 1] + jnp.where(lane < HALF, got_ref[2 * m], 0.0)
        assembled_ref[:, m * LANES : (m + 1) * LANES] = own + jnp.where(
            lane >= LANES - NC, got_ref[following], 0.0
        )


def owned_terms(device_ref, assembled_ref, z):
    device = device_ref[0]
    tile = assembled_ref[:, pl.ds(pl.multiple_of((device // 2) * LANES, LANES), LANES)]
    even = lax.rem(device, 2) == 0
    return jnp.where(even, tile[:, :HALF], tile[:, HALF:]) * z


def send_blocks(z, coupling_ref, local_ref, pieces_ref, slots, riding_ref=None):
    blocks = local_ref[...] + dot(z, coupling_ref[...], NN)
    main, extra = blocks[:, :LANES], blocks[:, LANES:]
    turned = pltpu.roll(extra, HALF, 1)
    packed = extra[0:4] + turned[4:8]
    for d in range(pieces_ref.shape[0] // slots):
        pieces_ref[slots * d] = main[0:4]
        pieces_ref[slots * d + 1] = main[4:8]
        pieces_ref[slots * d + 2] = packed
        if riding_ref is not None:
            pieces_ref[slots * d + 3] = riding_ref[d]


def first_body(got_ref, parts_ref, coupling_ref, local_ref, pieces_ref, z_ref, assembled_ref):
    assemble_first(got_ref, assembled_ref)
    z = coarse_product(assembled_ref, parts_ref)
    z_ref[...] = z
    send_blocks(z, coupling_ref, local_ref, pieces_ref, 3)


def second_body(
    device_ref, got_ref, parts_ref, coupling_ref, local_ref, square_ref, pieces_ref, z_ref, terms_ref, assembled_ref
):
    assemble_packed(got_ref, assembled_ref, 3)
    z = coarse_product(assembled_ref, parts_ref)
    z_ref[...] = z
    terms_ref[...] = owned_terms(device_ref, assembled_ref, z)
    send_blocks(z, coupling_ref, local_ref, pieces_ref, 4, square_ref)


def choose_rows(select_ref, rows):
    high, middle, low = three_parts(rows)
    select = select_ref[...]
    return fast(select, high, NT) + fast(select, middle, NT) + fast(select, low, NT)


def by_offset(field):
    lane = lax.broadcasted_iota(jnp.int32, field.shape, 1)
    return [jnp.where(lane % 4 == o, field, 0.0) for o in range(4)]


def early_body(select_ref, green_ref, chosen_ref):
    rows = by_offset(green_ref[0]) + by_offset(green_ref[1])
    rows.append(jnp.zeros((HALF, green_ref.shape[2]), f32))
    chosen_ref[...] = choose_rows(select_ref, jnp.concatenate(rows, axis=0))


def third_body(
    device_ref, got_ref, parts_ref, local_ref, modes_ref, right_ref, select_ref, sums_2_ref, sums_3_ref, terms_ref,
    image_ref, early_ref,
    sent_ref, z_ref, assembled_ref,
):
    assemble_packed(got_ref, assembled_ref, 4)
    z = coarse_product(assembled_ref, parts_ref)
    z_ref[...] = z
    square = got_ref[3]
    for d in range(1, got_ref.shape[0] // 4):
        square = square + got_ref[4 * d + 3]
    y_0 = local_ref[0] + dot(z[:, :NC], modes_ref[0, NC:], NN)
    y_1 = local_ref[1] + dot(z, modes_ref[1], NN)
    y_2 = dot(z[:, NC:], right_ref[0, :NC], NN)
    rows = by_offset(y_0) + by_offset(y_1) + by_offset(y_2)
    rows.append(jnp.zeros((32, y_0.shape[1]), f32))
    late = choose_rows(select_ref, jnp.concatenate(rows, axis=0))
    curvature = jnp.sum(owned_terms(device_ref, assembled_ref, z), axis=1, keepdims=True)
    lane = lax.broadcasted_iota(jnp.int32, (8, LANES), 1)
    case = lax.broadcasted_iota(jnp.int32, (8, LANES), 0)
    parts = [
        sums_2_ref[:, 0:1],
        sums_2_ref[:, 1:2] + jnp.sum(terms_ref[...], axis=1, keepdims=True),
        sums_3_ref[:, 0:1],
        sums_3_ref[:, 1:2] + curvature,
    ]
    placed = jnp.zeros((8, LANES), f32)
    for k in range(4):
        placed = placed + jnp.where(lane == 96 + 8 * k + case, parts[k], 0.0)
    late = late + jnp.sum(placed, axis=0, keepdims=True)
    rows = [jnp.zeros((HALF, y_0.shape[1]), f32)] + by_offset(image_ref[0]) + by_offset(image_ref[1])
    sent_ref[:, 0, 0, :] = early_ref[...] + choose_rows(select_ref, jnp.concatenate(rows, axis=0))
    sent_ref[:, 0, 1, :] = late
    sent_ref[:, 1] = jnp.broadcast_to(square[None, 0:2], (late.shape[0], 2, LANES))
    sent_ref[:, 2] = jnp.broadcast_to(square[None, 2:4], (late.shape[0], 2, LANES))


def project_body(got_ref, basis_ref, part_ref, rows_ref, gains_ref):
    early, late = got_ref[:, 0, 0, :], got_ref[:, 0, 1, :]
    sums = jnp.broadcast_to(jnp.sum(late, axis=0, keepdims=True), (8, LANES))
    lane = lax.broadcasted_iota(jnp.int32, (8, LANES), 1)
    bb, bf, ff, fff = (pltpu.roll(sums, 32 - 8 * k, 1) for k in range(4))
    good = lane < 8
    bb, bf = jnp.where(good, bb, 1.0), jnp.where(good, bf, 1.0)
    ff, fff = jnp.where(good, ff, 2.0), jnp.where(good, fff, 8.0)
    alpha_0 = bb / bf
    norm_1 = bb - 2.0 * alpha_0 * bf + alpha_0 * alpha_0 * ff
    gain = 1.0 + norm_1 / bb
    curvature = gain * gain * bf - 2.0 * gain * alpha_0 * ff + alpha_0 * alpha_0 * fff
    alpha_1 = norm_1 / curvature
    kappas = []
    for kappa in (alpha_0 + alpha_1 * gain, alpha_1 * alpha_0):
        kappa = jnp.where(good, kappa, 0.0)
        for shift in (8, 16, 32, 64):
            kappa = kappa + pltpu.roll(kappa, shift, 1)
        kappas.append(kappa)
    gains_ref[0], gains_ref[1] = kappas[0], kappas[1]
    kappa_1, kappa_2 = kappas[0][:1], kappas[1][:1]
    wide = lax.broadcasted_iota(jnp.int32, late.shape, 1)
    extra = pltpu.roll(pltpu.roll(late, HALF, 1), 1, 0)
    last = late + jnp.where(wide < NC, extra, 0.0)
    rows = early - kappa_1 * pltpu.roll(early, HALF, 1) + kappa_2 * last
    turned = jnp.transpose(rows)
    snapshots = jnp.concatenate([turned[8 * j : 8 * j + 8] for j in range(8)], axis=1)
    rows_ref[...] = snapshots
    high, low = two_parts(snapshots)
    both = jnp.concatenate([high, low], axis=0)
    count = snapshots.shape[1]
    product = fast(both, basis_ref[:count], NN) + fast(both, basis_ref[count:], NN)
    gram = dot(snapshots, jnp.concatenate([snapshots, jnp.zeros((LANES - 8, count), f32)], axis=0), NT)
    part = jnp.concatenate([product[:8] + product[8:], gram], axis=1)
    for d in range(part_ref.shape[0]):
        part_ref[d] = part


def finish_body(got_ref, square_ref, basis_ref, rows_ref, columns_ref, projection_ref, factor_ref, *, scale):
    count = got_ref.shape[0]
    reduced = got_ref[0]
    for i in range(1, count):
        reduced = reduced + got_ref[i]
    rank = reduced.shape[1] - LANES
    coefficients = reduced[:, :rank]
    projection_ref[...] = coefficients
    low_rows, high_rows = coefficients[:, :LANES], coefficients[:, LANES:]
    squares = [square_ref[:, 1 + i // 2, i % 2, :] for i in range(4)]
    image = jnp.concatenate(
        [
            dot(low_rows, squares[0], NN) + dot(high_rows, squares[2], NN),
            dot(low_rows, squares[1], NN) + dot(high_rows, squares[3], NN),
        ],
        axis=1,
    )
    gap = image - 2.0 * coefficients
    blank = jnp.zeros((LANES - 8, rank), f32)
    gram = reduced[:, rank:] + dot(coefficients, jnp.concatenate([gap, blank], axis=0), NT)
    row = lax.broadcasted_iota(jnp.int32, (8, LANES), 0)
    lane = lax.broadcasted_iota(jnp.int32, (8, LANES), 1)
    gram = jnp.where(lane < 8, gram, 0.0)
    work = gram + jnp.where(lane == row + 8, 1.0, 0.0)
    upper = jnp.zeros((8, LANES), f32)
    for j in range(8):
        pivot = jnp.sum(jnp.where((row == j) & (lane == j), work, 0.0), axis=(0, 1), keepdims=True)
        line = jnp.sum(jnp.where(row == j, work, 0.0), axis=0, keepdims=True) / jnp.sqrt(pivot)
        upper = jnp.where(row == j, line, upper)
        column = jnp.sum(jnp.where(lane == j, work, 0.0), axis=1, keepdims=True) / jnp.sqrt(pivot)
        work = jnp.where(row > j, work - column * line, work)
    factor_ref[...] = jnp.where((lane >= row) & (lane < 8), upper, 0.0) * (1.0 / scale)
    inverse = pltpu.roll(upper, LANES - 8, 1)
    inverse = jnp.where((lane <= row) & (lane < 8), inverse, 0.0)[:, :8]
    high, low = two_parts(coefficients)
    total = rows_ref.shape[1]
    both = jnp.concatenate([high, low], axis=0)
    product = fast(both, basis_ref[:total], NT) + fast(both, basis_ref[total:], NT)
    remainder = rows_ref[...] - (product[:8] + product[8:])
    columns = dot(inverse, remainder, NN) * scale
    for t in range(8):
        index = 16 * t + lane // 8
        out = jnp.zeros((8, LANES), f32)
        for j in range(8):
            picked = jnp.take_along_axis(columns[:, j * LANES : (j + 1) * LANES], index, axis=1)
            out = jnp.where(lane % 8 == j, picked, out)
        columns_ref[:, t * LANES : (t + 1) * LANES] = out


def shards(
    rr_inverse,
    corner_modes,
    coarse_inverse,
    inertia,
    disp_now,
    vel_now,
    acc_now,
    load_next,
    basis_rows,
    piece_owner,
):
    case_count, _, unknowns = disp_now.shape
    devices = lax.axis_size(AXES)
    coarse_total = coarse_inverse.shape[1]
    rank = basis_rows.shape[1]
    last = unknowns - NI
    device = lax.axis_index(AXES).reshape(1).astype(jnp.int32)
    pair = ((2, case_count, unknowns),)
    z_shape = ((case_count, 2 * NC),)
    blocks_shape = ((case_count, 2 * LANES),)
    assembled = [pltpu.VMEM((case_count, coarse_total), f32)]

    start, right_side = call(start_body, [((devices, case_count, LANES),), pair], [SMEM] + [VMEM] * 6, grant=60 * 1024)(
        device, load_next, inertia, disp_now, vel_now, acc_now, corner_modes
    )
    got_1 = exchange(start)
    left_edge = shifted(corner_modes[1, :, last:], 1)
    right_modes = shifted(corner_modes, -1)
    coarse_parts, local_0 = call(pre_body, [((4 * NC, coarse_total), bf16), pair], [VMEM] * 3, flops=1 << 26)(
        coarse_inverse, right_side, rr_inverse
    )
    blocks_0, coupling, to_blocks = call(
        couple_body, [blocks_shape, ((2 * NC, 2 * LANES),), ((2 * LANES, 4 * NI),)], [SMEM] + [VMEM] * 4, flops=1 << 26
    )(device, corner_modes, right_modes, left_edge, local_0)

    def finish(local, z):
        mine, to_right, to_left = call(
            edge_body, [pair, ((case_count, 2 * NI),), ((case_count, NI),)], [VMEM] * 3, flops=1 << 20
        )(local, z, corner_modes)
        from_left = shifted(to_right, 1)
        from_right = shifted(to_left, -1)
        return call(join_body, [pair, pair, blocks_shape, ((case_count, LANES),)], [VMEM] * 8, flops=1 << 26, grant=60 * 1024)(
            mine, from_left, from_right, z, corner_modes, right_modes, rr_inverse, to_blocks
        )

    pieces, z_0 = call(first_body, [((3 * devices, 4, LANES),), z_shape], [VMEM] * 4, assembled, flops=1 << 24)(
        got_1, coarse_parts, coupling, blocks_0
    )
    got_2 = exchange(pieces)
    basis_parts, square, select = call(
        prep_body,
        [((2 * basis_rows.shape[0], rank), bf16), ((devices, 4, LANES),), ((devices, unknowns), bf16)],
        [VMEM, VMEM, VMEM],
        flops=1 << 26,
        grant=60 * 1024,
    )(basis_rows.reshape(devices, -1, rank), piece_owner.reshape(1, devices), z_0)
    green, local_1, blocks_1, sums_2 = finish(local_0, z_0)
    pieces, z_1, terms_1 = call(
        second_body, [((4 * devices, 4, LANES),), z_shape, z_shape], [SMEM] + [VMEM] * 5, assembled, flops=1 << 24, grant=60 * 1024
    )(device, got_2, coarse_parts, coupling, blocks_1, square)
    got_3 = exchange(pieces)
    image_1, local_2, _, sums_3 = finish(local_1, z_1)
    (early,) = call(early_body, [((devices, LANES),)], [VMEM] * 2, flops=1 << 24)(select, green)
    sent, z_2 = call(third_body, [((devices, 3, 2, LANES),), z_shape], [SMEM] + [VMEM] * 11, assembled, flops=1 << 24, grant=60 * 1024)(
        device, got_3, coarse_parts, local_2, corner_modes, right_modes, select, sums_2, sums_3, terms_1, image_1, early
    )
    got_4 = exchange(sent)
    ghost = shifted(z_2, 1)
    (late,) = call(late_body, [pair], [VMEM] * 4, flops=1 << 20)(local_2, z_2, ghost, corner_modes)
    part, snapshots, gains = call(
        project_body,
        [
            ((lax.axis_size(NEAR), case_count, rank + LANES),),
            ((case_count, basis_rows.shape[0]),),
            ((2, case_count, LANES),),
        ],
        [VMEM] * 2,
        flops=1 << 24,
    )(got_4, basis_parts)
    near = exchange(part, NEAR)
    near = near.sum(axis=0)
    got_5 = to_everyone(near, FAR)
    disp_new, vel_new = call(
        out_body, [(disp_now.shape,), (disp_now.shape,)], [VMEM] * 7, flops=1 << 22
    )(green, image_1, late, gains, disp_now, vel_now, acc_now)
    scale = math.sqrt(basis_rows.shape[0] * devices)
    new_columns, projection, factor = call(
        functools.partial(finish_body, scale=scale),
        [((case_count, basis_rows.shape[0]),), ((case_count, rank),), ((case_count, LANES),)],
        [VMEM] * 4,
        flops=1 << 24,
    )(got_5, got_4, basis_parts, snapshots)
    return (disp_new, vel_new, projection.T, factor[:, :case_count], new_columns)


def solution(mesh):
    finer = Mesh(
        mesh.devices.reshape(4, 4, 2, mesh.shape["grp"]), ("sub_0", "sub_1", "sub_2", "grp")
    )
    placed = (
        P(AXES, None, None),
        P(AXES, None, None),
        P(AXES, None),
        P(AXES, None),
        P(None, AXES, None),
        P(None, AXES, None),
        P(None, AXES, None),
        P(None, AXES, None),
        P(AXES, None),
        P(),
    )

    return jax.shard_map(
        shards,
        mesh=finer,
        in_specs=placed,
        out_specs=(P(None, AXES, None), P(None, AXES, None), P(), P(), P(None, AXES)),
        check_vma=False,
    )
```

```python
import functools
import math

import jax
import jax.numpy as jnp
from jax import lax
from jax.experimental import pallas as pl
from jax.experimental.pallas import tpu as pltpu
from jax.sharding import Mesh
from jax.sharding import PartitionSpec as P

NC = 32
NI = 128
LANES = 128
HALF = 64
AXES = ("sub_0", "sub_1", "sub_2", "grp")
FAR, NEAR = ("sub_0", "sub_1"), ("sub_2", "grp")

highest = lax.Precision.HIGHEST
time_step = 0.5
newmark_beta = 0.25
newmark_gamma = 0.5
f32, bf16 = jnp.float32, jnp.bfloat16
NT = (((1,), (1,)), ((), ()))
NN = (((1,), (0,)), ((), ()))
VMEM = pl.BlockSpec(memory_space=pltpu.VMEM)
SMEM = pl.BlockSpec(memory_space=pltpu.SMEM)


def exchange(pieces, axes=AXES):
    return lax.all_to_all(pieces, axes, split_axis=0, concat_axis=0, tiled=True)


def to_everyone(array, axes=AXES):
    return exchange(jnp.broadcast_to(array, (lax.axis_size(axes), *array.shape)), axes)


def shifted(array, by):
    count = lax.axis_size(AXES)
    return lax.ppermute(array, AXES, [(i, (i + by) % count) for i in range(count)])


def swapped(array, offset):
    count = lax.axis_size(AXES)
    pairs = [(i % count, (i + 1) % count) for i in range(offset, count + offset, 2)]
    return lax.ppermute(array, AXES, pairs + [(b, a) for a, b in pairs])


def dot(a, b, dims):
    return lax.dot_general(a, b, dims, precision=highest, preferred_element_type=f32)


def fast(a, b, dims):
    return lax.dot_general(a, b, dims, preferred_element_type=f32)


def call(body, outs, ins, scratch=(), flops=0, grant=16000):
    return pl.pallas_call(
        body,
        out_shape=[jax.ShapeDtypeStruct(shape, f32 if len(rest) == 0 else rest[0]) for shape, *rest in outs],
        in_specs=ins,
        out_specs=[VMEM] * len(outs),
        scratch_shapes=list(scratch),
        compiler_params=pltpu.CompilerParams(vmem_limit_bytes=grant << 10),
        cost_estimate=pl.CostEstimate(flops=flops, bytes_accessed=1 << 20, transcendentals=0),
    )


def two_parts(x):
    high = x.astype(bf16)
    return high, (x - high.astype(f32)).astype(bf16)


def three_parts(x):
    high = x.astype(bf16)
    rest = x - high.astype(f32)
    middle = rest.astype(bf16)
    return high, middle, (rest - middle.astype(f32)).astype(bf16)


def start_body(device_ref, load_ref, inertia_ref, disp_ref, vel_ref, acc_ref, modes_ref, start_ref, right_ref):
    blank = jnp.zeros((NC, modes_ref.shape[2]), f32)
    fields = []
    for s in range(2):
        moved = disp_ref[:, s, :] + time_step * vel_ref[:, s, :]
        moved = moved + (0.5 - newmark_beta) * time_step * time_step * acc_ref[:, s, :]
        fields.append(load_ref[:, s, :] + inertia_ref[s : s + 1] * moved)
        right_ref[s] = fields[s]
    part_0 = jnp.concatenate([modes_ref[0, NC:], blank, blank, modes_ref[0, :NC]], axis=0)
    part_1 = jnp.concatenate([modes_ref[1, :NC], modes_ref[1, NC:], blank, blank], axis=0)
    blocks = dot(fields[0], part_0, NT) + dot(fields[1], part_1, NT)
    even = lax.rem(device_ref[0], 2) == 0
    blocks = jnp.where(even, blocks, pltpu.roll(blocks, HALF, 1))
    for d in range(start_ref.shape[0]):
        start_ref[d] = blocks


def pre_body(matrix_ref, right_ref, rr_ref, parts_ref, local_ref):
    rows = matrix_ref.shape[0]
    high, low = two_parts(matrix_ref[...])
    parts_ref[:rows] = high
    parts_ref[rows:] = low
    for s in range(2):
        local_ref[s] = dot(right_ref[s], rr_ref[s], NN)


def couple_body(
    device_ref, modes_ref, swap_a_ref, swap_b_ref, local_ref, blocks_ref, coupling_ref, to_blocks_ref, right_ref
):
    last = modes_ref.shape[2] - NI
    first_right = lax.rem(device_ref[0], 2) == 0
    for s in range(2):
        right_ref[s] = jnp.where(first_right, swap_a_ref[s], swap_b_ref[s])
    left = jnp.where(first_right, swap_b_ref[1, :, last:], swap_a_ref[1, :, last:])
    even = jnp.where(first_right, 1, 0)
    first, final = [modes_ref[s, :, :NI] for s in range(2)], [modes_ref[s, :, last:] for s in range(2)]
    right_first, right_final = [right_ref[s, :, :NI] for s in range(2)], right_ref[0, :, last:]
    rows = [
        {0: left[:NC]},
        {0: left[NC:] - first[0][:NC], 1: final[0][:NC]},
        {0: -first[0][NC:], 1: final[0][NC:] - first[1][:NC], 2: final[1][:NC]},
        {1: -first[1][NC:], 2: final[1][NC:] - right_first[0][:NC], 3: right_final[:NC]},
        {2: -right_first[0][NC:], 3: right_final[NC:] - right_first[1][:NC]},
        {3: -right_first[1][NC:]},
    ]
    to_blocks_ref[...] = jnp.zeros(to_blocks_ref.shape, f32)
    for i, parts in enumerate(rows):
        at = pl.multiple_of(lax.rem(i * NC + 192 * even, 256), NC)
        for k, values in parts.items():
            to_blocks_ref[pl.ds(at, NC), k * NI : (k + 1) * NI] = values
    blank = jnp.zeros((NC, modes_ref.shape[2]), f32)
    unit_0 = jnp.concatenate([modes_ref[0, NC:], blank], axis=0)
    unit_1 = modes_ref[1]
    unit_2 = jnp.concatenate([blank, right_ref[0, :NC]], axis=0)
    jumps = jnp.concatenate(
        [-unit_0[:, :NI], unit_0[:, last:] - unit_1[:, :NI], unit_1[:, last:] - unit_2[:, :NI], unit_2[:, last:]], axis=1
    )
    coupling_ref[...] = dot(jumps, to_blocks_ref[...], NT)
    blocks_ref[...] = own_blocks(local_ref[0], local_ref[1], to_blocks_ref)


def own_blocks(field_0, field_1, to_blocks_ref):
    last = field_0.shape[1] - NI
    jumps = [-field_0[:, :NI], field_0[:, last:] - field_1[:, :NI], field_1[:, last:]]
    return dot(jnp.concatenate(jumps, axis=1), to_blocks_ref[:, : 3 * NI], NT)


def edge_body(device_ref, local_ref, z_ref, modes_ref, mine_ref, swap_a_ref, swap_b_ref):
    last = local_ref.shape[2] - NI
    z = z_ref[...]
    mine_0 = local_ref[0] + dot(z[:, :NC], modes_ref[0, NC:], NN)
    mine_1 = local_ref[1] + dot(z, modes_ref[1], NN)
    mine_ref[0], mine_ref[1] = mine_0, mine_1
    first_right = lax.rem(device_ref[0], 2) == 0
    to_left = jnp.concatenate([mine_0[:, :NI], jnp.zeros_like(mine_0[:, :NI])], axis=1)
    to_right = jnp.concatenate([mine_1[:, last:], jnp.concatenate([z, z], axis=1)], axis=1)
    swap_a_ref[...] = jnp.where(first_right, to_right, to_left)
    swap_b_ref[...] = jnp.where(first_right, to_left, to_right)


def join_body(
    device_ref, mine_ref, swap_a_ref, swap_b_ref, z_ref, modes_ref, right_ref, rr_ref, to_blocks_ref,
    field_ref, local_ref, blocks_ref, sums_ref,
):
    last = mine_ref.shape[2] - NI
    mine_1 = mine_ref[1]
    first_right = lax.rem(device_ref[0], 2) == 0
    from_left = jnp.where(first_right, swap_b_ref[...], swap_a_ref[...])
    from_right = jnp.where(first_right, swap_a_ref[...], swap_b_ref[...])[:, :NI]
    ghost = from_left[:, NI : NI + 2 * NC]
    mine_0 = mine_ref[0] + dot(ghost[:, NC:], modes_ref[0, :NC], NN)
    field_ref[0], field_ref[1] = mine_0, mine_1
    jump_a = from_left[:, :NI] - mine_0[:, :NI]
    jump_b = mine_0[:, last:] - mine_1[:, :NI]
    jump_c = mine_1[:, last:] - (from_right + dot(z_ref[:, NC:], right_ref[0, :NC, :NI], NN))
    inner = jnp.zeros((mine_1.shape[0], 1), f32)
    outs = []
    for s, (first, final) in enumerate([(-jump_a, jump_b), (-jump_b, jump_c)]):
        out = dot(first, rr_ref[s, :NI], NN) + dot(final, rr_ref[s, last:], NN)
        local_ref[s] = out
        inner = inner + jnp.sum(out[:, :NI] * first + out[:, last:] * final, axis=1, keepdims=True)
        outs.append(out)
    blocks_ref[...] = own_blocks(outs[0], outs[1], to_blocks_ref)
    square = jnp.sum(jump_b * jump_b + jump_c * jump_c, axis=1, keepdims=True)
    lane = lax.broadcasted_iota(jnp.int32, sums_ref.shape, 1)
    sums_ref[...] = jnp.where(lane == 0, square, 0.0) + jnp.where(lane == 1, inner, 0.0)


def prep_body(basis_ref, owner_ref, after_ref, parts_ref, square_ref, select_ref):
    devices, width, rank = basis_ref.shape
    total = devices * width
    square = jnp.zeros((rank, rank), f32)
    for j in range(width):
        rows = basis_ref[:, j, :]
        high, low = two_parts(rows)
        parts_ref[j * devices : (j + 1) * devices] = high
        parts_ref[total + j * devices : total + (j + 1) * devices] = low
        turned_high, turned_low = two_parts(jnp.transpose(rows))
        square = square + fast(turned_high, high, NN) + (fast(turned_high, low, NN) + fast(turned_low, high, NN))
    for i in range(4):
        r, h = i // 2, i % 2
        square_ref[:, i, :] = square[r * LANES : (r + 1) * LANES, h * LANES : (h + 1) * LANES]
    unknowns = select_ref.shape[1]
    rows = lax.broadcasted_iota(jnp.int32, (devices, unknowns), 0)
    columns = lax.broadcasted_iota(jnp.int32, (devices, unknowns), 1)
    each = unknowns // devices
    repeat = jnp.where(columns // each == rows, 1.0, 0.0).astype(bf16)
    owner = jnp.broadcast_to(owner_ref[...].astype(f32), (8, devices)).astype(bf16)
    owner = fast(owner, repeat, NN)[:1]
    select_ref[...] = jnp.where(owner == rows.astype(f32), 1.0, 0.0).astype(bf16)


def late_body(local_ref, z_ref, ghost_ref, modes_ref, late_ref):
    z = z_ref[...]
    ghost = ghost_ref[...][:, NC:]
    late_ref[0] = local_ref[0] + dot(z[:, :NC], modes_ref[0, NC:], NN) + dot(ghost, modes_ref[0, :NC], NN)
    late_ref[1] = local_ref[1] + dot(z, modes_ref[1], NN)


def out_body(
    green_ref, image_ref, late_ref, gains_ref, disp_ref, vel_ref, acc_ref, disp_out_ref, vel_out_ref
):
    kappa_1, kappa_2 = gains_ref[0], gains_ref[1]
    case = lax.broadcasted_iota(jnp.int32, kappa_1.shape, 0)
    lane = lax.broadcasted_iota(jnp.int32, kappa_1.shape, 1)
    kappa_1 = jnp.sum(jnp.where(case == lane, kappa_1, 0.0), axis=1, keepdims=True)
    kappa_2 = jnp.sum(jnp.where(case == lane, kappa_2, 0.0), axis=1, keepdims=True)
    for s in range(2):
        disp = green_ref[s] - kappa_1 * image_ref[s] + kappa_2 * late_ref[s]
        vel, acc = vel_ref[:, s, :], acc_ref[:, s, :]
        accel = (
            (disp - disp_ref[:, s, :]) * (1.0 / (newmark_beta * time_step * time_step))
            - vel * (1.0 / (newmark_beta * time_step))
            - (0.5 / newmark_beta - 1.0) * acc
        )
        disp_out_ref[:, s, :] = disp
        vel_out_ref[:, s, :] = vel + time_step * ((1.0 - newmark_gamma) * acc + newmark_gamma * accel)


def coarse_product(assembled_ref, parts_ref):
    cases = assembled_ref.shape[0]
    high, low = two_parts(assembled_ref[...])
    both = fast(jnp.concatenate([high, low], axis=0), parts_ref[...], NT)
    both = both[:cases] + both[cases:]
    return both[:, :HALF] + both[:, HALF:]


def assemble_packed(got_ref, assembled_ref, slots):
    tiles = assembled_ref.shape[1] // LANES
    lane = lax.broadcasted_iota(jnp.int32, (4, LANES), 1)
    lower = lane < HALF
    for m in range(tiles):
        even, odd = 2 * slots * m, 2 * slots * m + slots
        following = 2 * slots * ((m + 1) % tiles) + 2
        previous = 2 * slots * ((m - 1) % tiles) + slots + 2
        extra_even, extra_odd = got_ref[following], got_ref[previous]
        top = got_ref[even] + got_ref[odd] + jnp.where(lower, extra_odd, extra_even)
        turned = pltpu.roll(jnp.where(lower, extra_even, extra_odd), HALF, 1)
        bottom = got_ref[even + 1] + got_ref[odd + 1] + turned
        assembled_ref[0:4, m * LANES : (m + 1) * LANES] = top
        assembled_ref[4:8, m * LANES : (m + 1) * LANES] = bottom


def assemble_first(got_ref, assembled_ref):
    tiles = assembled_ref.shape[1] // LANES
    lane = lax.broadcasted_iota(jnp.int32, (8, LANES), 1)
    for m in range(tiles):
        following = (2 * m + 2) % (2 * tiles)
        own = got_ref[2 * m + 1] + jnp.where(lane < HALF, got_ref[2 * m], 0.0)
        assembled_ref[:, m * LANES : (m + 1) * LANES] = own + jnp.where(
            lane >= LANES - NC, got_ref[following], 0.0
        )


def owned_terms(device_ref, assembled_ref, z):
    device = device_ref[0]
    tile = assembled_ref[:, pl.ds(pl.multiple_of((device // 2) * LANES, LANES), LANES)]
    even = lax.rem(device, 2) == 0
    return jnp.where(even, tile[:, :HALF], tile[:, HALF:]) * z


def send_blocks(z, coupling_ref, local_ref, pieces_ref, slots, riding_ref=None):
    blocks = local_ref[...] + dot(z, coupling_ref[...], NN)
    main, extra = blocks[:, :LANES], blocks[:, LANES:]
    turned = pltpu.roll(extra, HALF, 1)
    packed = extra[0:4] + turned[4:8]
    for d in range(pieces_ref.shape[0] // slots):
        pieces_ref[slots * d] = main[0:4]
        pieces_ref[slots * d + 1] = main[4:8]
        pieces_ref[slots * d + 2] = packed
        if riding_ref is not None:
            pieces_ref[slots * d + 3] = riding_ref[d]


def first_body(got_ref, parts_ref, coupling_ref, local_ref, pieces_ref, z_ref, assembled_ref):
    assemble_first(got_ref, assembled_ref)
    z = coarse_product(assembled_ref, parts_ref)
    z_ref[...] = z
    send_blocks(z, coupling_ref, local_ref, pieces_ref, 3)


def second_body(
    device_ref, got_ref, parts_ref, coupling_ref, local_ref, square_ref, pieces_ref, z_ref, terms_ref, assembled_ref
):
    assemble_packed(got_ref, assembled_ref, 3)
    z = coarse_product(assembled_ref, parts_ref)
    z_ref[...] = z
    terms_ref[...] = owned_terms(device_ref, assembled_ref, z)
    send_blocks(z, coupling_ref, local_ref, pieces_ref, 4, square_ref)


def choose_rows(select_ref, rows):
    high, middle, low = three_parts(rows)
    select = select_ref[...]
    return fast(select, high, NT) + fast(select, middle, NT) + fast(select, low, NT)


def by_offset(field):
    lane = lax.broadcasted_iota(jnp.int32, field.shape, 1)
    return [jnp.where(lane % 4 == o, field, 0.0) for o in range(4)]


def early_body(select_ref, green_ref, chosen_ref):
    rows = by_offset(green_ref[0]) + by_offset(green_ref[1])
    rows.append(jnp.zeros((HALF, green_ref.shape[2]), f32))
    chosen_ref[...] = choose_rows(select_ref, jnp.concatenate(rows, axis=0))


def third_body(
    device_ref, got_ref, parts_ref, local_ref, modes_ref, right_ref, select_ref, sums_2_ref, sums_3_ref, terms_ref,
    image_ref, early_ref,
    sent_ref, z_ref, assembled_ref,
):
    assemble_packed(got_ref, assembled_ref, 4)
    z = coarse_product(assembled_ref, parts_ref)
    z_ref[...] = z
    square = got_ref[3]
    for d in range(1, got_ref.shape[0] // 4):
        square = square + got_ref[4 * d + 3]
    y_0 = local_ref[0] + dot(z[:, :NC], modes_ref[0, NC:], NN)
    y_1 = local_ref[1] + dot(z, modes_ref[1], NN)
    y_2 = dot(z[:, NC:], right_ref[0, :NC], NN)
    rows = by_offset(y_0) + by_offset(y_1) + by_offset(y_2)
    rows.append(jnp.zeros((32, y_0.shape[1]), f32))
    late = choose_rows(select_ref, jnp.concatenate(rows, axis=0))
    curvature = jnp.sum(owned_terms(device_ref, assembled_ref, z), axis=1, keepdims=True)
    lane = lax.broadcasted_iota(jnp.int32, (8, LANES), 1)
    case = lax.broadcasted_iota(jnp.int32, (8, LANES), 0)
    parts = [
        sums_2_ref[:, 0:1],
        sums_2_ref[:, 1:2] + jnp.sum(terms_ref[...], axis=1, keepdims=True),
        sums_3_ref[:, 0:1],
        sums_3_ref[:, 1:2] + curvature,
    ]
    placed = jnp.zeros((8, LANES), f32)
    for k in range(4):
        placed = placed + jnp.where(lane == 96 + 8 * k + case, parts[k], 0.0)
    late = late + jnp.sum(placed, axis=0, keepdims=True)
    rows = [jnp.zeros((HALF, y_0.shape[1]), f32)] + by_offset(image_ref[0]) + by_offset(image_ref[1])
    sent_ref[:, 0, 0, :] = early_ref[...] + choose_rows(select_ref, jnp.concatenate(rows, axis=0))
    sent_ref[:, 0, 1, :] = late
    sent_ref[:, 1] = jnp.broadcast_to(square[None, 0:2], (late.shape[0], 2, LANES))
    sent_ref[:, 2] = jnp.broadcast_to(square[None, 2:4], (late.shape[0], 2, LANES))


def project_body(got_ref, basis_ref, part_ref, rows_ref, gains_ref):
    early, late = got_ref[:, 0, 0, :], got_ref[:, 0, 1, :]
    sums = jnp.broadcast_to(jnp.sum(late, axis=0, keepdims=True), (8, LANES))
    lane = lax.broadcasted_iota(jnp.int32, (8, LANES), 1)
    bb, bf, ff, fff = (pltpu.roll(sums, 32 - 8 * k, 1) for k in range(4))
    good = lane < 8
    bb, bf = jnp.where(good, bb, 1.0), jnp.where(good, bf, 1.0)
    ff, fff = jnp.where(good, ff, 2.0), jnp.where(good, fff, 8.0)
    alpha_0 = bb / bf
    norm_1 = bb - 2.0 * alpha_0 * bf + alpha_0 * alpha_0 * ff
    gain = 1.0 + norm_1 / bb
    curvature = gain * gain * bf - 2.0 * gain * alpha_0 * ff + alpha_0 * alpha_0 * fff
    alpha_1 = norm_1 / curvature
    kappas = []
    for kappa in (alpha_0 + alpha_1 * gain, alpha_1 * alpha_0):
        kappa = jnp.where(good, kappa, 0.0)
        for shift in (8, 16, 32, 64):
            kappa = kappa + pltpu.roll(kappa, shift, 1)
        kappas.append(kappa)
    gains_ref[0], gains_ref[1] = kappas[0], kappas[1]
    kappa_1, kappa_2 = kappas[0][:1], kappas[1][:1]
    wide = lax.broadcasted_iota(jnp.int32, late.shape, 1)
    extra = pltpu.roll(pltpu.roll(late, HALF, 1), 1, 0)
    last = late + jnp.where(wide < NC, extra, 0.0)
    rows = early - kappa_1 * pltpu.roll(early, HALF, 1) + kappa_2 * last
    turned = jnp.transpose(rows)
    snapshots = jnp.concatenate([turned[8 * j : 8 * j + 8] for j in range(8)], axis=1)
    rows_ref[...] = snapshots
    high, low = two_parts(snapshots)
    both = jnp.concatenate([high, low], axis=0)
    count = snapshots.shape[1]
    product = fast(both, basis_ref[:count], NN) + fast(both, basis_ref[count:], NN)
    gram = dot(snapshots, jnp.concatenate([snapshots, jnp.zeros((LANES - 8, count), f32)], axis=0), NT)
    part = jnp.concatenate([product[:8] + product[8:], gram], axis=1)
    for d in range(part_ref.shape[0]):
        part_ref[d] = part


def finish_body(got_ref, square_ref, basis_ref, rows_ref, columns_ref, projection_ref, factor_ref, *, scale):
    count = got_ref.shape[0]
    reduced = got_ref[0]
    for i in range(1, count):
        reduced = reduced + got_ref[i]
    rank = reduced.shape[1] - LANES
    coefficients = reduced[:, :rank]
    projection_ref[...] = coefficients
    low_rows, high_rows = coefficients[:, :LANES], coefficients[:, LANES:]
    squares = [square_ref[:, 1 + i // 2, i % 2, :] for i in range(4)]
    image = jnp.concatenate(
        [
            dot(low_rows, squares[0], NN) + dot(high_rows, squares[2], NN),
            dot(low_rows, squares[1], NN) + dot(high_rows, squares[3], NN),
        ],
        axis=1,
    )
    gap = image - 2.0 * coefficients
    blank = jnp.zeros((LANES - 8, rank), f32)
    gram = reduced[:, rank:] + dot(coefficients, jnp.concatenate([gap, blank], axis=0), NT)
    row = lax.broadcasted_iota(jnp.int32, (8, LANES), 0)
    lane = lax.broadcasted_iota(jnp.int32, (8, LANES), 1)
    gram = jnp.where(lane < 8, gram, 0.0)
    work = gram + jnp.where(lane == row + 8, 1.0, 0.0)
    upper = jnp.zeros((8, LANES), f32)
    for j in range(8):
        pivot = jnp.sum(jnp.where((row == j) & (lane == j), work, 0.0), axis=(0, 1), keepdims=True)
        line = jnp.sum(jnp.where(row == j, work, 0.0), axis=0, keepdims=True) / jnp.sqrt(pivot)
        upper = jnp.where(row == j, line, upper)
        column = jnp.sum(jnp.where(lane == j, work, 0.0), axis=1, keepdims=True) / jnp.sqrt(pivot)
        work = jnp.where(row > j, work - column * line, work)
    factor_ref[...] = jnp.where((lane >= row) & (lane < 8), upper, 0.0) * (1.0 / scale)
    inverse = pltpu.roll(upper, LANES - 8, 1)
    inverse = jnp.where((lane <= row) & (lane < 8), inverse, 0.0)[:, :8]
    high, low = two_parts(coefficients)
    total = rows_ref.shape[1]
    both = jnp.concatenate([high, low], axis=0)
    product = fast(both, basis_ref[:total], NT) + fast(both, basis_ref[total:], NT)
    remainder = rows_ref[...] - (product[:8] + product[8:])
    columns = dot(inverse, remainder, NN) * scale
    for t in range(8):
        index = 16 * t + lane // 8
        out = jnp.zeros((8, LANES), f32)
        for j in range(8):
            picked = jnp.take_along_axis(columns[:, j * LANES : (j + 1) * LANES], index, axis=1)
            out = jnp.where(lane % 8 == j, picked, out)
        columns_ref[:, t * LANES : (t + 1) * LANES] = out


def shards(
    rr_inverse,
    corner_modes,
    coarse_inverse,
    inertia,
    disp_now,
    vel_now,
    acc_now,
    load_next,
    basis_rows,
    piece_owner,
):
    case_count, _, unknowns = disp_now.shape
    devices = lax.axis_size(AXES)
    coarse_total = coarse_inverse.shape[1]
    rank = basis_rows.shape[1]
    device = lax.axis_index(AXES).reshape(1).astype(jnp.int32)
    pair = ((2, case_count, unknowns),)
    z_shape = ((case_count, 2 * NC),)
    blocks_shape = ((case_count, 2 * LANES),)
    assembled = [pltpu.VMEM((case_count, coarse_total), f32)]

    start, right_side = call(start_body, [((devices, case_count, LANES),), pair], [SMEM] + [VMEM] * 6, grant=60 * 1024)(
        device, load_next, inertia, disp_now, vel_now, acc_now, corner_modes
    )
    got_1 = exchange(start)
    swap_a = swapped(corner_modes, 0)
    swap_b = swapped(corner_modes, 1)
    coarse_parts, local_0 = call(pre_body, [((4 * NC, coarse_total), bf16), pair], [VMEM] * 3, flops=1 << 26)(
        coarse_inverse, right_side, rr_inverse
    )
    blocks_0, coupling, to_blocks, right_modes = call(
        couple_body, [blocks_shape, ((2 * NC, 2 * LANES),), ((2 * LANES, 4 * NI),), (corner_modes.shape,)],
        [SMEM] + [VMEM] * 4, flops=1 << 26,
    )(device, corner_modes, swap_a, swap_b, local_0)

    def finish(local, z):
        mine, to_a, to_b = call(edge_body, [pair, blocks_shape, blocks_shape], [SMEM] + [VMEM] * 3, flops=1 << 20)(
            device, local, z, corner_modes
        )
        from_a = swapped(to_a, 0)
        from_b = swapped(to_b, 1)
        return call(join_body, [pair, pair, blocks_shape, ((case_count, LANES),)], [SMEM] + [VMEM] * 8, flops=1 << 26, grant=60 * 1024)(
            device, mine, from_a, from_b, z, corner_modes, right_modes, rr_inverse, to_blocks
        )

    pieces, z_0 = call(first_body, [((3 * devices, 4, LANES),), z_shape], [VMEM] * 4, assembled, flops=1 << 24)(
        got_1, coarse_parts, coupling, blocks_0
    )
    got_2 = exchange(pieces)
    basis_parts, square, select = call(
        prep_body,
        [((2 * basis_rows.shape[0], rank), bf16), ((devices, 4, LANES),), ((devices, unknowns), bf16)],
        [VMEM, VMEM, VMEM],
        flops=1 << 26,
        grant=60 * 1024,
    )(basis_rows.reshape(devices, -1, rank), piece_owner.reshape(1, devices), z_0)
    green, local_1, blocks_1, sums_2 = finish(local_0, z_0)
    pieces, z_1, terms_1 = call(
        second_body, [((4 * devices, 4, LANES),), z_shape, z_shape], [SMEM] + [VMEM] * 5, assembled, flops=1 << 24, grant=60 * 1024
    )(device, got_2, coarse_parts, coupling, blocks_1, square)
    got_3 = exchange(pieces)
    image_1, local_2, _, sums_3 = finish(local_1, z_1)
    (early,) = call(early_body, [((devices, LANES),)], [VMEM] * 2, flops=1 << 24)(select, green)
    sent, z_2 = call(third_body, [((devices, 3, 2, LANES),), z_shape], [SMEM] + [VMEM] * 11, assembled, flops=1 << 24, grant=60 * 1024)(
        device, got_3, coarse_parts, local_2, corner_modes, right_modes, select, sums_2, sums_3, terms_1, image_1, early
    )
    got_4 = exchange(sent)
    ghost = shifted(z_2, 1)
    (late,) = call(late_body, [pair], [VMEM] * 4, flops=1 << 20)(local_2, z_2, ghost, corner_modes)
    part, snapshots, gains = call(
        project_body,
        [
            ((lax.axis_size(NEAR), case_count, rank + LANES),),
            ((case_count, basis_rows.shape[0]),),
            ((2, case_count, LANES),),
        ],
        [VMEM] * 2,
        flops=1 << 24,
    )(got_4, basis_parts)
    near = exchange(part, NEAR)
    near = near.sum(axis=0)
    got_5 = to_everyone(near, FAR)
    disp_new, vel_new = call(
        out_body, [(disp_now.shape,), (disp_now.shape,)], [VMEM] * 7, flops=1 << 22
    )(green, image_1, late, gains, disp_now, vel_now, acc_now)
    scale = math.sqrt(basis_rows.shape[0] * devices)
    new_columns, projection, factor = call(
        functools.partial(finish_body, scale=scale),
        [((case_count, basis_rows.shape[0]),), ((case_count, rank),), ((case_count, LANES),)],
        [VMEM] * 4,
        flops=1 << 24,
    )(got_5, got_4, basis_parts, snapshots)
    return (disp_new, vel_new, projection.T, factor[:, :case_count], new_columns)


def solution(mesh):
    finer = Mesh(
        mesh.devices.reshape(4, 4, 2, mesh.shape["grp"]), ("sub_0", "sub_1", "sub_2", "grp")
    )
    placed = (
        P(AXES, None, None),
        P(AXES, None, None),
        P(AXES, None),
        P(AXES, None),
        P(None, AXES, None),
        P(None, AXES, None),
        P(None, AXES, None),
        P(None, AXES, None),
        P(AXES, None),
        P(),
    )

    return jax.shard_map(
        shards,
        mesh=finer,
        in_specs=placed,
        out_specs=(P(None, AXES, None), P(None, AXES, None), P(), P(), P(None, AXES)),
        check_vma=False,
    )
```

```python
import functools
import math

import jax
import jax.numpy as jnp
from jax import lax
from jax.experimental import pallas as pl
from jax.experimental.pallas import tpu as pltpu
from jax.sharding import Mesh
from jax.sharding import PartitionSpec as P

NC = 32
NI = 128
LANES = 128
HALF = 64
AXES = ("sub_0", "sub_1", "sub_2", "grp")
FAR, NEAR = ("sub_0", "sub_1"), ("sub_2", "grp")

highest = lax.Precision.HIGHEST
time_step = 0.5
newmark_beta = 0.25
newmark_gamma = 0.5
f32, bf16 = jnp.float32, jnp.bfloat16
NT = (((1,), (1,)), ((), ()))
NN = (((1,), (0,)), ((), ()))
VMEM = pl.BlockSpec(memory_space=pltpu.VMEM)
SMEM = pl.BlockSpec(memory_space=pltpu.SMEM)


def exchange(pieces, axes=AXES):
    return lax.all_to_all(pieces, axes, split_axis=0, concat_axis=0, tiled=True)


def to_everyone(array, axes=AXES):
    return exchange(jnp.broadcast_to(array, (lax.axis_size(axes), *array.shape)), axes)


def shifted(array, by):
    count = lax.axis_size(AXES)
    return lax.ppermute(array, AXES, [(i, (i + by) % count) for i in range(count)])


def dot(a, b, dims):
    return lax.dot_general(a, b, dims, precision=highest, preferred_element_type=f32)


def fast(a, b, dims):
    return lax.dot_general(a, b, dims, preferred_element_type=f32)


def call(body, outs, ins, scratch=(), flops=0, grant=16000):
    return pl.pallas_call(
        body,
        out_shape=[jax.ShapeDtypeStruct(shape, f32 if len(rest) == 0 else rest[0]) for shape, *rest in outs],
        in_specs=ins,
        out_specs=[VMEM] * len(outs),
        scratch_shapes=list(scratch),
        compiler_params=pltpu.CompilerParams(vmem_limit_bytes=grant << 10),
        cost_estimate=pl.CostEstimate(flops=flops, bytes_accessed=1 << 20, transcendentals=0),
    )


def two_parts(x):
    high = x.astype(bf16)
    return high, (x - high.astype(f32)).astype(bf16)


def three_parts(x):
    high = x.astype(bf16)
    rest = x - high.astype(f32)
    middle = rest.astype(bf16)
    return high, middle, (rest - middle.astype(f32)).astype(bf16)


def start_body(device_ref, load_ref, inertia_ref, disp_ref, vel_ref, acc_ref, modes_ref, start_ref, right_ref):
    blank = jnp.zeros((NC, modes_ref.shape[2]), f32)
    fields = []
    for s in range(2):
        moved = disp_ref[:, s, :] + time_step * vel_ref[:, s, :]
        moved = moved + (0.5 - newmark_beta) * time_step * time_step * acc_ref[:, s, :]
        fields.append(load_ref[:, s, :] + inertia_ref[s : s + 1] * moved)
        right_ref[s] = fields[s]
    part_0 = jnp.concatenate([modes_ref[0, NC:], blank, blank, modes_ref[0, :NC]], axis=0)
    part_1 = jnp.concatenate([modes_ref[1, :NC], modes_ref[1, NC:], blank, blank], axis=0)
    blocks = dot(fields[0], part_0, NT) + dot(fields[1], part_1, NT)
    even = lax.rem(device_ref[0], 2) == 0
    blocks = jnp.where(even, blocks, pltpu.roll(blocks, HALF, 1))
    for d in range(start_ref.shape[0]):
        start_ref[d] = blocks


def pre_body(matrix_ref, right_ref, rr_ref, parts_ref, local_ref):
    rows = matrix_ref.shape[0]
    high, low = two_parts(matrix_ref[...])
    parts_ref[:rows] = high
    parts_ref[rows:] = low
    for s in range(2):
        local_ref[s] = dot(right_ref[s], rr_ref[s], NN)


def couple_body(device_ref, modes_ref, right_ref, left_ref, local_ref, blocks_ref, coupling_ref, to_blocks_ref):
    last = modes_ref.shape[2] - NI
    even = jnp.where(lax.rem(device_ref[0], 2) == 0, 1, 0)
    first, final = [modes_ref[s, :, :NI] for s in range(2)], [modes_ref[s, :, last:] for s in range(2)]
    right_first, right_final = [right_ref[s, :, :NI] for s in range(2)], right_ref[0, :, last:]
    left = left_ref[...]
    rows = [
        {0: left[:NC]},
        {0: left[NC:] - first[0][:NC], 1: final[0][:NC]},
        {0: -first[0][NC:], 1: final[0][NC:] - first[1][:NC], 2: final[1][:NC]},
        {1: -first[1][NC:], 2: final[1][NC:] - right_first[0][:NC], 3: right_final[:NC]},
        {2: -right_first[0][NC:], 3: right_final[NC:] - right_first[1][:NC]},
        {3: -right_first[1][NC:]},
    ]
    to_blocks_ref[...] = jnp.zeros(to_blocks_ref.shape, f32)
    for i, parts in enumerate(rows):
        at = pl.multiple_of(lax.rem(i * NC + 192 * even, 256), NC)
        for k, values in parts.items():
            to_blocks_ref[pl.ds(at, NC), k * NI : (k + 1) * NI] = values
    blank = jnp.zeros((NC, modes_ref.shape[2]), f32)
    unit_0 = jnp.concatenate([modes_ref[0, NC:], blank], axis=0)
    unit_1 = modes_ref[1]
    unit_2 = jnp.concatenate([blank, right_ref[0, :NC]], axis=0)
    jumps = jnp.concatenate(
        [-unit_0[:, :NI], unit_0[:, last:] - unit_1[:, :NI], unit_1[:, last:] - unit_2[:, :NI], unit_2[:, last:]], axis=1
    )
    coupling_ref[...] = dot(jumps, to_blocks_ref[...], NT)
    blocks_ref[...] = own_blocks(local_ref[0], local_ref[1], to_blocks_ref)


def own_blocks(field_0, field_1, to_blocks_ref):
    last = field_0.shape[1] - NI
    jumps = [-field_0[:, :NI], field_0[:, last:] - field_1[:, :NI], field_1[:, last:]]
    return dot(jnp.concatenate(jumps, axis=1), to_blocks_ref[:, : 3 * NI], NT)


def edge_body(local_ref, z_ref, modes_ref, mine_ref, to_right_ref, to_left_ref):
    last = local_ref.shape[2] - NI
    z = z_ref[...]
    mine_0 = local_ref[0] + dot(z[:, :NC], modes_ref[0, NC:], NN)
    mine_1 = local_ref[1] + dot(z, modes_ref[1], NN)
    mine_ref[0], mine_ref[1] = mine_0, mine_1
    to_left_ref[...] = mine_0[:, :NI]
    to_right_ref[:, :NI] = mine_1[:, last:]
    to_right_ref[:, NI:] = jnp.concatenate([z, z], axis=1)


def join_body(
    mine_ref, from_left_ref, from_right_ref, z_ref, modes_ref, right_ref, rr_ref, to_blocks_ref,
    field_ref, local_ref, blocks_ref, sums_ref,
):
    last = mine_ref.shape[2] - NI
    mine_1 = mine_ref[1]
    ghost = from_left_ref[:, NI : NI + 2 * NC]
    mine_0 = mine_ref[0] + dot(ghost[:, NC:], modes_ref[0, :NC], NN)
    field_ref[0], field_ref[1] = mine_0, mine_1
    jump_a = from_left_ref[:, :NI] - mine_0[:, :NI]
    jump_b = mine_0[:, last:] - mine_1[:, :NI]
    jump_c = mine_1[:, last:] - (from_right_ref[...] + dot(z_ref[:, NC:], right_ref[0, :NC, :NI], NN))
    inner = jnp.zeros((mine_1.shape[0], 1), f32)
    outs = []
    for s, (first, final) in enumerate([(-jump_a, jump_b), (-jump_b, jump_c)]):
        out = dot(first, rr_ref[s, :NI], NN) + dot(final, rr_ref[s, last:], NN)
        local_ref[s] = out
        inner = inner + jnp.sum(out[:, :NI] * first + out[:, last:] * final, axis=1, keepdims=True)
        outs.append(out)
    blocks_ref[...] = own_blocks(outs[0], outs[1], to_blocks_ref)
    square = jnp.sum(jump_b * jump_b + jump_c * jump_c, axis=1, keepdims=True)
    lane = lax.broadcasted_iota(jnp.int32, sums_ref.shape, 1)
    sums_ref[...] = jnp.where(lane == 0, square, 0.0) + jnp.where(lane == 1, inner, 0.0)


def prep_body(basis_ref, owner_ref, after_ref, parts_ref, square_ref, select_ref):
    devices, width, rank = basis_ref.shape
    total = devices * width
    square = jnp.zeros((rank, rank), f32)
    for j in range(width):
        rows = basis_ref[:, j, :]
        high, low = two_parts(rows)
        parts_ref[j * devices : (j + 1) * devices] = high
        parts_ref[total + j * devices : total + (j + 1) * devices] = low
        turned_high, turned_low = two_parts(jnp.transpose(rows))
        square = square + fast(turned_high, high, NN) + (fast(turned_high, low, NN) + fast(turned_low, high, NN))
    for i in range(4):
        r, h = i // 2, i % 2
        square_ref[:, i, :] = square[r * LANES : (r + 1) * LANES, h * LANES : (h + 1) * LANES]
    unknowns = select_ref.shape[1]
    rows = lax.broadcasted_iota(jnp.int32, (devices, unknowns), 0)
    columns = lax.broadcasted_iota(jnp.int32, (devices, unknowns), 1)
    each = unknowns // devices
    repeat = jnp.where(columns // each == rows, 1.0, 0.0).astype(bf16)
    owner = jnp.broadcast_to(owner_ref[...].astype(f32), (8, devices)).astype(bf16)
    owner = fast(owner, repeat, NN)[:1]
    select_ref[...] = jnp.where(owner == rows.astype(f32), 1.0, 0.0).astype(bf16)


def late_body(local_ref, z_ref, ghost_ref, modes_ref, late_ref):
    z = z_ref[...]
    ghost = ghost_ref[...][:, NC:]
    late_ref[0] = local_ref[0] + dot(z[:, :NC], modes_ref[0, NC:], NN) + dot(ghost, modes_ref[0, :NC], NN)
    late_ref[1] = local_ref[1] + dot(z, modes_ref[1], NN)


def out_body(
    green_ref, image_ref, late_ref, gains_ref, disp_ref, vel_ref, acc_ref, disp_out_ref, vel_out_ref
):
    kappa_1, kappa_2 = gains_ref[0], gains_ref[1]
    case = lax.broadcasted_iota(jnp.int32, kappa_1.shape, 0)
    lane = lax.broadcasted_iota(jnp.int32, kappa_1.shape, 1)
    kappa_1 = jnp.sum(jnp.where(case == lane, kappa_1, 0.0), axis=1, keepdims=True)
    kappa_2 = jnp.sum(jnp.where(case == lane, kappa_2, 0.0), axis=1, keepdims=True)
    for s in range(2):
        disp = green_ref[s] - kappa_1 * image_ref[s] + kappa_2 * late_ref[s]
        vel, acc = vel_ref[:, s, :], acc_ref[:, s, :]
        accel = (
            (disp - disp_ref[:, s, :]) * (1.0 / (newmark_beta * time_step * time_step))
            - vel * (1.0 / (newmark_beta * time_step))
            - (0.5 / newmark_beta - 1.0) * acc
        )
        disp_out_ref[:, s, :] = disp
        vel_out_ref[:, s, :] = vel + time_step * ((1.0 - newmark_gamma) * acc + newmark_gamma * accel)


def coarse_product(assembled_ref, parts_ref):
    cases = assembled_ref.shape[0]
    high, low = two_parts(assembled_ref[...])
    both = fast(jnp.concatenate([high, low], axis=0), parts_ref[...], NT)
    both = both[:cases] + both[cases:]
    return both[:, :HALF] + both[:, HALF:]


def assemble_packed(got_ref, assembled_ref, slots):
    tiles = assembled_ref.shape[1] // LANES
    lane = lax.broadcasted_iota(jnp.int32, (4, LANES), 1)
    lower = lane < HALF
    for m in range(tiles):
        even, odd = 2 * slots * m, 2 * slots * m + slots
        following = 2 * slots * ((m + 1) % tiles) + 2
        previous = 2 * slots * ((m - 1) % tiles) + slots + 2
        extra_even, extra_odd = got_ref[following], got_ref[previous]
        top = got_ref[even] + got_ref[odd] + jnp.where(lower, extra_odd, extra_even)
        turned = pltpu.roll(jnp.where(lower, extra_even, extra_odd), HALF, 1)
        bottom = got_ref[even + 1] + got_ref[odd + 1] + turned
        assembled_ref[0:4, m * LANES : (m + 1) * LANES] = top
        assembled_ref[4:8, m * LANES : (m + 1) * LANES] = bottom


def assemble_first(got_ref, assembled_ref):
    tiles = assembled_ref.shape[1] // LANES
    lane = lax.broadcasted_iota(jnp.int32, (8, LANES), 1)
    for m in range(tiles):
        following = (2 * m + 2) % (2 * tiles)
        own = got_ref[2 * m + 1] + jnp.where(lane < HALF, got_ref[2 * m], 0.0)
        assembled_ref[:, m * LANES : (m + 1) * LANES] = own + jnp.where(
            lane >= LANES - NC, got_ref[following], 0.0
        )


def owned_terms(device_ref, assembled_ref, z):
    device = device_ref[0]
    tile = assembled_ref[:, pl.ds(pl.multiple_of((device // 2) * LANES, LANES), LANES)]
    even = lax.rem(device, 2) == 0
    return jnp.where(even, tile[:, :HALF], tile[:, HALF:]) * z


def send_blocks(z, coupling_ref, local_ref, pieces_ref, slots, riding_ref=None):
    blocks = local_ref[...] + dot(z, coupling_ref[...], NN)
    main, extra = blocks[:, :LANES], blocks[:, LANES:]
    turned = pltpu.roll(extra, HALF, 1)
    packed = extra[0:4] + turned[4:8]
    for d in range(pieces_ref.shape[0] // slots):
        pieces_ref[slots * d] = main[0:4]
        pieces_ref[slots * d + 1] = main[4:8]
        pieces_ref[slots * d + 2] = packed
        if riding_ref is not None:
            pieces_ref[slots * d + 3] = riding_ref[d]


def first_body(got_ref, parts_ref, coupling_ref, local_ref, pieces_ref, z_ref, assembled_ref):
    assemble_first(got_ref, assembled_ref)
    z = coarse_product(assembled_ref, parts_ref)
    z_ref[...] = z
    send_blocks(z, coupling_ref, local_ref, pieces_ref, 3)


def second_body(
    device_ref, got_ref, parts_ref, coupling_ref, local_ref, square_ref, pieces_ref, z_ref, terms_ref, assembled_ref
):
    assemble_packed(got_ref, assembled_ref, 3)
    z = coarse_product(assembled_ref, parts_ref)
    z_ref[...] = z
    terms_ref[...] = owned_terms(device_ref, assembled_ref, z)
    send_blocks(z, coupling_ref, local_ref, pieces_ref, 4, square_ref)


def join_second_body(
    device_ref, got_ref, parts_ref, coupling_ref, square_ref, mine_ref, from_left_ref, from_right_ref, before_ref,
    modes_ref, right_ref, rr_ref, to_blocks_ref,
    pieces_ref, z_ref, terms_ref, field_ref, local_ref, sums_ref, assembled_ref, blocks_ref,
):
    join_body(
        mine_ref, from_left_ref, from_right_ref, before_ref, modes_ref, right_ref, rr_ref, to_blocks_ref,
        field_ref, local_ref, blocks_ref, sums_ref,
    )
    second_body(
        device_ref, got_ref, parts_ref, coupling_ref, blocks_ref, square_ref, pieces_ref, z_ref, terms_ref, assembled_ref
    )


def join_third_body(
    device_ref, got_ref, parts_ref, mine_ref, from_left_ref, from_right_ref, before_ref,
    modes_ref, right_ref, rr_ref, to_blocks_ref, select_ref, sums_2_ref, terms_ref, early_ref,
    sent_ref, z_ref, field_ref, local_ref, assembled_ref, blocks_ref, sums_3_ref,
):
    join_body(
        mine_ref, from_left_ref, from_right_ref, before_ref, modes_ref, right_ref, rr_ref, to_blocks_ref,
        field_ref, local_ref, blocks_ref, sums_3_ref,
    )
    third_body(
        device_ref, got_ref, parts_ref, local_ref, modes_ref, right_ref, select_ref, sums_2_ref, sums_3_ref, terms_ref,
        field_ref, early_ref, sent_ref, z_ref, assembled_ref,
    )


def choose_rows(select_ref, rows):
    high, middle, low = three_parts(rows)
    select = select_ref[...]
    return fast(select, high, NT) + fast(select, middle, NT) + fast(select, low, NT)


def by_offset(field):
    lane = lax.broadcasted_iota(jnp.int32, field.shape, 1)
    return [jnp.where(lane % 4 == o, field, 0.0) for o in range(4)]


def early_body(select_ref, green_ref, chosen_ref):
    rows = by_offset(green_ref[0]) + by_offset(green_ref[1])
    rows.append(jnp.zeros((HALF, green_ref.shape[2]), f32))
    chosen_ref[...] = choose_rows(select_ref, jnp.concatenate(rows, axis=0))


def third_body(
    device_ref, got_ref, parts_ref, local_ref, modes_ref, right_ref, select_ref, sums_2_ref, sums_3_ref, terms_ref,
    image_ref, early_ref,
    sent_ref, z_ref, assembled_ref,
):
    assemble_packed(got_ref, assembled_ref, 4)
    z = coarse_product(assembled_ref, parts_ref)
    z_ref[...] = z
    square = got_ref[3]
    for d in range(1, got_ref.shape[0] // 4):
        square = square + got_ref[4 * d + 3]
    y_0 = local_ref[0] + dot(z[:, :NC], modes_ref[0, NC:], NN)
    y_1 = local_ref[1] + dot(z, modes_ref[1], NN)
    y_2 = dot(z[:, NC:], right_ref[0, :NC], NN)
    rows = by_offset(y_0) + by_offset(y_1) + by_offset(y_2)
    rows.append(jnp.zeros((32, y_0.shape[1]), f32))
    late = choose_rows(select_ref, jnp.concatenate(rows, axis=0))
    curvature = jnp.sum(owned_terms(device_ref, assembled_ref, z), axis=1, keepdims=True)
    lane = lax.broadcasted_iota(jnp.int32, (8, LANES), 1)
    case = lax.broadcasted_iota(jnp.int32, (8, LANES), 0)
    parts = [
        sums_2_ref[:, 0:1],
        sums_2_ref[:, 1:2] + jnp.sum(terms_ref[...], axis=1, keepdims=True),
        sums_3_ref[:, 0:1],
        sums_3_ref[:, 1:2] + curvature,
    ]
    placed = jnp.zeros((8, LANES), f32)
    for k in range(4):
        placed = placed + jnp.where(lane == 96 + 8 * k + case, parts[k], 0.0)
    late = late + jnp.sum(placed, axis=0, keepdims=True)
    rows = [jnp.zeros((HALF, y_0.shape[1]), f32)] + by_offset(image_ref[0]) + by_offset(image_ref[1])
    sent_ref[:, 0, 0, :] = early_ref[...] + choose_rows(select_ref, jnp.concatenate(rows, axis=0))
    sent_ref[:, 0, 1, :] = late
    sent_ref[:, 1] = jnp.broadcast_to(square[None, 0:2], (late.shape[0], 2, LANES))
    sent_ref[:, 2] = jnp.broadcast_to(square[None, 2:4], (late.shape[0], 2, LANES))


def project_body(got_ref, basis_ref, part_ref, rows_ref, gains_ref):
    early, late = got_ref[:, 0, 0, :], got_ref[:, 0, 1, :]
    sums = jnp.broadcast_to(jnp.sum(late, axis=0, keepdims=True), (8, LANES))
    lane = lax.broadcasted_iota(jnp.int32, (8, LANES), 1)
    bb, bf, ff, fff = (pltpu.roll(sums, 32 - 8 * k, 1) for k in range(4))
    good = lane < 8
    bb, bf = jnp.where(good, bb, 1.0), jnp.where(good, bf, 1.0)
    ff, fff = jnp.where(good, ff, 2.0), jnp.where(good, fff, 8.0)
    alpha_0 = bb / bf
    norm_1 = bb - 2.0 * alpha_0 * bf + alpha_0 * alpha_0 * ff
    gain = 1.0 + norm_1 / bb
    curvature = gain * gain * bf - 2.0 * gain * alpha_0 * ff + alpha_0 * alpha_0 * fff
    alpha_1 = norm_1 / curvature
    kappas = []
    for kappa in (alpha_0 + alpha_1 * gain, alpha_1 * alpha_0):
        kappa = jnp.where(good, kappa, 0.0)
        for shift in (8, 16, 32, 64):
            kappa = kappa + pltpu.roll(kappa, shift, 1)
        kappas.append(kappa)
    gains_ref[0], gains_ref[1] = kappas[0], kappas[1]
    kappa_1, kappa_2 = kappas[0][:1], kappas[1][:1]
    wide = lax.broadcasted_iota(jnp.int32, late.shape, 1)
    extra = pltpu.roll(pltpu.roll(late, HALF, 1), 1, 0)
    last = late + jnp.where(wide < NC, extra, 0.0)
    rows = early - kappa_1 * pltpu.roll(early, HALF, 1) + kappa_2 * last
    turned = jnp.transpose(rows)
    snapshots = jnp.concatenate([turned[8 * j : 8 * j + 8] for j in range(8)], axis=1)
    rows_ref[...] = snapshots
    high, low = two_parts(snapshots)
    both = jnp.concatenate([high, low], axis=0)
    count = snapshots.shape[1]
    product = fast(both, basis_ref[:count], NN) + fast(both, basis_ref[count:], NN)
    gram = dot(snapshots, jnp.concatenate([snapshots, jnp.zeros((LANES - 8, count), f32)], axis=0), NT)
    part = jnp.concatenate([product[:8] + product[8:], gram], axis=1)
    for d in range(part_ref.shape[0]):
        part_ref[d] = part


def finish_body(got_ref, square_ref, basis_ref, rows_ref, columns_ref, projection_ref, factor_ref, *, scale):
    count = got_ref.shape[0]
    reduced = got_ref[0]
    for i in range(1, count):
        reduced = reduced + got_ref[i]
    rank = reduced.shape[1] - LANES
    coefficients = reduced[:, :rank]
    projection_ref[...] = coefficients
    low_rows, high_rows = coefficients[:, :LANES], coefficients[:, LANES:]
    squares = [square_ref[:, 1 + i // 2, i % 2, :] for i in range(4)]
    image = jnp.concatenate(
        [
            dot(low_rows, squares[0], NN) + dot(high_rows, squares[2], NN),
            dot(low_rows, squares[1], NN) + dot(high_rows, squares[3], NN),
        ],
        axis=1,
    )
    gap = image - 2.0 * coefficients
    blank = jnp.zeros((LANES - 8, rank), f32)
    gram = reduced[:, rank:] + dot(coefficients, jnp.concatenate([gap, blank], axis=0), NT)
    row = lax.broadcasted_iota(jnp.int32, (8, LANES), 0)
    lane = lax.broadcasted_iota(jnp.int32, (8, LANES), 1)
    gram = jnp.where(lane < 8, gram, 0.0)
    work = gram + jnp.where(lane == row + 8, 1.0, 0.0)
    upper = jnp.zeros((8, LANES), f32)
    for j in range(8):
        pivot = jnp.sum(jnp.where((row == j) & (lane == j), work, 0.0), axis=(0, 1), keepdims=True)
        line = jnp.sum(jnp.where(row == j, work, 0.0), axis=0, keepdims=True) / jnp.sqrt(pivot)
        upper = jnp.where(row == j, line, upper)
        column = jnp.sum(jnp.where(lane == j, work, 0.0), axis=1, keepdims=True) / jnp.sqrt(pivot)
        work = jnp.where(row > j, work - column * line, work)
    factor_ref[...] = jnp.where((lane >= row) & (lane < 8), upper, 0.0) * (1.0 / scale)
    inverse = pltpu.roll(upper, LANES - 8, 1)
    inverse = jnp.where((lane <= row) & (lane < 8), inverse, 0.0)[:, :8]
    high, low = two_parts(coefficients)
    total = rows_ref.shape[1]
    both = jnp.concatenate([high, low], axis=0)
    product = fast(both, basis_ref[:total], NT) + fast(both, basis_ref[total:], NT)
    remainder = rows_ref[...] - (product[:8] + product[8:])
    columns = dot(inverse, remainder, NN) * scale
    for t in range(8):
        index = 16 * t + lane // 8
        out = jnp.zeros((8, LANES), f32)
        for j in range(8):
            picked = jnp.take_along_axis(columns[:, j * LANES : (j + 1) * LANES], index, axis=1)
            out = jnp.where(lane % 8 == j, picked, out)
        columns_ref[:, t * LANES : (t + 1) * LANES] = out


def shards(
    rr_inverse,
    corner_modes,
    coarse_inverse,
    inertia,
    disp_now,
    vel_now,
    acc_now,
    load_next,
    basis_rows,
    piece_owner,
):
    case_count, _, unknowns = disp_now.shape
    devices = lax.axis_size(AXES)
    coarse_total = coarse_inverse.shape[1]
    rank = basis_rows.shape[1]
    last = unknowns - NI
    device = lax.axis_index(AXES).reshape(1).astype(jnp.int32)
    pair = ((2, case_count, unknowns),)
    z_shape = ((case_count, 2 * NC),)
    blocks_shape = ((case_count, 2 * LANES),)
    assembled = [pltpu.VMEM((case_count, coarse_total), f32)]

    start, right_side = call(start_body, [((devices, case_count, LANES),), pair], [SMEM] + [VMEM] * 6, grant=60 * 1024)(
        device, load_next, inertia, disp_now, vel_now, acc_now, corner_modes
    )
    got_1 = exchange(start)
    left_edge = shifted(corner_modes[1, :, last:], 1)
    right_modes = shifted(corner_modes, -1)
    coarse_parts, local_0 = call(pre_body, [((4 * NC, coarse_total), bf16), pair], [VMEM] * 3, flops=1 << 26)(
        coarse_inverse, right_side, rr_inverse
    )
    blocks_0, coupling, to_blocks = call(
        couple_body, [blocks_shape, ((2 * NC, 2 * LANES),), ((2 * LANES, 4 * NI),)], [SMEM] + [VMEM] * 4, flops=1 << 26
    )(device, corner_modes, right_modes, left_edge, local_0)

    def finish(local, z):
        mine, to_right, to_left = call(
            edge_body, [pair, ((case_count, 2 * NI),), ((case_count, NI),)], [VMEM] * 3, flops=1 << 20
        )(local, z, corner_modes)
        from_left = shifted(to_right, 1)
        from_right = shifted(to_left, -1)
        return mine, from_left, from_right, z, corner_modes, right_modes, rr_inverse, to_blocks

    blocks_scratch = pltpu.VMEM((case_count, 2 * LANES), f32)
    sums_shape = (case_count, LANES)
    pieces, z_0 = call(first_body, [((3 * devices, 4, LANES),), z_shape], [VMEM] * 4, assembled, flops=1 << 24)(
        got_1, coarse_parts, coupling, blocks_0
    )
    got_2 = exchange(pieces)
    basis_parts, square, select = call(
        prep_body,
        [((2 * basis_rows.shape[0], rank), bf16), ((devices, 4, LANES),), ((devices, unknowns), bf16)],
        [VMEM, VMEM, VMEM],
        flops=1 << 26,
        grant=60 * 1024,
    )(basis_rows.reshape(devices, -1, rank), piece_owner.reshape(1, devices), z_0)
    pieces, z_1, terms_1, green, local_1, sums_2 = call(
        join_second_body,
        [((4 * devices, 4, LANES),), z_shape, z_shape, pair, pair, (sums_shape,)],
        [SMEM] + [VMEM] * 12,
        assembled + [blocks_scratch],
        flops=1 << 26,
        grant=60 * 1024,
    )(device, got_2, coarse_parts, coupling, square, *finish(local_0, z_0))
    got_3 = exchange(pieces)
    (early,) = call(early_body, [((devices, LANES),)], [VMEM] * 2, flops=1 << 24)(select, green)
    sent, z_2, image_1, local_2 = call(
        join_third_body,
        [((devices, 3, 2, LANES),), z_shape, pair, pair],
        [SMEM] + [VMEM] * 14,
        assembled + [blocks_scratch, pltpu.VMEM(sums_shape, f32)],
        flops=1 << 26,
        grant=60 * 1024,
    )(device, got_3, coarse_parts, *finish(local_1, z_1), select, sums_2, terms_1, early)
    got_4 = exchange(sent)
    ghost = shifted(z_2, 1)
    (late,) = call(late_body, [pair], [VMEM] * 4, flops=1 << 20)(local_2, z_2, ghost, corner_modes)
    part, snapshots, gains = call(
        project_body,
        [
            ((lax.axis_size(NEAR), case_count, rank + LANES),),
            ((case_count, basis_rows.shape[0]),),
            ((2, case_count, LANES),),
        ],
        [VMEM] * 2,
        flops=1 << 24,
    )(got_4, basis_parts)
    near = exchange(part, NEAR)
    near = near.sum(axis=0)
    got_5 = to_everyone(near, FAR)
    disp_new, vel_new = call(
        out_body, [(disp_now.shape,), (disp_now.shape,)], [VMEM] * 7, flops=1 << 22
    )(green, image_1, late, gains, disp_now, vel_now, acc_now)
    scale = math.sqrt(basis_rows.shape[0] * devices)
    new_columns, projection, factor = call(
        functools.partial(finish_body, scale=scale),
        [((case_count, basis_rows.shape[0]),), ((case_count, rank),), ((case_count, LANES),)],
        [VMEM] * 4,
        flops=1 << 24,
    )(got_5, got_4, basis_parts, snapshots)
    return (disp_new, vel_new, projection.T, factor[:, :case_count], new_columns)


def solution(mesh):
    finer = Mesh(
        mesh.devices.reshape(4, 4, 2, mesh.shape["grp"]), ("sub_0", "sub_1", "sub_2", "grp")
    )
    placed = (
        P(AXES, None, None),
        P(AXES, None, None),
        P(AXES, None),
        P(AXES, None),
        P(None, AXES, None),
        P(None, AXES, None),
        P(None, AXES, None),
        P(None, AXES, None),
        P(AXES, None),
        P(),
    )

    return jax.shard_map(
        shards,
        mesh=finer,
        in_specs=placed,
        out_specs=(P(None, AXES, None), P(None, AXES, None), P(), P(), P(None, AXES)),
        check_vma=False,
    )
```

```python
import functools
import math

import jax
import jax.numpy as jnp
from jax import lax
from jax.experimental import pallas as pl
from jax.experimental.pallas import tpu as pltpu
from jax.sharding import Mesh
from jax.sharding import PartitionSpec as P

NC = 32
NI = 128
LANES = 128
HALF = 64
AXES = ("sub_0", "sub_1", "sub_2", "grp")
FAR, NEAR = ("sub_0", "sub_1"), ("sub_2", "grp")

highest = lax.Precision.HIGHEST
time_step = 0.5
newmark_beta = 0.25
newmark_gamma = 0.5
f32, bf16 = jnp.float32, jnp.bfloat16
NT = (((1,), (1,)), ((), ()))
NN = (((1,), (0,)), ((), ()))
VMEM = pl.BlockSpec(memory_space=pltpu.VMEM)
SMEM = pl.BlockSpec(memory_space=pltpu.SMEM)


def exchange(pieces, axes=AXES):
    return lax.all_to_all(pieces, axes, split_axis=0, concat_axis=0, tiled=True)


def to_everyone(array, axes=AXES):
    return exchange(jnp.broadcast_to(array, (lax.axis_size(axes), *array.shape)), axes)


def shifted(array, by):
    count = lax.axis_size(AXES)
    return lax.ppermute(array, AXES, [(i, (i + by) % count) for i in range(count)])


def dot(a, b, dims):
    return lax.dot_general(a, b, dims, precision=highest, preferred_element_type=f32)


def fast(a, b, dims):
    return lax.dot_general(a, b, dims, preferred_element_type=f32)


def call(body, outs, ins, scratch=(), flops=0, grant=16000):
    return pl.pallas_call(
        body,
        out_shape=[jax.ShapeDtypeStruct(shape, f32 if len(rest) == 0 else rest[0]) for shape, *rest in outs],
        in_specs=ins,
        out_specs=[VMEM] * len(outs),
        scratch_shapes=list(scratch),
        compiler_params=pltpu.CompilerParams(vmem_limit_bytes=grant << 10),
        cost_estimate=pl.CostEstimate(flops=flops, bytes_accessed=1 << 20, transcendentals=0),
    )


def two_parts(x):
    high = x.astype(bf16)
    return high, (x - high.astype(f32)).astype(bf16)


def three_parts(x):
    high = x.astype(bf16)
    rest = x - high.astype(f32)
    middle = rest.astype(bf16)
    return high, middle, (rest - middle.astype(f32)).astype(bf16)


def start_body(device_ref, load_ref, inertia_ref, disp_ref, vel_ref, acc_ref, modes_ref, start_ref, right_ref, to_left_ref, to_right_ref):
    blank = jnp.zeros((NC, modes_ref.shape[2]), f32)
    fields = []
    for s in range(2):
        moved = disp_ref[:, s, :] + time_step * vel_ref[:, s, :]
        moved = moved + (0.5 - newmark_beta) * time_step * time_step * acc_ref[:, s, :]
        fields.append(load_ref[:, s, :] + inertia_ref[s : s + 1] * moved)
        right_ref[s] = fields[s]
    part_0 = jnp.concatenate([modes_ref[0, NC:], blank, blank, modes_ref[0, :NC]], axis=0)
    part_1 = jnp.concatenate([modes_ref[1, :NC], modes_ref[1, NC:], blank, blank], axis=0)
    blocks = dot(fields[0], part_0, NT) + dot(fields[1], part_1, NT)
    even = lax.rem(device_ref[0], 2) == 0
    blocks = jnp.where(even, blocks, pltpu.roll(blocks, HALF, 1))
    for d in range(start_ref.shape[0]):
        start_ref[d] = blocks
    unknowns = modes_ref.shape[2]
    to_left_ref[:, :unknowns] = modes_ref[0]
    to_left_ref[:, unknowns:] = modes_ref[1, :, :NI]
    to_right_ref[...] = modes_ref[1, :, unknowns - NI :]


def pre_body(matrix_ref, right_ref, rr_ref, parts_ref, local_ref):
    rows = matrix_ref.shape[0]
    high, low = two_parts(matrix_ref[...])
    parts_ref[:rows] = high
    parts_ref[rows:] = low
    for s in range(2):
        local_ref[s] = dot(right_ref[s], rr_ref[s], NN)


def couple_body(device_ref, modes_ref, right_ref, left_ref, local_ref, blocks_ref, coupling_ref, to_blocks_ref):
    last = modes_ref.shape[2] - NI
    even = jnp.where(lax.rem(device_ref[0], 2) == 0, 1, 0)
    first, final = [modes_ref[s, :, :NI] for s in range(2)], [modes_ref[s, :, last:] for s in range(2)]
    unknowns = modes_ref.shape[2]
    right_first, right_final = [right_ref[:, :NI], right_ref[:, unknowns:]], right_ref[:, last:unknowns]
    left = left_ref[...]
    rows = [
        {0: left[:NC]},
        {0: left[NC:] - first[0][:NC], 1: final[0][:NC]},
        {0: -first[0][NC:], 1: final[0][NC:] - first[1][:NC], 2: final[1][:NC]},
        {1: -first[1][NC:], 2: final[1][NC:] - right_first[0][:NC], 3: right_final[:NC]},
        {2: -right_first[0][NC:], 3: right_final[NC:] - right_first[1][:NC]},
        {3: -right_first[1][NC:]},
    ]
    to_blocks_ref[...] = jnp.zeros(to_blocks_ref.shape, f32)
    for i, parts in enumerate(rows):
        at = pl.multiple_of(lax.rem(i * NC + 192 * even, 256), NC)
        for k, values in parts.items():
            to_blocks_ref[pl.ds(at, NC), k * NI : (k + 1) * NI] = values
    blank = jnp.zeros((NC, modes_ref.shape[2]), f32)
    unit_0 = jnp.concatenate([modes_ref[0, NC:], blank], axis=0)
    unit_1 = modes_ref[1]
    unit_2 = jnp.concatenate([blank, right_ref[:NC, :unknowns]], axis=0)
    jumps = jnp.concatenate(
        [-unit_0[:, :NI], unit_0[:, last:] - unit_1[:, :NI], unit_1[:, last:] - unit_2[:, :NI], unit_2[:, last:]], axis=1
    )
    coupling_ref[...] = dot(jumps, to_blocks_ref[...], NT)
    blocks_ref[...] = own_blocks(local_ref[0], local_ref[1], to_blocks_ref)


def own_blocks(field_0, field_1, to_blocks_ref):
    last = field_0.shape[1] - NI
    jumps = [-field_0[:, :NI], field_0[:, last:] - field_1[:, :NI], field_1[:, last:]]
    return dot(jnp.concatenate(jumps, axis=1), to_blocks_ref[:, : 3 * NI], NT)


def edge_body(local_ref, z_ref, modes_ref, mine_ref, to_right_ref, to_left_ref):
    last = local_ref.shape[2] - NI
    z = z_ref[...]
    mine_0 = local_ref[0] + dot(z[:, :NC], modes_ref[0, NC:], NN)
    mine_1 = local_ref[1] + dot(z, modes_ref[1], NN)
    mine_ref[0], mine_ref[1] = mine_0, mine_1
    to_left_ref[...] = mine_0[:, :NI]
    to_right_ref[:, :NI] = mine_1[:, last:]
    to_right_ref[:, NI:] = jnp.concatenate([z, z], axis=1)


def join_body(
    mine_ref, from_left_ref, from_right_ref, z_ref, modes_ref, right_ref, rr_ref, to_blocks_ref,
    field_ref, local_ref, blocks_ref, sums_ref,
):
    last = mine_ref.shape[2] - NI
    mine_1 = mine_ref[1]
    ghost = from_left_ref[:, NI : NI + 2 * NC]
    mine_0 = mine_ref[0] + dot(ghost[:, NC:], modes_ref[0, :NC], NN)
    field_ref[0], field_ref[1] = mine_0, mine_1
    jump_a = from_left_ref[:, :NI] - mine_0[:, :NI]
    jump_b = mine_0[:, last:] - mine_1[:, :NI]
    jump_c = mine_1[:, last:] - (from_right_ref[...] + dot(z_ref[:, NC:], right_ref[:NC, :NI], NN))
    inner = jnp.zeros((mine_1.shape[0], 1), f32)
    outs = []
    for s, (first, final) in enumerate([(-jump_a, jump_b), (-jump_b, jump_c)]):
        out = dot(first, rr_ref[s, :NI], NN) + dot(final, rr_ref[s, last:], NN)
        local_ref[s] = out
        inner = inner + jnp.sum(out[:, :NI] * first + out[:, last:] * final, axis=1, keepdims=True)
        outs.append(out)
    blocks_ref[...] = own_blocks(outs[0], outs[1], to_blocks_ref)
    square = jnp.sum(jump_b * jump_b + jump_c * jump_c, axis=1, keepdims=True)
    lane = lax.broadcasted_iota(jnp.int32, sums_ref.shape, 1)
    sums_ref[...] = jnp.where(lane == 0, square, 0.0) + jnp.where(lane == 1, inner, 0.0)


def prep_body(basis_ref, owner_ref, after_ref, parts_ref, square_ref, select_ref):
    devices, width, rank = basis_ref.shape
    total = devices * width
    square = jnp.zeros((rank, rank), f32)
    for j in range(width):
        rows = basis_ref[:, j, :]
        high, low = two_parts(rows)
        parts_ref[j * devices : (j + 1) * devices] = high
        parts_ref[total + j * devices : total + (j + 1) * devices] = low
        turned_high, turned_low = two_parts(jnp.transpose(rows))
        square = square + fast(turned_high, high, NN) + (fast(turned_high, low, NN) + fast(turned_low, high, NN))
    for i in range(4):
        r, h = i // 2, i % 2
        square_ref[:, i, :] = square[r * LANES : (r + 1) * LANES, h * LANES : (h + 1) * LANES]
    unknowns = select_ref.shape[1]
    rows = lax.broadcasted_iota(jnp.int32, (devices, unknowns), 0)
    columns = lax.broadcasted_iota(jnp.int32, (devices, unknowns), 1)
    each = unknowns // devices
    repeat = jnp.where(columns // each == rows, 1.0, 0.0).astype(bf16)
    owner = jnp.broadcast_to(owner_ref[...].astype(f32), (8, devices)).astype(bf16)
    owner = fast(owner, repeat, NN)[:1]
    select_ref[...] = jnp.where(owner == rows.astype(f32), 1.0, 0.0).astype(bf16)


def late_body(local_ref, z_ref, ghost_ref, modes_ref, late_ref):
    z = z_ref[...]
    ghost = ghost_ref[...][:, NC:]
    late_ref[0] = local_ref[0] + dot(z[:, :NC], modes_ref[0, NC:], NN) + dot(ghost, modes_ref[0, :NC], NN)
    late_ref[1] = local_ref[1] + dot(z, modes_ref[1], NN)


def out_body(
    green_ref, image_ref, late_ref, gains_ref, disp_ref, vel_ref, acc_ref, disp_out_ref, vel_out_ref
):
    kappa_1, kappa_2 = gains_ref[0], gains_ref[1]
    case = lax.broadcasted_iota(jnp.int32, kappa_1.shape, 0)
    lane = lax.broadcasted_iota(jnp.int32, kappa_1.shape, 1)
    kappa_1 = jnp.sum(jnp.where(case == lane, kappa_1, 0.0), axis=1, keepdims=True)
    kappa_2 = jnp.sum(jnp.where(case == lane, kappa_2, 0.0), axis=1, keepdims=True)
    for s in range(2):
        disp = green_ref[s] - kappa_1 * image_ref[s] + kappa_2 * late_ref[s]
        vel, acc = vel_ref[:, s, :], acc_ref[:, s, :]
        accel = (
            (disp - disp_ref[:, s, :]) * (1.0 / (newmark_beta * time_step * time_step))
            - vel * (1.0 / (newmark_beta * time_step))
            - (0.5 / newmark_beta - 1.0) * acc
        )
        disp_out_ref[:, s, :] = disp
        vel_out_ref[:, s, :] = vel + time_step * ((1.0 - newmark_gamma) * acc + newmark_gamma * accel)


def coarse_product(assembled_ref, parts_ref):
    cases = assembled_ref.shape[0]
    high, low = two_parts(assembled_ref[...])
    both = fast(jnp.concatenate([high, low], axis=0), parts_ref[...], NT)
    both = both[:cases] + both[cases:]
    return both[:, :HALF] + both[:, HALF:]


def assemble_packed(got_ref, assembled_ref, slots):
    tiles = assembled_ref.shape[1] // LANES
    lane = lax.broadcasted_iota(jnp.int32, (4, LANES), 1)
    lower = lane < HALF
    for m in range(tiles):
        even, odd = 2 * slots * m, 2 * slots * m + slots
        following = 2 * slots * ((m + 1) % tiles) + 2
        previous = 2 * slots * ((m - 1) % tiles) + slots + 2
        extra_even, extra_odd = got_ref[following], got_ref[previous]
        top = got_ref[even] + got_ref[odd] + jnp.where(lower, extra_odd, extra_even)
        turned = pltpu.roll(jnp.where(lower, extra_even, extra_odd), HALF, 1)
        bottom = got_ref[even + 1] + got_ref[odd + 1] + turned
        assembled_ref[0:4, m * LANES : (m + 1) * LANES] = top
        assembled_ref[4:8, m * LANES : (m + 1) * LANES] = bottom


def assemble_first(got_ref, assembled_ref):
    tiles = assembled_ref.shape[1] // LANES
    lane = lax.broadcasted_iota(jnp.int32, (8, LANES), 1)
    for m in range(tiles):
        following = (2 * m + 2) % (2 * tiles)
        own = got_ref[2 * m + 1] + jnp.where(lane < HALF, got_ref[2 * m], 0.0)
        assembled_ref[:, m * LANES : (m + 1) * LANES] = own + jnp.where(
            lane >= LANES - NC, got_ref[following], 0.0
        )


def owned_terms(device_ref, assembled_ref, z):
    device = device_ref[0]
    tile = assembled_ref[:, pl.ds(pl.multiple_of((device // 2) * LANES, LANES), LANES)]
    even = lax.rem(device, 2) == 0
    return jnp.where(even, tile[:, :HALF], tile[:, HALF:]) * z


def send_blocks(z, coupling_ref, local_ref, pieces_ref, slots, riding_ref=None):
    blocks = local_ref[...] + dot(z, coupling_ref[...], NN)
    main, extra = blocks[:, :LANES], blocks[:, LANES:]
    turned = pltpu.roll(extra, HALF, 1)
    packed = extra[0:4] + turned[4:8]
    for d in range(pieces_ref.shape[0] // slots):
        pieces_ref[slots * d] = main[0:4]
        pieces_ref[slots * d + 1] = main[4:8]
        pieces_ref[slots * d + 2] = packed
        if riding_ref is not None:
            pieces_ref[slots * d + 3] = riding_ref[d]


def first_body(got_ref, parts_ref, coupling_ref, local_ref, pieces_ref, z_ref, assembled_ref):
    assemble_first(got_ref, assembled_ref)
    z = coarse_product(assembled_ref, parts_ref)
    z_ref[...] = z
    send_blocks(z, coupling_ref, local_ref, pieces_ref, 3)


def second_body(
    device_ref, got_ref, parts_ref, coupling_ref, local_ref, square_ref, pieces_ref, z_ref, terms_ref, assembled_ref
):
    assemble_packed(got_ref, assembled_ref, 3)
    z = coarse_product(assembled_ref, parts_ref)
    z_ref[...] = z
    terms_ref[...] = owned_terms(device_ref, assembled_ref, z)
    send_blocks(z, coupling_ref, local_ref, pieces_ref, 4, square_ref)


def join_second_body(
    device_ref, got_ref, parts_ref, coupling_ref, square_ref, mine_ref, from_left_ref, from_right_ref, before_ref,
    modes_ref, right_ref, rr_ref, to_blocks_ref,
    pieces_ref, z_ref, terms_ref, field_ref, local_ref, sums_ref, assembled_ref, blocks_ref,
):
    join_body(
        mine_ref, from_left_ref, from_right_ref, before_ref, modes_ref, right_ref, rr_ref, to_blocks_ref,
        field_ref, local_ref, blocks_ref, sums_ref,
    )
    second_body(
        device_ref, got_ref, parts_ref, coupling_ref, blocks_ref, square_ref, pieces_ref, z_ref, terms_ref, assembled_ref
    )


def join_third_body(
    device_ref, got_ref, parts_ref, mine_ref, from_left_ref, from_right_ref, before_ref,
    modes_ref, right_ref, rr_ref, to_blocks_ref, select_ref, sums_2_ref, terms_ref, early_ref,
    sent_ref, z_ref, field_ref, local_ref, assembled_ref, blocks_ref, sums_3_ref,
):
    join_body(
        mine_ref, from_left_ref, from_right_ref, before_ref, modes_ref, right_ref, rr_ref, to_blocks_ref,
        field_ref, local_ref, blocks_ref, sums_3_ref,
    )
    third_body(
        device_ref, got_ref, parts_ref, local_ref, modes_ref, right_ref, select_ref, sums_2_ref, sums_3_ref, terms_ref,
        field_ref, early_ref, sent_ref, z_ref, assembled_ref,
    )


def choose_rows(select_ref, rows):
    high, middle, low = three_parts(rows)
    select = select_ref[...]
    return fast(select, high, NT) + fast(select, middle, NT) + fast(select, low, NT)


def by_offset(field):
    lane = lax.broadcasted_iota(jnp.int32, field.shape, 1)
    return [jnp.where(lane % 4 == o, field, 0.0) for o in range(4)]


def early_body(select_ref, green_ref, chosen_ref):
    rows = by_offset(green_ref[0]) + by_offset(green_ref[1])
    rows.append(jnp.zeros((HALF, green_ref.shape[2]), f32))
    chosen_ref[...] = choose_rows(select_ref, jnp.concatenate(rows, axis=0))


def third_body(
    device_ref, got_ref, parts_ref, local_ref, modes_ref, right_ref, select_ref, sums_2_ref, sums_3_ref, terms_ref,
    image_ref, early_ref,
    sent_ref, z_ref, assembled_ref,
):
    assemble_packed(got_ref, assembled_ref, 4)
    z = coarse_product(assembled_ref, parts_ref)
    z_ref[...] = z
    square = got_ref[3]
    for d in range(1, got_ref.shape[0] // 4):
        square = square + got_ref[4 * d + 3]
    y_0 = local_ref[0] + dot(z[:, :NC], modes_ref[0, NC:], NN)
    y_1 = local_ref[1] + dot(z, modes_ref[1], NN)
    y_2 = dot(z[:, NC:], right_ref[:NC, : modes_ref.shape[2]], NN)
    rows = by_offset(y_0) + by_offset(y_1) + by_offset(y_2)
    rows.append(jnp.zeros((32, y_0.shape[1]), f32))
    late = choose_rows(select_ref, jnp.concatenate(rows, axis=0))
    curvature = jnp.sum(owned_terms(device_ref, assembled_ref, z), axis=1, keepdims=True)
    lane = lax.broadcasted_iota(jnp.int32, (8, LANES), 1)
    case = lax.broadcasted_iota(jnp.int32, (8, LANES), 0)
    parts = [
        sums_2_ref[:, 0:1],
        sums_2_ref[:, 1:2] + jnp.sum(terms_ref[...], axis=1, keepdims=True),
        sums_3_ref[:, 0:1],
        sums_3_ref[:, 1:2] + curvature,
    ]
    placed = jnp.zeros((8, LANES), f32)
    for k in range(4):
        placed = placed + jnp.where(lane == 96 + 8 * k + case, parts[k], 0.0)
    late = late + jnp.sum(placed, axis=0, keepdims=True)
    rows = [jnp.zeros((HALF, y_0.shape[1]), f32)] + by_offset(image_ref[0]) + by_offset(image_ref[1])
    sent_ref[:, 0, 0, :] = early_ref[...] + choose_rows(select_ref, jnp.concatenate(rows, axis=0))
    sent_ref[:, 0, 1, :] = late
    sent_ref[:, 1] = jnp.broadcast_to(square[None, 0:2], (late.shape[0], 2, LANES))
    sent_ref[:, 2] = jnp.broadcast_to(square[None, 2:4], (late.shape[0], 2, LANES))


def project_body(got_ref, basis_ref, part_ref, rows_ref, gains_ref):
    early, late = got_ref[:, 0, 0, :], got_ref[:, 0, 1, :]
    sums = jnp.broadcast_to(jnp.sum(late, axis=0, keepdims=True), (8, LANES))
    lane = lax.broadcasted_iota(jnp.int32, (8, LANES), 1)
    bb, bf, ff, fff = (pltpu.roll(sums, 32 - 8 * k, 1) for k in range(4))
    good = lane < 8
    bb, bf = jnp.where(good, bb, 1.0), jnp.where(good, bf, 1.0)
    ff, fff = jnp.where(good, ff, 2.0), jnp.where(good, fff, 8.0)
    alpha_0 = bb / bf
    norm_1 = bb - 2.0 * alpha_0 * bf + alpha_0 * alpha_0 * ff
    gain = 1.0 + norm_1 / bb
    curvature = gain * gain * bf - 2.0 * gain * alpha_0 * ff + alpha_0 * alpha_0 * fff
    alpha_1 = norm_1 / curvature
    kappas = []
    for kappa in (alpha_0 + alpha_1 * gain, alpha_1 * alpha_0):
        kappa = jnp.where(good, kappa, 0.0)
        for shift in (8, 16, 32, 64):
            kappa = kappa + pltpu.roll(kappa, shift, 1)
        kappas.append(kappa)
    gains_ref[0], gains_ref[1] = kappas[0], kappas[1]
    kappa_1, kappa_2 = kappas[0][:1], kappas[1][:1]
    wide = lax.broadcasted_iota(jnp.int32, late.shape, 1)
    extra = pltpu.roll(pltpu.roll(late, HALF, 1), 1, 0)
    last = late + jnp.where(wide < NC, extra, 0.0)
    rows = early - kappa_1 * pltpu.roll(early, HALF, 1) + kappa_2 * last
    turned = jnp.transpose(rows)
    snapshots = jnp.concatenate([turned[8 * j : 8 * j + 8] for j in range(8)], axis=1)
    rows_ref[...] = snapshots
    high, low = two_parts(snapshots)
    both = jnp.concatenate([high, low], axis=0)
    count = snapshots.shape[1]
    product = fast(both, basis_ref[:count], NN) + fast(both, basis_ref[count:], NN)
    gram = dot(snapshots, jnp.concatenate([snapshots, jnp.zeros((LANES - 8, count), f32)], axis=0), NT)
    part = jnp.concatenate([product[:8] + product[8:], gram], axis=1)
    for d in range(part_ref.shape[0]):
        part_ref[d] = part


def finish_body(got_ref, square_ref, basis_ref, rows_ref, columns_ref, projection_ref, factor_ref, *, scale):
    count = got_ref.shape[0]
    reduced = got_ref[0]
    for i in range(1, count):
        reduced = reduced + got_ref[i]
    rank = reduced.shape[1] - LANES
    coefficients = reduced[:, :rank]
    projection_ref[...] = coefficients
    low_rows, high_rows = coefficients[:, :LANES], coefficients[:, LANES:]
    squares = [square_ref[:, 1 + i // 2, i % 2, :] for i in range(4)]
    image = jnp.concatenate(
        [
            dot(low_rows, squares[0], NN) + dot(high_rows, squares[2], NN),
            dot(low_rows, squares[1], NN) + dot(high_rows, squares[3], NN),
        ],
        axis=1,
    )
    gap = image - 2.0 * coefficients
    blank = jnp.zeros((LANES - 8, rank), f32)
    gram = reduced[:, rank:] + dot(coefficients, jnp.concatenate([gap, blank], axis=0), NT)
    row = lax.broadcasted_iota(jnp.int32, (8, LANES), 0)
    lane = lax.broadcasted_iota(jnp.int32, (8, LANES), 1)
    gram = jnp.where(lane < 8, gram, 0.0)
    work = gram + jnp.where(lane == row + 8, 1.0, 0.0)
    upper = jnp.zeros((8, LANES), f32)
    for j in range(8):
        pivot = jnp.sum(jnp.where((row == j) & (lane == j), work, 0.0), axis=(0, 1), keepdims=True)
        line = jnp.sum(jnp.where(row == j, work, 0.0), axis=0, keepdims=True) / jnp.sqrt(pivot)
        upper = jnp.where(row == j, line, upper)
        column = jnp.sum(jnp.where(lane == j, work, 0.0), axis=1, keepdims=True) / jnp.sqrt(pivot)
        work = jnp.where(row > j, work - column * line, work)
    factor_ref[...] = jnp.where((lane >= row) & (lane < 8), upper, 0.0) * (1.0 / scale)
    inverse = pltpu.roll(upper, LANES - 8, 1)
    inverse = jnp.where((lane <= row) & (lane < 8), inverse, 0.0)[:, :8]
    high, low = two_parts(coefficients)
    total = rows_ref.shape[1]
    both = jnp.concatenate([high, low], axis=0)
    product = fast(both, basis_ref[:total], NT) + fast(both, basis_ref[total:], NT)
    remainder = rows_ref[...] - (product[:8] + product[8:])
    columns = dot(inverse, remainder, NN) * scale
    for t in range(8):
        index = 16 * t + lane // 8
        out = jnp.zeros((8, LANES), f32)
        for j in range(8):
            picked = jnp.take_along_axis(columns[:, j * LANES : (j + 1) * LANES], index, axis=1)
            out = jnp.where(lane % 8 == j, picked, out)
        columns_ref[:, t * LANES : (t + 1) * LANES] = out


def shards(
    rr_inverse,
    corner_modes,
    coarse_inverse,
    inertia,
    disp_now,
    vel_now,
    acc_now,
    load_next,
    basis_rows,
    piece_owner,
):
    case_count, _, unknowns = disp_now.shape
    devices = lax.axis_size(AXES)
    coarse_total = coarse_inverse.shape[1]
    rank = basis_rows.shape[1]
    device = lax.axis_index(AXES).reshape(1).astype(jnp.int32)
    pair = ((2, case_count, unknowns),)
    z_shape = ((case_count, 2 * NC),)
    blocks_shape = ((case_count, 2 * LANES),)
    assembled = [pltpu.VMEM((case_count, coarse_total), f32)]

    modes_rows = corner_modes.shape[1]
    start, right_side, to_left, to_right = call(
        start_body,
        [((devices, case_count, LANES),), pair, ((modes_rows, unknowns + NI),), ((modes_rows, NI),)],
        [SMEM] + [VMEM] * 6,
        grant=60 * 1024,
    )(device, load_next, inertia, disp_now, vel_now, acc_now, corner_modes)
    got_1 = exchange(start)
    left_edge = shifted(to_right, 1)
    right_modes = shifted(to_left, -1)
    coarse_parts, local_0 = call(pre_body, [((4 * NC, coarse_total), bf16), pair], [VMEM] * 3, flops=1 << 26)(
        coarse_inverse, right_side, rr_inverse
    )
    blocks_0, coupling, to_blocks = call(
        couple_body, [blocks_shape, ((2 * NC, 2 * LANES),), ((2 * LANES, 4 * NI),)], [SMEM] + [VMEM] * 4, flops=1 << 26
    )(device, corner_modes, right_modes, left_edge, local_0)

    def finish(local, z):
        mine, to_right, to_left = call(
            edge_body, [pair, ((case_count, 2 * NI),), ((case_count, NI),)], [VMEM] * 3, flops=1 << 20
        )(local, z, corner_modes)
        from_left = shifted(to_right, 1)
        from_right = shifted(to_left, -1)
        return mine, from_left, from_right, z, corner_modes, right_modes, rr_inverse, to_blocks

    blocks_scratch = pltpu.VMEM((case_count, 2 * LANES), f32)
    sums_shape = (case_count, LANES)
    pieces, z_0 = call(first_body, [((3 * devices, 4, LANES),), z_shape], [VMEM] * 4, assembled, flops=1 << 24)(
        got_1, coarse_parts, coupling, blocks_0
    )
    got_2 = exchange(pieces)
    basis_parts, square, select = call(
        prep_body,
        [((2 * basis_rows.shape[0], rank), bf16), ((devices, 4, LANES),), ((devices, unknowns), bf16)],
        [VMEM, VMEM, VMEM],
        flops=1 << 26,
        grant=60 * 1024,
    )(basis_rows.reshape(devices, -1, rank), piece_owner.reshape(1, devices), z_0)
    pieces, z_1, terms_1, green, local_1, sums_2 = call(
        join_second_body,
        [((4 * devices, 4, LANES),), z_shape, z_shape, pair, pair, (sums_shape,)],
        [SMEM] + [VMEM] * 12,
        assembled + [blocks_scratch],
        flops=1 << 26,
        grant=60 * 1024,
    )(device, got_2, coarse_parts, coupling, square, *finish(local_0, z_0))
    got_3 = exchange(pieces)
    (early,) = call(early_body, [((devices, LANES),)], [VMEM] * 2, flops=1 << 24)(select, green)
    sent, z_2, image_1, local_2 = call(
        join_third_body,
        [((devices, 3, 2, LANES),), z_shape, pair, pair],
        [SMEM] + [VMEM] * 14,
        assembled + [blocks_scratch, pltpu.VMEM(sums_shape, f32)],
        flops=1 << 26,
        grant=60 * 1024,
    )(device, got_3, coarse_parts, *finish(local_1, z_1), select, sums_2, terms_1, early)
    got_4 = exchange(sent)
    ghost = shifted(z_2, 1)
    (late,) = call(late_body, [pair], [VMEM] * 4, flops=1 << 20)(local_2, z_2, ghost, corner_modes)
    part, snapshots, gains = call(
        project_body,
        [
            ((lax.axis_size(NEAR), case_count, rank + LANES),),
            ((case_count, basis_rows.shape[0]),),
            ((2, case_count, LANES),),
        ],
        [VMEM] * 2,
        flops=1 << 24,
    )(got_4, basis_parts)
    near = exchange(part, NEAR)
    near = near.sum(axis=0)
    got_5 = to_everyone(near, FAR)
    disp_new, vel_new = call(
        out_body, [(disp_now.shape,), (disp_now.shape,)], [VMEM] * 7, flops=1 << 22
    )(green, image_1, late, gains, disp_now, vel_now, acc_now)
    scale = math.sqrt(basis_rows.shape[0] * devices)
    new_columns, projection, factor = call(
        functools.partial(finish_body, scale=scale),
        [((case_count, basis_rows.shape[0]),), ((case_count, rank),), ((case_count, LANES),)],
        [VMEM] * 4,
        flops=1 << 24,
    )(got_5, got_4, basis_parts, snapshots)
    return (disp_new, vel_new, projection.T, factor[:, :case_count], new_columns)


def solution(mesh):
    finer = Mesh(
        mesh.devices.reshape(4, 4, 2, mesh.shape["grp"]), ("sub_0", "sub_1", "sub_2", "grp")
    )
    placed = (
        P(AXES, None, None),
        P(AXES, None, None),
        P(AXES, None),
        P(AXES, None),
        P(None, AXES, None),
        P(None, AXES, None),
        P(None, AXES, None),
        P(None, AXES, None),
        P(AXES, None),
        P(),
    )

    return jax.shard_map(
        shards,
        mesh=finer,
        in_specs=placed,
        out_specs=(P(None, AXES, None), P(None, AXES, None), P(), P(), P(None, AXES)),
        check_vma=False,
    )
```

```python
import functools
import math

import jax
import jax.numpy as jnp
from jax import lax
from jax.experimental import pallas as pl
from jax.experimental.pallas import tpu as pltpu
from jax.sharding import Mesh
from jax.sharding import PartitionSpec as P

NC = 32
NI = 128
LANES = 128
HALF = 64
AXES = ("sub_0", "sub_1", "sub_2", "grp")
FAR, NEAR = ("sub_0", "sub_1"), ("sub_2", "grp")

highest = lax.Precision.HIGHEST
time_step = 0.5
newmark_beta = 0.25
newmark_gamma = 0.5
f32, bf16 = jnp.float32, jnp.bfloat16
NT = (((1,), (1,)), ((), ()))
NN = (((1,), (0,)), ((), ()))
VMEM = pl.BlockSpec(memory_space=pltpu.VMEM)
SMEM = pl.BlockSpec(memory_space=pltpu.SMEM)


def exchange(pieces, axes=AXES):
    return lax.all_to_all(pieces, axes, split_axis=0, concat_axis=0, tiled=True)


def to_everyone(array, axes=AXES):
    return exchange(jnp.broadcast_to(array, (lax.axis_size(axes), *array.shape)), axes)


def shifted(array, by):
    count = lax.axis_size(AXES)
    return lax.ppermute(array, AXES, [(i, (i + by) % count) for i in range(count)])


def dot(a, b, dims):
    return lax.dot_general(a, b, dims, precision=highest, preferred_element_type=f32)


def fast(a, b, dims):
    return lax.dot_general(a, b, dims, preferred_element_type=f32)


def call(body, outs, ins, scratch=(), flops=0, grant=16000):
    return pl.pallas_call(
        body,
        out_shape=[jax.ShapeDtypeStruct(shape, f32 if len(rest) == 0 else rest[0]) for shape, *rest in outs],
        in_specs=ins,
        out_specs=[VMEM] * len(outs),
        scratch_shapes=list(scratch),
        compiler_params=pltpu.CompilerParams(vmem_limit_bytes=grant << 10),
        cost_estimate=pl.CostEstimate(flops=flops, bytes_accessed=1 << 20, transcendentals=0),
    )


def two_parts(x):
    high = x.astype(bf16)
    return high, (x - high.astype(f32)).astype(bf16)


def three_parts(x):
    high = x.astype(bf16)
    rest = x - high.astype(f32)
    middle = rest.astype(bf16)
    return high, middle, (rest - middle.astype(f32)).astype(bf16)


def start_body(device_ref, load_ref, inertia_ref, disp_ref, vel_ref, acc_ref, modes_ref, start_ref, right_ref, to_left_ref, to_right_ref):
    blank = jnp.zeros((NC, modes_ref.shape[2]), f32)
    fields = []
    for s in range(2):
        moved = disp_ref[:, s, :] + time_step * vel_ref[:, s, :]
        moved = moved + (0.5 - newmark_beta) * time_step * time_step * acc_ref[:, s, :]
        fields.append(load_ref[:, s, :] + inertia_ref[s : s + 1] * moved)
        right_ref[s] = fields[s]
    part_0 = jnp.concatenate([modes_ref[0, NC:], blank, blank, modes_ref[0, :NC]], axis=0)
    part_1 = jnp.concatenate([modes_ref[1, :NC], modes_ref[1, NC:], blank, blank], axis=0)
    blocks = dot(fields[0], part_0, NT) + dot(fields[1], part_1, NT)
    even = lax.rem(device_ref[0], 2) == 0
    blocks = jnp.where(even, blocks, pltpu.roll(blocks, HALF, 1))
    for d in range(start_ref.shape[0]):
        start_ref[d] = blocks
    unknowns = modes_ref.shape[2]
    to_left_ref[:, :unknowns] = modes_ref[0]
    to_left_ref[:, unknowns:] = modes_ref[1, :, :NI]
    to_right_ref[...] = modes_ref[1, :, unknowns - NI :]


def pre_body(matrix_ref, right_ref, rr_ref, parts_ref, local_ref):
    rows = matrix_ref.shape[0]
    high, low = two_parts(matrix_ref[...])
    parts_ref[:rows] = high
    parts_ref[rows:] = low
    for s in range(2):
        local_ref[s] = dot(right_ref[s], rr_ref[s], NN)


def couple_body(device_ref, modes_ref, right_ref, left_ref, local_ref, blocks_ref, coupling_ref, to_blocks_ref):
    last = modes_ref.shape[2] - NI
    even = jnp.where(lax.rem(device_ref[0], 2) == 0, 1, 0)
    first, final = [modes_ref[s, :, :NI] for s in range(2)], [modes_ref[s, :, last:] for s in range(2)]
    unknowns = modes_ref.shape[2]
    right_first, right_final = [right_ref[:, :NI], right_ref[:, unknowns:]], right_ref[:, last:unknowns]
    left = left_ref[...]
    rows = [
        {0: left[:NC]},
        {0: left[NC:] - first[0][:NC], 1: final[0][:NC]},
        {0: -first[0][NC:], 1: final[0][NC:] - first[1][:NC], 2: final[1][:NC]},
        {1: -first[1][NC:], 2: final[1][NC:] - right_first[0][:NC], 3: right_final[:NC]},
        {2: -right_first[0][NC:], 3: right_final[NC:] - right_first[1][:NC]},
        {3: -right_first[1][NC:]},
    ]
    to_blocks_ref[...] = jnp.zeros(to_blocks_ref.shape, f32)
    for i, parts in enumerate(rows):
        at = pl.multiple_of(lax.rem(i * NC + 192 * even, 256), NC)
        for k, values in parts.items():
            to_blocks_ref[pl.ds(at, NC), k * NI : (k + 1) * NI] = values
    blank = jnp.zeros((NC, modes_ref.shape[2]), f32)
    unit_0 = jnp.concatenate([modes_ref[0, NC:], blank], axis=0)
    unit_1 = modes_ref[1]
    unit_2 = jnp.concatenate([blank, right_ref[:NC, :unknowns]], axis=0)
    jumps = jnp.concatenate(
        [-unit_0[:, :NI], unit_0[:, last:] - unit_1[:, :NI], unit_1[:, last:] - unit_2[:, :NI], unit_2[:, last:]], axis=1
    )
    coupling_ref[...] = dot(jumps, to_blocks_ref[...], NT)
    blocks_ref[...] = own_blocks(local_ref[0], local_ref[1], to_blocks_ref)


def own_blocks(field_0, field_1, to_blocks_ref):
    last = field_0.shape[1] - NI
    jumps = [-field_0[:, :NI], field_0[:, last:] - field_1[:, :NI], field_1[:, last:]]
    return dot(jnp.concatenate(jumps, axis=1), to_blocks_ref[:, : 3 * NI], NT)


def edge_body(local_ref, z_ref, modes_ref, mine_ref, to_right_ref, to_left_ref):
    last = local_ref.shape[2] - NI
    z = z_ref[...]
    mine_0 = local_ref[0] + dot(z[:, :NC], modes_ref[0, NC:], NN)
    mine_1 = local_ref[1] + dot(z, modes_ref[1], NN)
    mine_ref[0], mine_ref[1] = mine_0, mine_1
    to_left_ref[...] = mine_0[:, :NI]
    to_right_ref[:, :NI] = mine_1[:, last:]
    to_right_ref[:, NI:] = jnp.concatenate([z, z], axis=1)


def join_body(
    mine_ref, from_left_ref, from_right_ref, z_ref, modes_ref, right_ref, rr_ref, to_blocks_ref,
    field_ref, local_ref, blocks_ref, sums_ref,
):
    last = mine_ref.shape[2] - NI
    mine_1 = mine_ref[1]
    ghost = from_left_ref[:, NI : NI + 2 * NC]
    mine_0 = mine_ref[0] + dot(ghost[:, NC:], modes_ref[0, :NC], NN)
    field_ref[0], field_ref[1] = mine_0, mine_1
    jump_a = from_left_ref[:, :NI] - mine_0[:, :NI]
    jump_b = mine_0[:, last:] - mine_1[:, :NI]
    jump_c = mine_1[:, last:] - (from_right_ref[...] + dot(z_ref[:, NC:], right_ref[:NC, :NI], NN))
    inner = jnp.zeros((mine_1.shape[0], 1), f32)
    outs = []
    for s, (first, final) in enumerate([(-jump_a, jump_b), (-jump_b, jump_c)]):
        out = dot(first, rr_ref[s, :NI], NN) + dot(final, rr_ref[s, last:], NN)
        local_ref[s] = out
        inner = inner + jnp.sum(out[:, :NI] * first + out[:, last:] * final, axis=1, keepdims=True)
        outs.append(out)
    blocks_ref[...] = own_blocks(outs[0], outs[1], to_blocks_ref)
    square = jnp.sum(jump_b * jump_b + jump_c * jump_c, axis=1, keepdims=True)
    lane = lax.broadcasted_iota(jnp.int32, sums_ref.shape, 1)
    sums_ref[...] = jnp.where(lane == 0, square, 0.0) + jnp.where(lane == 1, inner, 0.0)


def prep_body(basis_ref, owner_ref, after_ref, parts_ref, square_ref, select_ref):
    devices, width, rank = basis_ref.shape
    total = devices * width
    square = jnp.zeros((rank, rank), f32)
    for j in range(width):
        rows = basis_ref[:, j, :]
        high, low = two_parts(rows)
        parts_ref[j * devices : (j + 1) * devices] = high
        parts_ref[total + j * devices : total + (j + 1) * devices] = low
        turned_high, turned_low = two_parts(jnp.transpose(rows))
        square = square + fast(turned_high, high, NN) + (fast(turned_high, low, NN) + fast(turned_low, high, NN))
    for i in range(4):
        r, h = i // 2, i % 2
        square_ref[:, i, :] = square[r * LANES : (r + 1) * LANES, h * LANES : (h + 1) * LANES]
    unknowns = select_ref.shape[1]
    rows = lax.broadcasted_iota(jnp.int32, (devices, unknowns), 0)
    columns = lax.broadcasted_iota(jnp.int32, (devices, unknowns), 1)
    each = unknowns // devices
    repeat = jnp.where(columns // each == rows, 1.0, 0.0).astype(bf16)
    owner = jnp.broadcast_to(owner_ref[...].astype(f32), (8, devices)).astype(bf16)
    owner = fast(owner, repeat, NN)[:1]
    select_ref[...] = jnp.where(owner == rows.astype(f32), 1.0, 0.0).astype(bf16)


def late_body(local_ref, z_ref, modes_ref, late_ref):
    z = z_ref[...]
    late_ref[0] = local_ref[0] + dot(z[:, :NC], modes_ref[0, NC:], NN)
    late_ref[1] = local_ref[1] + dot(z, modes_ref[1], NN)


def out_body(
    green_ref, image_ref, late_ref, ghost_ref, modes_ref, gains_ref, disp_ref, vel_ref, acc_ref, disp_out_ref, vel_out_ref
):
    kappa_1, kappa_2 = gains_ref[0], gains_ref[1]
    case = lax.broadcasted_iota(jnp.int32, kappa_1.shape, 0)
    lane = lax.broadcasted_iota(jnp.int32, kappa_1.shape, 1)
    kappa_1 = jnp.sum(jnp.where(case == lane, kappa_1, 0.0), axis=1, keepdims=True)
    kappa_2 = jnp.sum(jnp.where(case == lane, kappa_2, 0.0), axis=1, keepdims=True)
    ghost = ghost_ref[...][:, NC:]
    late = [late_ref[0] + dot(ghost, modes_ref[0, :NC], NN), late_ref[1]]
    for s in range(2):
        disp = green_ref[s] - kappa_1 * image_ref[s] + kappa_2 * late[s]
        vel, acc = vel_ref[:, s, :], acc_ref[:, s, :]
        accel = (
            (disp - disp_ref[:, s, :]) * (1.0 / (newmark_beta * time_step * time_step))
            - vel * (1.0 / (newmark_beta * time_step))
            - (0.5 / newmark_beta - 1.0) * acc
        )
        disp_out_ref[:, s, :] = disp
        vel_out_ref[:, s, :] = vel + time_step * ((1.0 - newmark_gamma) * acc + newmark_gamma * accel)


def coarse_product(assembled_ref, parts_ref):
    cases = assembled_ref.shape[0]
    high, low = two_parts(assembled_ref[...])
    both = fast(jnp.concatenate([high, low], axis=0), parts_ref[...], NT)
    both = both[:cases] + both[cases:]
    return both[:, :HALF] + both[:, HALF:]


def assemble_packed(got_ref, assembled_ref, slots):
    tiles = assembled_ref.shape[1] // LANES
    lane = lax.broadcasted_iota(jnp.int32, (4, LANES), 1)
    lower = lane < HALF
    for m in range(tiles):
        even, odd = 2 * slots * m, 2 * slots * m + slots
        following = 2 * slots * ((m + 1) % tiles) + 2
        previous = 2 * slots * ((m - 1) % tiles) + slots + 2
        extra_even, extra_odd = got_ref[following], got_ref[previous]
        top = got_ref[even] + got_ref[odd] + jnp.where(lower, extra_odd, extra_even)
        turned = pltpu.roll(jnp.where(lower, extra_even, extra_odd), HALF, 1)
        bottom = got_ref[even + 1] + got_ref[odd + 1] + turned
        assembled_ref[0:4, m * LANES : (m + 1) * LANES] = top
        assembled_ref[4:8, m * LANES : (m + 1) * LANES] = bottom


def assemble_first(got_ref, assembled_ref):
    tiles = assembled_ref.shape[1] // LANES
    lane = lax.broadcasted_iota(jnp.int32, (8, LANES), 1)
    for m in range(tiles):
        following = (2 * m + 2) % (2 * tiles)
        own = got_ref[2 * m + 1] + jnp.where(lane < HALF, got_ref[2 * m], 0.0)
        assembled_ref[:, m * LANES : (m + 1) * LANES] = own + jnp.where(
            lane >= LANES - NC, got_ref[following], 0.0
        )


def owned_terms(device_ref, assembled_ref, z):
    device = device_ref[0]
    tile = assembled_ref[:, pl.ds(pl.multiple_of((device // 2) * LANES, LANES), LANES)]
    even = lax.rem(device, 2) == 0
    return jnp.where(even, tile[:, :HALF], tile[:, HALF:]) * z


def send_blocks(z, coupling_ref, local_ref, pieces_ref, slots, riding_ref=None):
    blocks = local_ref[...] + dot(z, coupling_ref[...], NN)
    main, extra = blocks[:, :LANES], blocks[:, LANES:]
    turned = pltpu.roll(extra, HALF, 1)
    packed = extra[0:4] + turned[4:8]
    for d in range(pieces_ref.shape[0] // slots):
        pieces_ref[slots * d] = main[0:4]
        pieces_ref[slots * d + 1] = main[4:8]
        pieces_ref[slots * d + 2] = packed
        if riding_ref is not None:
            pieces_ref[slots * d + 3] = riding_ref[d]


def first_body(got_ref, parts_ref, coupling_ref, local_ref, pieces_ref, z_ref, assembled_ref):
    assemble_first(got_ref, assembled_ref)
    z = coarse_product(assembled_ref, parts_ref)
    z_ref[...] = z
    send_blocks(z, coupling_ref, local_ref, pieces_ref, 3)


def second_body(
    device_ref, got_ref, parts_ref, coupling_ref, local_ref, square_ref, pieces_ref, z_ref, terms_ref, assembled_ref
):
    assemble_packed(got_ref, assembled_ref, 3)
    z = coarse_product(assembled_ref, parts_ref)
    z_ref[...] = z
    terms_ref[...] = owned_terms(device_ref, assembled_ref, z)
    send_blocks(z, coupling_ref, local_ref, pieces_ref, 4, square_ref)


def join_second_body(
    device_ref, got_ref, parts_ref, coupling_ref, square_ref, mine_ref, from_left_ref, from_right_ref, before_ref,
    modes_ref, right_ref, rr_ref, to_blocks_ref,
    pieces_ref, z_ref, terms_ref, field_ref, local_ref, sums_ref, assembled_ref, blocks_ref,
):
    join_body(
        mine_ref, from_left_ref, from_right_ref, before_ref, modes_ref, right_ref, rr_ref, to_blocks_ref,
        field_ref, local_ref, blocks_ref, sums_ref,
    )
    second_body(
        device_ref, got_ref, parts_ref, coupling_ref, blocks_ref, square_ref, pieces_ref, z_ref, terms_ref, assembled_ref
    )


def join_third_body(
    device_ref, got_ref, parts_ref, mine_ref, from_left_ref, from_right_ref, before_ref,
    modes_ref, right_ref, rr_ref, to_blocks_ref, select_ref, sums_2_ref, terms_ref, early_ref,
    sent_ref, z_ref, field_ref, local_ref, assembled_ref, blocks_ref, sums_3_ref,
):
    join_body(
        mine_ref, from_left_ref, from_right_ref, before_ref, modes_ref, right_ref, rr_ref, to_blocks_ref,
        field_ref, local_ref, blocks_ref, sums_3_ref,
    )
    third_body(
        device_ref, got_ref, parts_ref, local_ref, modes_ref, right_ref, select_ref, sums_2_ref, sums_3_ref, terms_ref,
        field_ref, early_ref, sent_ref, z_ref, assembled_ref,
    )


def choose_rows(select_ref, rows):
    high, middle, low = three_parts(rows)
    select = select_ref[...]
    return fast(select, high, NT) + fast(select, middle, NT) + fast(select, low, NT)


def by_offset(field):
    lane = lax.broadcasted_iota(jnp.int32, field.shape, 1)
    return [jnp.where(lane % 4 == o, field, 0.0) for o in range(4)]


def early_body(select_ref, green_ref, chosen_ref):
    rows = by_offset(green_ref[0]) + by_offset(green_ref[1])
    rows.append(jnp.zeros((HALF, green_ref.shape[2]), f32))
    chosen_ref[...] = choose_rows(select_ref, jnp.concatenate(rows, axis=0))


def third_body(
    device_ref, got_ref, parts_ref, local_ref, modes_ref, right_ref, select_ref, sums_2_ref, sums_3_ref, terms_ref,
    image_ref, early_ref,
    sent_ref, z_ref, assembled_ref,
):
    assemble_packed(got_ref, assembled_ref, 4)
    z = coarse_product(assembled_ref, parts_ref)
    z_ref[...] = z
    square = got_ref[3]
    for d in range(1, got_ref.shape[0] // 4):
        square = square + got_ref[4 * d + 3]
    y_0 = local_ref[0] + dot(z[:, :NC], modes_ref[0, NC:], NN)
    y_1 = local_ref[1] + dot(z, modes_ref[1], NN)
    y_2 = dot(z[:, NC:], right_ref[:NC, : modes_ref.shape[2]], NN)
    rows = by_offset(y_0) + by_offset(y_1) + by_offset(y_2)
    rows.append(jnp.zeros((32, y_0.shape[1]), f32))
    late = choose_rows(select_ref, jnp.concatenate(rows, axis=0))
    curvature = jnp.sum(owned_terms(device_ref, assembled_ref, z), axis=1, keepdims=True)
    lane = lax.broadcasted_iota(jnp.int32, (8, LANES), 1)
    case = lax.broadcasted_iota(jnp.int32, (8, LANES), 0)
    parts = [
        sums_2_ref[:, 0:1],
        sums_2_ref[:, 1:2] + jnp.sum(terms_ref[...], axis=1, keepdims=True),
        sums_3_ref[:, 0:1],
        sums_3_ref[:, 1:2] + curvature,
    ]
    placed = jnp.zeros((8, LANES), f32)
    for k in range(4):
        placed = placed + jnp.where(lane == 96 + 8 * k + case, parts[k], 0.0)
    late = late + jnp.sum(placed, axis=0, keepdims=True)
    rows = [jnp.zeros((HALF, y_0.shape[1]), f32)] + by_offset(image_ref[0]) + by_offset(image_ref[1])
    sent_ref[:, 0, 0, :] = early_ref[...] + choose_rows(select_ref, jnp.concatenate(rows, axis=0))
    sent_ref[:, 0, 1, :] = late
    sent_ref[:, 1] = jnp.broadcast_to(square[None, 0:2], (late.shape[0], 2, LANES))
    sent_ref[:, 2] = jnp.broadcast_to(square[None, 2:4], (late.shape[0], 2, LANES))


def project_body(got_ref, basis_ref, part_ref, rows_ref, gains_ref):
    early, late = got_ref[:, 0, 0, :], got_ref[:, 0, 1, :]
    sums = jnp.broadcast_to(jnp.sum(late, axis=0, keepdims=True), (8, LANES))
    lane = lax.broadcasted_iota(jnp.int32, (8, LANES), 1)
    bb, bf, ff, fff = (pltpu.roll(sums, 32 - 8 * k, 1) for k in range(4))
    good = lane < 8
    bb, bf = jnp.where(good, bb, 1.0), jnp.where(good, bf, 1.0)
    ff, fff = jnp.where(good, ff, 2.0), jnp.where(good, fff, 8.0)
    alpha_0 = bb / bf
    norm_1 = bb - 2.0 * alpha_0 * bf + alpha_0 * alpha_0 * ff
    gain = 1.0 + norm_1 / bb
    curvature = gain * gain * bf - 2.0 * gain * alpha_0 * ff + alpha_0 * alpha_0 * fff
    alpha_1 = norm_1 / curvature
    kappas = []
    for kappa in (alpha_0 + alpha_1 * gain, alpha_1 * alpha_0):
        kappa = jnp.where(good, kappa, 0.0)
        for shift in (8, 16, 32, 64):
            kappa = kappa + pltpu.roll(kappa, shift, 1)
        kappas.append(kappa)
    gains_ref[0], gains_ref[1] = kappas[0], kappas[1]
    kappa_1, kappa_2 = kappas[0][:1], kappas[1][:1]
    wide = lax.broadcasted_iota(jnp.int32, late.shape, 1)
    extra = pltpu.roll(pltpu.roll(late, HALF, 1), 1, 0)
    last = late + jnp.where(wide < NC, extra, 0.0)
    rows = early - kappa_1 * pltpu.roll(early, HALF, 1) + kappa_2 * last
    turned = jnp.transpose(rows)
    snapshots = jnp.concatenate([turned[8 * j : 8 * j + 8] for j in range(8)], axis=1)
    rows_ref[...] = snapshots
    high, low = two_parts(snapshots)
    both = jnp.concatenate([high, low], axis=0)
    count = snapshots.shape[1]
    product = fast(both, basis_ref[:count], NN) + fast(both, basis_ref[count:], NN)
    gram = dot(snapshots, jnp.concatenate([snapshots, jnp.zeros((LANES - 8, count), f32)], axis=0), NT)
    part = jnp.concatenate([product[:8] + product[8:], gram], axis=1)
    for d in range(part_ref.shape[0]):
        part_ref[d] = part


def finish_body(got_ref, square_ref, basis_ref, rows_ref, columns_ref, projection_ref, factor_ref, *, scale):
    count = got_ref.shape[0]
    reduced = got_ref[0]
    for i in range(1, count):
        reduced = reduced + got_ref[i]
    rank = reduced.shape[1] - LANES
    coefficients = reduced[:, :rank]
    projection_ref[...] = coefficients
    low_rows, high_rows = coefficients[:, :LANES], coefficients[:, LANES:]
    squares = [square_ref[:, 1 + i // 2, i % 2, :] for i in range(4)]
    image = jnp.concatenate(
        [
            dot(low_rows, squares[0], NN) + dot(high_rows, squares[2], NN),
            dot(low_rows, squares[1], NN) + dot(high_rows, squares[3], NN),
        ],
        axis=1,
    )
    gap = image - 2.0 * coefficients
    blank = jnp.zeros((LANES - 8, rank), f32)
    gram = reduced[:, rank:] + dot(coefficients, jnp.concatenate([gap, blank], axis=0), NT)
    row = lax.broadcasted_iota(jnp.int32, (8, LANES), 0)
    lane = lax.broadcasted_iota(jnp.int32, (8, LANES), 1)
    gram = jnp.where(lane < 8, gram, 0.0)
    work = gram + jnp.where(lane == row + 8, 1.0, 0.0)
    upper = jnp.zeros((8, LANES), f32)
    for j in range(8):
        pivot = jnp.sum(jnp.where((row == j) & (lane == j), work, 0.0), axis=(0, 1), keepdims=True)
        line = jnp.sum(jnp.where(row == j, work, 0.0), axis=0, keepdims=True) / jnp.sqrt(pivot)
        upper = jnp.where(row == j, line, upper)
        column = jnp.sum(jnp.where(lane == j, work, 0.0), axis=1, keepdims=True) / jnp.sqrt(pivot)
        work = jnp.where(row > j, work - column * line, work)
    factor_ref[...] = jnp.where((lane >= row) & (lane < 8), upper, 0.0) * (1.0 / scale)
    inverse = pltpu.roll(upper, LANES - 8, 1)
    inverse = jnp.where((lane <= row) & (lane < 8), inverse, 0.0)[:, :8]
    high, low = two_parts(coefficients)
    total = rows_ref.shape[1]
    both = jnp.concatenate([high, low], axis=0)
    product = fast(both, basis_ref[:total], NT) + fast(both, basis_ref[total:], NT)
    remainder = rows_ref[...] - (product[:8] + product[8:])
    columns = dot(inverse, remainder, NN) * scale
    for t in range(8):
        index = 16 * t + lane // 8
        out = jnp.zeros((8, LANES), f32)
        for j in range(8):
            picked = jnp.take_along_axis(columns[:, j * LANES : (j + 1) * LANES], index, axis=1)
            out = jnp.where(lane % 8 == j, picked, out)
        columns_ref[:, t * LANES : (t + 1) * LANES] = out


def shards(
    rr_inverse,
    corner_modes,
    coarse_inverse,
    inertia,
    disp_now,
    vel_now,
    acc_now,
    load_next,
    basis_rows,
    piece_owner,
):
    case_count, _, unknowns = disp_now.shape
    devices = lax.axis_size(AXES)
    coarse_total = coarse_inverse.shape[1]
    rank = basis_rows.shape[1]
    device = lax.axis_index(AXES).reshape(1).astype(jnp.int32)
    pair = ((2, case_count, unknowns),)
    z_shape = ((case_count, 2 * NC),)
    blocks_shape = ((case_count, 2 * LANES),)
    assembled = [pltpu.VMEM((case_count, coarse_total), f32)]

    modes_rows = corner_modes.shape[1]
    start, right_side, to_left, to_right = call(
        start_body,
        [((devices, case_count, LANES),), pair, ((modes_rows, unknowns + NI),), ((modes_rows, NI),)],
        [SMEM] + [VMEM] * 6,
        grant=60 * 1024,
    )(device, load_next, inertia, disp_now, vel_now, acc_now, corner_modes)
    got_1 = exchange(start)
    left_edge = shifted(to_right, 1)
    right_modes = shifted(to_left, -1)
    coarse_parts, local_0 = call(pre_body, [((4 * NC, coarse_total), bf16), pair], [VMEM] * 3, flops=1 << 26)(
        coarse_inverse, right_side, rr_inverse
    )
    blocks_0, coupling, to_blocks = call(
        couple_body, [blocks_shape, ((2 * NC, 2 * LANES),), ((2 * LANES, 4 * NI),)], [SMEM] + [VMEM] * 4, flops=1 << 26
    )(device, corner_modes, right_modes, left_edge, local_0)

    def finish(local, z):
        mine, to_right, to_left = call(
            edge_body, [pair, ((case_count, 2 * NI),), ((case_count, NI),)], [VMEM] * 3, flops=1 << 20
        )(local, z, corner_modes)
        from_left = shifted(to_right, 1)
        from_right = shifted(to_left, -1)
        return mine, from_left, from_right, z, corner_modes, right_modes, rr_inverse, to_blocks

    blocks_scratch = pltpu.VMEM((case_count, 2 * LANES), f32)
    sums_shape = (case_count, LANES)
    pieces, z_0 = call(first_body, [((3 * devices, 4, LANES),), z_shape], [VMEM] * 4, assembled, flops=1 << 24)(
        got_1, coarse_parts, coupling, blocks_0
    )
    got_2 = exchange(pieces)
    basis_parts, square, select = call(
        prep_body,
        [((2 * basis_rows.shape[0], rank), bf16), ((devices, 4, LANES),), ((devices, unknowns), bf16)],
        [VMEM, VMEM, VMEM],
        flops=1 << 26,
        grant=60 * 1024,
    )(basis_rows.reshape(devices, -1, rank), piece_owner.reshape(1, devices), z_0)
    pieces, z_1, terms_1, green, local_1, sums_2 = call(
        join_second_body,
        [((4 * devices, 4, LANES),), z_shape, z_shape, pair, pair, (sums_shape,)],
        [SMEM] + [VMEM] * 12,
        assembled + [blocks_scratch],
        flops=1 << 26,
        grant=60 * 1024,
    )(device, got_2, coarse_parts, coupling, square, *finish(local_0, z_0))
    got_3 = exchange(pieces)
    (early,) = call(early_body, [((devices, LANES),)], [VMEM] * 2, flops=1 << 24)(select, green)
    sent, z_2, image_1, local_2 = call(
        join_third_body,
        [((devices, 3, 2, LANES),), z_shape, pair, pair],
        [SMEM] + [VMEM] * 14,
        assembled + [blocks_scratch, pltpu.VMEM(sums_shape, f32)],
        flops=1 << 26,
        grant=60 * 1024,
    )(device, got_3, coarse_parts, *finish(local_1, z_1), select, sums_2, terms_1, early)
    got_4 = exchange(sent)
    ghost = shifted(z_2, 1)
    (late,) = call(late_body, [pair], [VMEM] * 3, flops=1 << 20)(local_2, z_2, corner_modes)
    part, snapshots, gains = call(
        project_body,
        [
            ((lax.axis_size(NEAR), case_count, rank + LANES),),
            ((case_count, basis_rows.shape[0]),),
            ((2, case_count, LANES),),
        ],
        [VMEM] * 2,
        flops=1 << 24,
    )(got_4, basis_parts)
    part, ghost = lax.optimization_barrier((part, ghost))
    near = exchange(part, NEAR)
    near = near.sum(axis=0)
    got_5 = to_everyone(near, FAR)
    disp_new, vel_new = call(
        out_body, [(disp_now.shape,), (disp_now.shape,)], [VMEM] * 9, flops=1 << 22
    )(green, image_1, late, ghost, corner_modes, gains, disp_now, vel_now, acc_now)
    scale = math.sqrt(basis_rows.shape[0] * devices)
    new_columns, projection, factor = call(
        functools.partial(finish_body, scale=scale),
        [((case_count, basis_rows.shape[0]),), ((case_count, rank),), ((case_count, LANES),)],
        [VMEM] * 4,
        flops=1 << 24,
    )(got_5, got_4, basis_parts, snapshots)
    return (disp_new, vel_new, projection.T, factor[:, :case_count], new_columns)


def solution(mesh):
    finer = Mesh(
        mesh.devices.reshape(4, 4, 2, mesh.shape["grp"]), ("sub_0", "sub_1", "sub_2", "grp")
    )
    placed = (
        P(AXES, None, None),
        P(AXES, None, None),
        P(AXES, None),
        P(AXES, None),
        P(None, AXES, None),
        P(None, AXES, None),
        P(None, AXES, None),
        P(None, AXES, None),
        P(AXES, None),
        P(),
    )

    return jax.shard_map(
        shards,
        mesh=finer,
        in_specs=placed,
        out_specs=(P(None, AXES, None), P(None, AXES, None), P(), P(), P(None, AXES)),
        check_vma=False,
    )
```
